32 devices in a mesh: param: 16 (over z, y, x), sensor: 2 (over core).
Axes of the slice: x: 2, y: 2, z: 4, core: 2. Of those that a mesh axis runs over, the one named last changes fastest.
Arguments:
- data: float32 [16, 512, 420], P(None, ('sensor', 'param')), may hold values from -6 to 6
- spectra: float32 [2, 512, 64, 421], P(None, 'sensor', 'param'), may hold values from -2 to 2
Outputs:
- gradient: float32 [16, 64, 420], P(None, 'param')
- rms: float32 [16], replicated
The draws below stay inside these ranges and needn't reach their ends.
All inputs are finite; a program needn't handle non-finite values.
Results may differ from the reference program's by a relative error of at most 0.0003.
Values sent between devices are 32-bit elements; how exact they have to be, the bound alone decides.
A program may use at most 128 MiB of HBM per device.

```python
import math
import jax
import jax.numpy as jnp
from jax import lax

SENSORS = 512
NT = 420
NF = 421
P_DEV = 4
NRHS = 16
PARAMS = 64
N_PARAM = 16


def draw_spectra(key, part):
    first = jax.random.fold_in(key, 0)
    shape = (2, SENSORS, PARAMS, NF)
    ramp = 1.0 + jnp.arange(PARAMS, dtype=jnp.float32) / max(PARAMS - 1, 1)
    base = jnp.clip(jax.random.normal(first, shape, jnp.float32), -6.0, 6.0)
    base = base * ramp[None, None, :, None]
    return jnp.clip(base / math.sqrt(SENSORS), -2.0, 2.0)


def shard_levels(rng, dims, cuts, smallest, largest):
    gain = 1.0
    for dim, blocks in cuts:
        heights = jax.random.uniform(jax.random.fold_in(jax.random.fold_in(rng, 6), dim), (blocks,), jnp.float32, smallest / len(cuts), largest / len(cuts))
        gain = gain * jnp.repeat(jnp.exp(heights), dims[dim] // blocks).reshape((-1,) + (1,) * (len(dims) - 1 - dim))
    return gain


def gaussian(rng, shape, scale, limit, shards=(), kind=jnp.bfloat16):
    values = jax.random.normal(rng, shape, jnp.float32) * scale
    if len(shards) > 0:
        values = shard_levels(rng, shape, shards, -0.22, 0.18) * values
    return jnp.clip(values, min=-limit, max=limit).astype(kind)


def setup_inputs(seed: int = 0) -> dict:
    seeds = jax.random.split(jax.random.key(seed), 3)
    data = gaussian(seeds[0], (NRHS, SENSORS, NT), 1.0, 6.0, ((1, 32),), jnp.float32)
    spectra = draw_spectra(jax.random.fold_in(seeds[2], 71), 0)
    return dict(data=data, spectra=spectra)


def reference(data, spectra):
    data_hat = jnp.fft.rfft(data, n=2 * NT, axis=-1)
    real_part = jnp.real(data_hat).astype(jnp.float32)
    imag_part = jnp.imag(data_hat).astype(jnp.float32)

    def one_block(index):
        start = (index * P_DEV).astype(jnp.int32)
        kernel = lax.dynamic_slice_in_dim(spectra, start, P_DEV, 2)
        kernel_re = kernel[0]
        kernel_im = kernel[1]
        hi = lax.Precision.HIGHEST
        out_re = jnp.einsum('spf,rsf->rpf', kernel_re, real_part, precision=hi) + jnp.einsum('spf,rsf->rpf', kernel_im, imag_part, precision=hi)
        out_im = jnp.einsum('spf,rsf->rpf', kernel_re, imag_part, precision=hi) - jnp.einsum('spf,rsf->rpf', kernel_im, real_part, precision=hi)
        return (out_re, out_im)
    blocks_re, blocks_im = lax.map(one_block, jnp.arange(N_PARAM, dtype=jnp.int32))
    whole_re = jnp.transpose(blocks_re, (1, 0, 2, 3)).reshape(data.shape[0], PARAMS, NF)
    whole_im = jnp.transpose(blocks_im, (1, 0, 2, 3)).reshape(data.shape[0], PARAMS, NF)
    field = jnp.fft.irfft(whole_re + 1j * whole_im, n=2 * NT, axis=-1)[..., :NT].astype(jnp.float32)
    rms = jnp.sqrt(lax.optimization_barrier(jnp.mean(field * field, axis=(1, 2))) + 1e-06)
    return (field / rms[:, None, None], rms)
```

```python
import functools
import math

import jax
import jax.numpy as jnp
import numpy as np
from jax import lax
from jax.experimental import pallas as pl
from jax.experimental.pallas import tpu as pltpu
from jax.sharding import PartitionSpec as P

MESH = pl.DeviceIdType.MESH
LANES = 128
GROUP = 8
CHUNKS = 8
PIECE = 3


def spectral_tables(steps):
    length = 2 * steps
    freqs = steps + 1
    times = lax.broadcasted_iota(jnp.int32, (steps, freqs), 0)
    bins = lax.broadcasted_iota(jnp.int32, (steps, freqs), 1)
    phase = 2.0 * math.pi / length * (times * bins % length).astype(jnp.float32)
    forward = jnp.concatenate([jnp.cos(phase), -jnp.sin(phase)], axis=1)
    weight = jnp.where((bins == 0) | (bins == steps), 1.0, 2.0) / length
    backward = jnp.concatenate([(weight * jnp.cos(phase)).T, (-weight * jnp.sin(phase)).T], axis=0)
    return (forward, backward)


def to_spectrum(series, forward):
    vectors, sensors, steps = series.shape
    flat = jnp.dot(
        series.reshape(vectors * sensors, steps),
        forward,
        precision=lax.Precision.HIGHEST,
        preferred_element_type=jnp.float32,
    )
    return flat.reshape(vectors, sensors, forward.shape[1])


def contract(kernel, spectrum):
    return jnp.einsum(
        "spf,rsf->rpf",
        kernel,
        spectrum,
        precision=lax.Precision.HIGHEST,
        preferred_element_type=jnp.float32,
    )


def general_body(data, spectra):
    steps = data.shape[2]
    freqs = steps + 1
    forward, backward = spectral_tables(steps)
    whole = to_spectrum(lax.all_gather(data, "param", axis=1, tiled=True), forward)
    real_part = whole[..., :freqs]
    imag_part = whole[..., freqs:]
    kernel_re = spectra[0]
    kernel_im = spectra[1]
    out_re = contract(kernel_re, real_part) + contract(kernel_im, imag_part)
    out_im = contract(kernel_re, imag_part) - contract(kernel_im, real_part)
    vectors, points = (out_re.shape[0], out_re.shape[1])
    stacked = jnp.concatenate([out_re, out_im], axis=2).reshape(vectors * points, 2 * freqs)
    partial_field = jnp.dot(
        stacked, backward, precision=lax.Precision.HIGHEST, preferred_element_type=jnp.float32
    ).reshape(vectors, points, steps)
    count = points * lax.axis_size("param") * steps
    share = lax.psum_scatter(partial_field, "sensor", scatter_dimension=0, tiled=True)
    squares = lax.psum(jnp.sum(share * share, axis=(1, 2)), "param")
    scale = jnp.sqrt(squares / count + 1e-06)
    normalized = share / scale[:, None, None]
    gradient, rms_all = (
        lax.all_gather(normalized, "sensor", axis=0, tiled=True),
        lax.all_gather(scale, "sensor", axis=0, tiled=True),
    )
    return (gradient, rms_all)


def split(value):
    high = value.astype(jnp.bfloat16)
    return high, (value - high.astype(jnp.float32)).astype(jnp.bfloat16)


NT_DIMS = (((1,), (1,)), ((), ()))


def product(left, right, dims):
    dot = functools.partial(lax.dot_general, dimension_numbers=dims, preferred_element_type=jnp.float32)
    size = left[0].shape[0]
    both = dot(jnp.concatenate(left, axis=0), right[0])
    return both[:size] + (both[size:] + dot(left[0], right[1]))


def split_product(table, rows, right):
    dot = functools.partial(lax.dot_general, dimension_numbers=NT_DIMS, preferred_element_type=jnp.float32)
    half = table.shape[0] // 2
    both = dot(table, right[0])
    return both[:rows] + (both[half : half + rows] + dot(table[:half], right[1])[:rows])


def folded_layout_fits(steps):
    half = steps // 2
    rest = half + 1 - LANES
    groups = -(-(steps + 1) // (2 * GROUP))
    fits = steps % 2 == 0 and 0 < rest < LANES and half - LANES - (LANES - rest) <= LANES - rest
    return fits and groups % PIECE == 0


def frequency_order(freqs, groups):
    bins = np.arange(groups * 2 * GROUP).reshape(groups, 2, GROUP)
    return [bins[:, core].reshape(-1) for core in range(2)]


def lane_times(steps):
    half = steps // 2
    rest = half + 1 - LANES
    room = LANES - rest
    lane = np.arange(LANES)
    first = np.where(lane < rest, LANES + lane, -1)
    first_odd = np.where(lane < rest - 1, LANES + lane, -1)
    second = np.where(lane >= room, LANES + lane - room, -1)
    tail_a = np.where(lane >= rest, LANES + lane - rest, -1)
    tail_b = np.where(lane < rest - 1 - room, LANES + room + lane, -1)
    return lane, first, first_odd, second, tail_a, tail_b


def fold_maps(steps):
    lane, first, first_odd, second, tail_a, tail_b = lane_times(steps)
    shared = np.where(second >= 0, second, tail_b)
    even = np.concatenate([lane, lane, first, first_odd])
    odd = np.concatenate([lane, lane, tail_a, shared])
    ones = np.ones(LANES, np.int64)
    even_sign = np.concatenate([ones, -ones, ones, -ones])
    odd_sign = np.concatenate([ones, -ones, -ones, np.where(second >= 0, 1, -1)])
    maps = np.full((8, 4 * LANES), -1, np.int32)
    for index, (time, sign) in enumerate(((even, even_sign), (odd, odd_sign))):
        mirror = np.where((time > 0) & (2 * time != steps), steps - time, -1)
        maps[3 * index] = time
        maps[3 * index + 1] = np.where(time < 0, -1, mirror)
        maps[3 * index + 2] = sign
    return maps


def halves(values):
    high = values.astype(jnp.bfloat16)
    return high, (values - high.astype(np.float32)).astype(jnp.bfloat16)


def paired_tables(steps, freqs, groups, rows_pad, wide):
    half = steps // 2
    lane, first, first_odd, second, tail_a, tail_b = lane_times(steps)
    tail = np.where(tail_a >= 0, tail_a, tail_b)
    forward, backward = [], []
    for bins in frequency_order(freqs, groups):
        count = bins.shape[0]
        known = (bins < freqs)[:, None]
        even = (bins % 2 == 0)[:, None]
        angle = bins[:, None] * np.arange(steps)[None, :] % (2 * steps)
        phase = np.pi / steps * angle
        sine = np.where(angle % steps == 0, 0.0, np.sin(phase))
        cosine = np.cos(phase)
        symmetric = np.where(known, np.where(even, cosine, -sine), 0.0)
        other = np.where(known, np.where(even, -sine, cosine), 0.0)
        blocks = []
        for table, times in (
            (symmetric, lane), (other, lane), (symmetric, first), (other, first_odd), (symmetric, second), (other, tail),
        ):
            limit = half if table is symmetric else half - 1
            inside = (times >= 0) & (times <= limit)
            value = np.where(inside[None, :], table[:, np.clip(times, 0, limit)], 0.0).astype(np.float32)
            block = np.zeros((2, rows_pad, LANES), jnp.bfloat16)
            block[0, :count], block[1, :count] = halves(value)
            blocks.append(block.reshape(2 * rows_pad, LANES))
        forward.append(np.stack(blocks))
        weight = np.where((bins == 0) | (bins == steps), 0.5, 1.0)[:, None] / steps
        inverse = np.zeros((2, 2, rows_pad, wide), jnp.bfloat16)
        for position, table in enumerate((symmetric, other)):
            value = (table * weight).astype(np.float32)
            inverse[0, position, :count, :steps], inverse[1, position, :count, :steps] = halves(value)
        backward.append(inverse)
    return np.stack(forward), np.stack(backward)


def kernel(
    n, lines, vectors, local, steps, points, freqs, groups, wide,
    data_ref, spectra_ref, forward_ref, backward_ref, maps_ref,
    out_ref, rms_ref,
    series, fold, raw, packed, kbuf, gathered, table, inverse, spectrum, product_s, own_val, send_val, recv_val,
    partial, pair, square, squares,
    load_sem, raw_sem, k_send, k_recv, z_send, z_recv, y_send, y_recv, c_send, c_recv, w_send, w_recv,
    v_send, v_recv, f_send, f_recv, r_send, r_recv,
):
    me = lax.axis_index("param")
    core = lax.axis_index("sensor")
    x = lax.rem(me, 2)
    y = lax.rem(me // 2, 2)
    z = me // 4
    plane = 4
    other_chip = me + 1 - 2 * x
    y_chip = me + 2 - 4 * y
    other_core = 1 - core
    z_mate = z + 1 - 2 * lax.rem(z, 2)
    half = steps // 2
    rest = half + 1 - LANES
    rows = points * GROUP
    count = groups * GROUP
    pieces = groups // PIECE
    span = PIECE * 2 * GROUP

    barrier = pltpu.get_barrier_semaphore()

    @pl.loop(1, n)
    def _(step):
        pl.semaphore_signal(barrier, inc=1, device_id=(lax.rem(me + step, n), core), device_id_type=MESH)

    pl.semaphore_signal(barrier, inc=1, device_id=(me, other_core), device_id_type=MESH)
    pl.semaphore_signal(barrier, inc=1, device_id=(other_chip, other_core), device_id_type=MESH)

    def raw_copy(piece):
        begin = piece * span
        size = min(span, freqs - begin)
        return pltpu.make_async_copy(
            spectra_ref.at[:, pl.ds(begin, size)], raw.at[:, pl.ds(begin, size)], raw_sem.at[piece]
        )

    data_copy = pltpu.make_async_copy(data_ref, series, load_sem.at[0])
    forward_copy = pltpu.make_async_copy(forward_ref.at[core], table, load_sem.at[1])
    backward_copy = pltpu.make_async_copy(
        backward_ref.at[core], inverse.at[:, :, pl.ds(0, backward_ref.shape[3])], load_sem.at[2]
    )
    raw_copy(0).start()
    data_copy.start()
    for piece in range(1, pieces):
        raw_copy(piece).start()
    forward_copy.start()
    backward_copy.start()

    raw[:, freqs:] = jnp.zeros((2, raw.shape[1] - freqs) + tuple(raw.shape[2:]), jnp.float32)
    pad = inverse.shape[2] - backward_ref.shape[3]
    inverse[:, :, inverse.shape[2] - pad :, :] = jnp.zeros((2, 2, pad, wide), jnp.bfloat16)
    own_val[count:, :] = jnp.zeros((own_val.shape[0] - count, LANES), jnp.float32)

    strip = 64

    @pl.loop(0, fold.shape[1] // strip)
    def _(part):
        begin = pl.multiple_of(part * strip, strip)
        time = lax.broadcasted_iota(jnp.int32, (strip, 4 * LANES), 0) + begin
        for side in range(2):
            direct = jnp.where(time == maps_ref[3 * side : 3 * side + 1, :], 1.0, 0.0)
            sign = maps_ref[3 * side + 2 : 3 * side + 3, :].astype(jnp.float32)
            mirror = jnp.where(time == maps_ref[3 * side + 1 : 3 * side + 2, :], sign, 0.0)
            fold[side, pl.ds(begin, strip), :] = (direct + mirror).astype(jnp.bfloat16)

    upper = lax.broadcasted_iota(jnp.int32, (8, LANES), 0) < points
    stripe = lax.broadcasted_iota(jnp.int32, (8, LANES), 1) // local % 2 == 0

    def sort_piece(piece):
        @pl.loop(0, 2)
        def _(part):
            @pl.loop(piece * PIECE, (piece + 1) * PIECE)
            def _(group):
                for side in range(2):
                    for duo in range(GROUP // 2):
                        begin = group * 2 * GROUP + side * GROUP + 2 * duo
                        first = raw[part, begin]
                        second = raw[part, begin + 1]
                        low = jnp.where(upper, first, pltpu.roll(second, points, 0))
                        high = jnp.where(upper, pltpu.roll(first, points, 0), second)
                        packed[0, part, group, side, duo] = jnp.where(stripe, low, pltpu.roll(high, local, 1))
                        packed[1, part, group, side, duo] = jnp.where(stripe, pltpu.roll(high, LANES - local, 1), low)

    def k_copy(piece, target):
        begin = piece * PIECE
        rel = core if target == 0 else other_core
        return pltpu.make_async_remote_copy(
            src_ref=packed.at[1 - x, :, pl.ds(begin, PIECE), target],
            dst_ref=kbuf.at[1 + rel, :, pl.ds(begin, PIECE)],
            send_sem=k_send.at[piece, target], recv_sem=k_recv.at[piece, 1 + rel],
            device_id=(other_chip, target), device_id_type=MESH,
        )

    def k_keep(piece):
        begin = piece * PIECE
        return pltpu.make_async_remote_copy(
            src_ref=packed.at[x, :, pl.ds(begin, PIECE), other_core],
            dst_ref=kbuf.at[0, :, pl.ds(begin, PIECE)],
            send_sem=k_send.at[piece, 2], recv_sem=k_recv.at[piece, 0],
            device_id=(me, other_core), device_id_type=MESH,
        )

    def k_arrival(piece, slot):
        begin = piece * PIECE
        return pltpu.make_async_remote_copy(
            src_ref=packed.at[0, :, pl.ds(begin, PIECE), 0],
            dst_ref=kbuf.at[slot, :, pl.ds(begin, PIECE)],
            send_sem=k_send.at[piece, 2], recv_sem=k_recv.at[piece, slot],
            device_id=(me, other_core), device_id_type=MESH,
        )

    def send_piece(piece):
        for target in range(2):
            k_copy(piece, target).start()
        k_keep(piece).start()

    raw_copy(0).wait()
    sort_piece(0)
    pl.semaphore_wait(barrier, n + 1)
    send_piece(0)

    def slot(line, row, column):
        return line * plane + row * 2 + column

    def place(line, row):
        upper_line = line // 2
        return lax.rem(line, 2) * plane + row * 2 + upper_line + x - 2 * upper_line * x

    def block(chunk, line, row, rel=0):
        position = rel * (n // 2) + place(line, row)
        return gathered.at[chunk, pl.ds(pl.multiple_of(position * local, local), local), :]

    data_copy.wait()
    plain = (((1,), (0,)), ((), ()))
    folded = []
    for side in range(2):
        values = jnp.concatenate([series[2 * chunk + side] for chunk in range(CHUNKS)], axis=0)
        high = values.astype(jnp.bfloat16)
        left = values - high.astype(jnp.float32)
        middle = left.astype(jnp.bfloat16)
        low = (left - middle.astype(jnp.float32)).astype(jnp.bfloat16)
        result = lax.dot_general(
            jnp.concatenate([high, middle, low], axis=0), fold[side, :steps, :], plain,
            preferred_element_type=jnp.float32,
        )
        size = CHUNKS * local
        folded.append(result[:size] + (result[size : 2 * size] + result[2 * size :]))
    own_row = pl.ds(pl.multiple_of(place(z, y) * local, local), local)
    for chunk in range(CHUNKS):
        even = folded[0][chunk * local : (chunk + 1) * local]
        odd = folded[1][chunk * local : (chunk + 1) * local]
        gathered[chunk, own_row, 0 : 2 * LANES] = even[:, : 2 * LANES]
        gathered[chunk, own_row, 2 * LANES : 4 * LANES] = odd[:, : 2 * LANES]
        gathered[chunk, own_row, 4 * LANES : 5 * LANES] = (
            even[:, 2 * LANES : 3 * LANES] + odd[:, 2 * LANES : 3 * LANES]
        )
        gathered[chunk, own_row, 5 * LANES : 6 * LANES] = even[:, 3 * LANES :]
        gathered[chunk, own_row, 6 * LANES :] = odd[:, 3 * LANES :]

    def send(source, target, send_sem, recv_sem):
        return pltpu.make_async_remote_copy(
            src_ref=source, dst_ref=source, send_sem=send_sem, recv_sem=recv_sem,
            device_id=target, device_id_type=MESH,
        )

    def line_copy(chunk, step, way):
        source = jnp.clip(z - way * step, 0, lines - 1)
        target = jnp.clip(z + way, 0, lines - 1)
        index = step if way > 0 else lines + step
        return send(
            block(chunk, source, y), (slot(target, y, x), core), z_send.at[chunk, index], z_recv.at[chunk, index]
        )

    def line_arrival(chunk, step, way):
        source = jnp.clip(z - way * (step + 1), 0, lines - 1)
        target = jnp.clip(z + way, 0, lines - 1)
        index = step if way > 0 else lines + step
        return source, send(
            block(chunk, source, y), (slot(target, y, x), core), z_send.at[chunk, index], z_recv.at[chunk, index]
        )

    def sends(step, way):
        inside = z + 1 < lines if way > 0 else z > 0
        begun = z >= step if way > 0 else z + step < lines
        return jnp.logical_and(inside, begun)

    def receives(step, way):
        return z >= step + 1 if way > 0 else z + step + 1 < lines

    def y_copy(chunk, line):
        return send(block(chunk, line, y), (y_chip, core), y_send.at[chunk, line], y_recv.at[chunk, line])

    def y_arrival(chunk, line):
        return send(block(chunk, line, 1 - y), (y_chip, core), y_send.at[chunk, line], y_recv.at[chunk, line])

    def turn_copy(chunk):
        return send(block(chunk, z, 1 - y), (slot(z_mate, y, x), core), w_send.at[chunk], w_recv.at[chunk])

    def turn_arrival(chunk):
        return send(block(chunk, z_mate, 1 - y), (slot(z_mate, y, x), core), w_send.at[chunk], w_recv.at[chunk])

    def turns(chunk):
        return lax.rem(chunk, 2) == 0

    def by_row(chunk, line):
        return jnp.logical_not(jnp.logical_and(turns(chunk), line == z_mate))

    def core_copy(chunk, row, line):
        index = row * lines + line
        return pltpu.make_async_remote_copy(
            src_ref=block(chunk, line, row), dst_ref=block(chunk, line, row, 1),
            send_sem=c_send.at[chunk, index], recv_sem=c_recv.at[chunk, index],
            device_id=(me, other_core), device_id_type=MESH,
        )

    def start_lines(chunk):
        for way in (1, -1):

            @pl.when(sends(0, way))
            def _():
                line_copy(chunk, 0, way).start()

        y_copy(chunk, z).start()
        core_copy(chunk, y, z).start()

    def from_lines(chunk, step):
        for way in (1, -1):

            @pl.when(receives(step, way))
            def _():
                source, arrival = line_arrival(chunk, step, way)
                arrival.wait_recv()
                if step + 1 < lines - 1:

                    @pl.when(sends(step + 1, way))
                    def _():
                        line_copy(chunk, step + 1, way).start()

                @pl.when(by_row(chunk, source))
                def _():
                    y_copy(chunk, source).start()

                core_copy(chunk, y, source).start()

    def from_mate(chunk):
        y_arrival(chunk, z).wait_recv()

        @pl.when(turns(chunk))
        def _():
            turn_copy(chunk).start()

        core_copy(chunk, 1 - y, z).start()

    def from_row(chunk):
        for step in range(1, lines):
            line = lax.rem(z + step, lines)

            @pl.when(by_row(chunk, line))
            def _():
                y_arrival(chunk, line).wait_recv()

            @pl.when(jnp.logical_not(by_row(chunk, line)))
            def _():
                turn_arrival(chunk).wait_recv()

            core_copy(chunk, 1 - y, line).start()

    def from_core(chunk):
        for line in range(lines):
            for row in range(2):
                core_copy(chunk, row, line).wait_recv()

    lane_index = lax.broadcasted_iota(jnp.int32, (gathered.shape[1], LANES), 1)

    def transform(chunk):
        def lanes(index):
            return gathered[chunk, :, index * LANES : (index + 1) * LANES]

        for which in range(4):
            odd = which // 2
            position = which % 2
            if which < 2:
                tail = lanes(4 + which)
            elif which == 2:
                tail = lanes(6)
            else:
                tail = jnp.where(lane_index >= rest, lanes(4), lanes(6))
            right = split(jnp.concatenate([lanes(which), tail], axis=1))
            left = jnp.concatenate([table[position], table[2 + which]], axis=1)
            result = split_product(left, count, right)
            for lane in range(2):
                spectrum[lane, pl.ds(position * vectors + 2 * chunk + odd, count, stride=2 * vectors), :] = result[
                    :, lane * LANES : (lane + 1) * LANES
                ]

    pl.loop(0, CHUNKS)(start_lines)

    for piece in range(1, pieces):
        raw_copy(piece).wait()
        sort_piece(piece)
        send_piece(piece)

    forward_copy.wait()
    backward_copy.wait()

    def finish(chunk):
        from_core(chunk)
        transform(chunk)

    stages = [
        (functools.partial(from_lines, step=0), 0), (from_mate, 0),
        (functools.partial(from_lines, step=1), 1), (functools.partial(from_lines, step=2), 2),
        (from_row, 3), (finish, 4),
    ]

    @pl.loop(0, CHUNKS + 4)
    def _(turn):
        for stage, age in stages:
            chunk = turn - age

            @pl.when(jnp.logical_and(chunk >= 0, chunk < CHUNKS))
            def _():
                stage(chunk)

    columns = GROUP * 2 * vectors
    row_freq = lax.broadcasted_iota(jnp.int32, (4 * rows, columns), 0) // points % GROUP
    col_freq = lax.broadcasted_iota(jnp.int32, (4 * rows, columns), 1) // (2 * vectors)
    own = row_freq == col_freq
    lane = lax.broadcasted_iota(jnp.int32, (2 * rows, LANES), 1)
    row = lax.broadcasted_iota(jnp.int32, (2 * rows, LANES), 0) // points % 2
    sign = jnp.where((lane % (2 * vectors) < vectors) == (row == 0), 1.0, -1.0)
    step_rows = PIECE * GROUP
    owner_lane = lax.broadcasted_iota(jnp.int32, (step_rows, LANES), 1) // (2 * vectors)

    def value_copy(piece):
        place_rows = pl.ds(pl.multiple_of(piece * step_rows, GROUP), step_rows)
        return pltpu.make_async_remote_copy(
            src_ref=send_val.at[place_rows], dst_ref=recv_val.at[place_rows],
            send_sem=v_send.at[piece], recv_sem=v_recv.at[piece],
            device_id=(other_chip, core), device_id_type=MESH,
        )

    @pl.loop(0, pieces)
    def _(piece):
        for arrival in range(3):
            k_arrival(piece, arrival).wait_recv()
        for step in range(PIECE):
            group = piece * PIECE + step
            begin = pl.multiple_of(group * columns, columns)
            right = split(
                jnp.concatenate([spectrum[0, pl.ds(begin, columns), :], spectrum[1, pl.ds(begin, columns), :]], axis=1)
            )
            parts = []
            for part in range(2):
                for near, far in (
                    (packed[x, part, group, core], kbuf[0, part, group]), (kbuf[1, part, group], kbuf[2, part, group]),
                ):
                    parts.append(jnp.concatenate([near.reshape(rows, LANES), far.reshape(rows, LANES)], axis=1))
            left = jnp.concatenate(parts, axis=0)
            found = jnp.where(own, product(split(left), right, NT_DIMS), 0.0)
            width = columns
            while width > LANES:
                width //= 2
                found = found[:, :width] + found[:, width:]
            hop = LANES // 2
            while hop >= 2 * vectors:
                found = found + pltpu.roll(found, hop, 1)
                hop //= 2
            value = found[: 2 * rows] + sign * pltpu.roll(found[2 * rows :], vectors, 1)
            for owner in range(2):
                product_s[owner, pl.ds(pl.multiple_of(group * rows, rows), rows), :] = value[
                    owner * rows : (owner + 1) * rows
                ]
        begin = piece * PIECE * rows
        for owner, target in ((1, send_val), (0, own_val)):
            merged = jnp.zeros((step_rows, LANES), jnp.float32)
            for point in range(points):
                merged = jnp.where(
                    owner_lane == point, product_s[owner, pl.ds(begin + point, step_rows, stride=points), :], merged
                )
            target[pl.ds(pl.multiple_of(piece * step_rows, GROUP), step_rows), :] = merged
        value_copy(piece).start()

    @pl.loop(0, pieces)
    def _(piece):
        value_copy(piece).wait_recv()

    own_val[:count, :] = own_val[:count, :] + recv_val[...]
    turned = own_val[...].T
    by_position = []
    for position in range(2):
        by_position.append(jnp.concatenate(
            [turned[(2 * point + position) * vectors : (2 * point + position + 1) * vectors] for point in range(points)],
            axis=0,
        ))
    left = split(jnp.concatenate(by_position, axis=1))
    deep = 2 * inverse.shape[2]
    partial[...] = product(left, (inverse[0].reshape(deep, wide), inverse[1].reshape(deep, wide)), plain)

    field_copy = pltpu.make_async_remote_copy(
        src_ref=partial, dst_ref=pair, send_sem=f_send.at[0], recv_sem=f_recv.at[0],
        device_id=(me, other_core), device_id_type=MESH,
    )
    field_copy.start()
    field_copy.wait_recv()

    total = partial[...] + pair[...]
    energy = total * total
    summed = energy[:vectors]
    for point in range(1, points):
        summed = summed + energy[point * vectors : (point + 1) * vectors]
    diagonal = lax.broadcasted_iota(jnp.int32, (vectors, LANES), 0) == lax.broadcasted_iota(
        jnp.int32, (vectors, LANES), 1
    )
    column = jnp.sum(summed, axis=1, keepdims=True)
    flat = jnp.sum(jnp.where(diagonal, column, 0.0), axis=0, keepdims=True)
    flat = jnp.broadcast_to(flat, (8, LANES))
    square[...] = flat
    squares[me] = flat

    def square_copy(step):
        return pltpu.make_async_remote_copy(
            src_ref=square, dst_ref=squares.at[me], send_sem=r_send.at[step], recv_sem=r_recv.at[step],
            device_id=(lax.rem(me + step, n), core), device_id_type=MESH,
        )

    def square_arrival(step):
        return pltpu.make_async_remote_copy(
            src_ref=square, dst_ref=squares.at[lax.rem(me + n - step, n)],
            send_sem=r_send.at[step], recv_sem=r_recv.at[step],
            device_id=(lax.rem(me + step, n), core), device_id_type=MESH,
        )

    @pl.loop(1, n)
    def _(step):
        square_copy(step).start()

    @pl.loop(0, CHUNKS)
    def _(chunk):
        for step in range(lines - 1):
            for way in (1, -1):

                @pl.when(sends(step, way))
                def _():
                    line_copy(chunk, step, way).wait_send()

        for line in range(lines):

            @pl.when(by_row(chunk, line))
            def _():
                y_copy(chunk, line).wait_send()

            for row in range(2):
                core_copy(chunk, row, line).wait_send()

        @pl.when(turns(chunk))
        def _():
            turn_copy(chunk).wait_send()

    for piece in range(pieces):
        for target in range(2):
            k_copy(piece, target).wait_send()
        k_keep(piece).wait_send()
        value_copy(piece).wait_send()
    field_copy.wait_send()

    @pl.loop(1, n)
    def _(step):
        square_arrival(step).wait()

    energy_all = squares[0]
    for device in range(1, n):
        energy_all = energy_all + squares[device]
    scale = jnp.sqrt(energy_all / (points * n * steps) + 1e-06)
    rms_ref[...] = scale
    spread = jnp.broadcast_to(scale[:1], (vectors, LANES))
    divisor = jnp.sum(jnp.where(diagonal, spread, 0.0), axis=1, keepdims=True)
    for point in range(points):
        out_ref[point] = total[point * vectors : (point + 1) * vectors, :steps] / divisor


def paired_body(data, spectra):
    n = lax.axis_size("param")
    vectors, local, steps = data.shape
    sensors, points, freqs = spectra.shape[1:]
    wide = -(-steps // LANES) * LANES
    groups = -(-freqs // (2 * GROUP))
    count = groups * GROUP
    rows_pad = -(-count // 16) * 16
    deep = -(-count // LANES) * LANES
    pieces = groups // PIECE
    lines = n // 4
    forward, backward = paired_tables(steps, freqs, groups, rows_pad, wide)
    maps = fold_maps(steps)

    turned = jnp.transpose(spectra, (0, 3, 2, 1)).reshape(2, freqs, points, 2, LANES)
    turned = jnp.transpose(turned, (0, 1, 3, 2, 4)).reshape(2, freqs, 2 * points, LANES)

    hbm = pl.BlockSpec(memory_space=pl.ANY)
    vmem = pl.BlockSpec(memory_space=pltpu.VMEM)
    dma = pltpu.SemaphoreType.DMA
    f32, bf16 = jnp.float32, jnp.bfloat16
    fields, scale = pl.pallas_call(
        functools.partial(kernel, n, lines, vectors, local, steps, points, freqs, groups, wide),
        out_shape=(
            jax.ShapeDtypeStruct((points, vectors, steps), f32),
            jax.ShapeDtypeStruct((8, LANES), f32),
        ),
        in_specs=[hbm, hbm, hbm, hbm, vmem],
        out_specs=(vmem, vmem),
        scratch_shapes=[
            pltpu.VMEM((vectors, local, steps), f32),
            pltpu.VMEM((2, wide, 4 * LANES), bf16),
            pltpu.VMEM((2, 2 * count, 2 * points, LANES), f32),
            pltpu.VMEM((2, 2, groups, 2, GROUP // 2, 2 * points, LANES), f32),
            pltpu.VMEM((3, 2, groups, GROUP // 2, 2 * points, LANES), f32),
            pltpu.VMEM((CHUNKS, sensors, 7 * LANES), f32),
            pltpu.VMEM((6, 2 * rows_pad, LANES), bf16),
            pltpu.VMEM((2, 2, deep, wide), bf16),
            pltpu.VMEM((2, count * 2 * vectors, LANES), f32),
            pltpu.VMEM((2, count * points, LANES), f32),
            pltpu.VMEM((deep, LANES), f32),
            pltpu.VMEM((count, LANES), f32),
            pltpu.VMEM((count, LANES), f32),
            pltpu.VMEM((points * vectors, wide), f32),
            pltpu.VMEM((points * vectors, wide), f32),
            pltpu.VMEM((8, LANES), f32),
            pltpu.VMEM((n, 8, LANES), f32),
            dma((3,)),
            dma((pieces,)),
            dma((pieces, 3)), dma((pieces, 3)),
            dma((CHUNKS, 2 * lines)), dma((CHUNKS, 2 * lines)),
            dma((CHUNKS, lines)), dma((CHUNKS, lines)),
            dma((CHUNKS, 2 * lines)), dma((CHUNKS, 2 * lines)),
            dma((CHUNKS,)), dma((CHUNKS,)),
            dma((pieces,)), dma((pieces,)),
            dma((1,)), dma((1,)),
            dma((n,)), dma((n,)),
        ],
        compiler_params=pltpu.CompilerParams(
            collective_id=0, has_side_effects=True, vmem_limit_bytes=60 * 1024 * 1024
        ),
    )(data, turned, jnp.asarray(forward), jnp.asarray(backward), jnp.asarray(maps))
    return (jnp.transpose(fields, (1, 0, 2)), scale[0, :vectors])


def solution(mesh):
    in_specs = (P(None, ("sensor", "param"), None), P(None, "sensor", "param", None))
    out_specs = (P(None, "param", None), P())
    n = mesh.shape["param"]
    pair = mesh.shape["sensor"] == 2 and n == 16

    def body(data, spectra):
        vectors, local, _ = data.shape
        sensors, points = spectra.shape[1:3]
        fits = local * n * 2 == 2 * sensors and sensors == 2 * LANES and vectors == 2 * CHUNKS
        fits = fits and points * 2 * vectors == LANES and folded_layout_fits(data.shape[2])
        return (paired_body if pair and fits else general_body)(data, spectra)

    return jax.shard_map(body, mesh=mesh, in_specs=in_specs, out_specs=out_specs, check_vma=False)
```

```python
import functools
import math

import jax
import jax.numpy as jnp
import numpy as np
from jax import lax
from jax.experimental import pallas as pl
from jax.experimental.pallas import tpu as pltpu
from jax.sharding import PartitionSpec as P

MESH = pl.DeviceIdType.MESH
LANES = 128
GROUP = 8
CHUNKS = 8
PIECE = 3
BATCHES = 3


def spectral_tables(steps):
    length = 2 * steps
    freqs = steps + 1
    times = lax.broadcasted_iota(jnp.int32, (steps, freqs), 0)
    bins = lax.broadcasted_iota(jnp.int32, (steps, freqs), 1)
    phase = 2.0 * math.pi / length * (times * bins % length).astype(jnp.float32)
    forward = jnp.concatenate([jnp.cos(phase), -jnp.sin(phase)], axis=1)
    weight = jnp.where((bins == 0) | (bins == steps), 1.0, 2.0) / length
    backward = jnp.concatenate([(weight * jnp.cos(phase)).T, (-weight * jnp.sin(phase)).T], axis=0)
    return (forward, backward)


def to_spectrum(series, forward):
    vectors, sensors, steps = series.shape
    flat = jnp.dot(
        series.reshape(vectors * sensors, steps),
        forward,
        precision=lax.Precision.HIGHEST,
        preferred_element_type=jnp.float32,
    )
    return flat.reshape(vectors, sensors, forward.shape[1])


def contract(kernel, spectrum):
    return jnp.einsum(
        "spf,rsf->rpf",
        kernel,
        spectrum,
        precision=lax.Precision.HIGHEST,
        preferred_element_type=jnp.float32,
    )


def general_body(data, spectra):
    steps = data.shape[2]
    freqs = steps + 1
    forward, backward = spectral_tables(steps)
    whole = to_spectrum(lax.all_gather(data, "param", axis=1, tiled=True), forward)
    real_part = whole[..., :freqs]
    imag_part = whole[..., freqs:]
    kernel_re = spectra[0]
    kernel_im = spectra[1]
    out_re = contract(kernel_re, real_part) + contract(kernel_im, imag_part)
    out_im = contract(kernel_re, imag_part) - contract(kernel_im, real_part)
    vectors, points = (out_re.shape[0], out_re.shape[1])
    stacked = jnp.concatenate([out_re, out_im], axis=2).reshape(vectors * points, 2 * freqs)
    partial_field = jnp.dot(
        stacked, backward, precision=lax.Precision.HIGHEST, preferred_element_type=jnp.float32
    ).reshape(vectors, points, steps)
    count = points * lax.axis_size("param") * steps
    share = lax.psum_scatter(partial_field, "sensor", scatter_dimension=0, tiled=True)
    squares = lax.psum(jnp.sum(share * share, axis=(1, 2)), "param")
    scale = jnp.sqrt(squares / count + 1e-06)
    normalized = share / scale[:, None, None]
    gradient, rms_all = (
        lax.all_gather(normalized, "sensor", axis=0, tiled=True),
        lax.all_gather(scale, "sensor", axis=0, tiled=True),
    )
    return (gradient, rms_all)


def split(value):
    high = value.astype(jnp.bfloat16)
    return high, (value - high.astype(jnp.float32)).astype(jnp.bfloat16)


NT_DIMS = (((1,), (1,)), ((), ()))


def product(left, right, dims):
    dot = functools.partial(lax.dot_general, dimension_numbers=dims, preferred_element_type=jnp.float32)
    size = left[0].shape[0]
    both = dot(jnp.concatenate(left, axis=0), right[0])
    return both[:size] + (both[size:] + dot(left[0], right[1]))


def split_product(table, rows, right):
    dot = functools.partial(lax.dot_general, dimension_numbers=NT_DIMS, preferred_element_type=jnp.float32)
    half = table.shape[0] // 2
    both = dot(table, right[0])
    return both[:rows] + (both[half : half + rows] + dot(table[:half], right[1])[:rows])


def folded_layout_fits(steps):
    half = steps // 2
    rest = half + 1 - LANES
    groups = -(-(steps + 1) // (2 * GROUP))
    fits = steps % 2 == 0 and 0 < rest < LANES and half - LANES - (LANES - rest) <= LANES - rest
    return fits and groups % (PIECE * BATCHES) == 0


def frequency_order(freqs, groups):
    bins = np.arange(groups * 2 * GROUP).reshape(groups, 2, GROUP)
    return [bins[:, core].reshape(-1) for core in range(2)]


def lane_times(steps):
    half = steps // 2
    rest = half + 1 - LANES
    room = LANES - rest
    lane = np.arange(LANES)
    first = np.where(lane < rest, LANES + lane, -1)
    first_odd = np.where(lane < rest - 1, LANES + lane, -1)
    second = np.where(lane >= room, LANES + lane - room, -1)
    tail_a = np.where(lane >= rest, LANES + lane - rest, -1)
    tail_b = np.where(lane < rest - 1 - room, LANES + room + lane, -1)
    return lane, first, first_odd, second, tail_a, tail_b


def fold_maps(steps):
    lane, first, first_odd, second, tail_a, tail_b = lane_times(steps)
    shared = np.where(second >= 0, second, tail_b)
    even = np.concatenate([lane, lane, first, first_odd])
    odd = np.concatenate([lane, lane, tail_a, shared])
    ones = np.ones(LANES, np.int64)
    even_sign = np.concatenate([ones, -ones, ones, -ones])
    odd_sign = np.concatenate([ones, -ones, -ones, np.where(second >= 0, 1, -1)])
    maps = np.full((8, 4 * LANES), -1, np.int32)
    for index, (time, sign) in enumerate(((even, even_sign), (odd, odd_sign))):
        mirror = np.where((time > 0) & (2 * time != steps), steps - time, -1)
        maps[3 * index] = time
        maps[3 * index + 1] = np.where(time < 0, -1, mirror)
        maps[3 * index + 2] = sign
    return maps


def halves(values):
    high = values.astype(jnp.bfloat16)
    return high, (values - high.astype(np.float32)).astype(jnp.bfloat16)


def paired_tables(steps, freqs, groups, rows_pad, wide):
    half = steps // 2
    lane, first, first_odd, second, tail_a, tail_b = lane_times(steps)
    tail = np.where(tail_a >= 0, tail_a, tail_b)
    forward, backward = [], []
    for bins in frequency_order(freqs, groups):
        count = bins.shape[0]
        known = (bins < freqs)[:, None]
        even = (bins % 2 == 0)[:, None]
        angle = bins[:, None] * np.arange(steps)[None, :] % (2 * steps)
        phase = np.pi / steps * angle
        sine = np.where(angle % steps == 0, 0.0, np.sin(phase))
        cosine = np.cos(phase)
        symmetric = np.where(known, np.where(even, cosine, -sine), 0.0)
        other = np.where(known, np.where(even, -sine, cosine), 0.0)
        blocks = []
        for table, times in (
            (symmetric, lane), (other, lane), (symmetric, first), (other, first_odd), (symmetric, second), (other, tail),
        ):
            limit = half if table is symmetric else half - 1
            inside = (times >= 0) & (times <= limit)
            value = np.where(inside[None, :], table[:, np.clip(times, 0, limit)], 0.0).astype(np.float32)
            block = np.zeros((2, rows_pad, LANES), jnp.bfloat16)
            block[0, :count], block[1, :count] = halves(value)
            blocks.append(block.reshape(2 * rows_pad, LANES))
        forward.append(np.stack(blocks))
        weight = np.where((bins == 0) | (bins == steps), 0.5, 1.0)[:, None] / steps
        inverse = np.zeros((2, 2, rows_pad, wide), jnp.bfloat16)
        for position, table in enumerate((symmetric, other)):
            value = (table * weight).astype(np.float32)
            inverse[0, position, :count, :steps], inverse[1, position, :count, :steps] = halves(value)
        backward.append(inverse)
    return np.stack(forward), np.stack(backward)


def kernel(
    n, lines, vectors, local, steps, points, freqs, groups, wide,
    data_ref, spectra_ref, forward_ref, backward_ref, maps_ref,
    out_ref, rms_ref,
    series, fold, raw, packed, kbuf, gathered, table, inverse, spectrum, product_s, own_val, send_val, recv_val,
    partial, pair, square, squares,
    load_sem, raw_sem, k_send, k_recv, z_send, z_recv, y_send, y_recv, c_send, c_recv, w_send, w_recv,
    v_send, v_recv, f_send, f_recv, r_send, r_recv,
):
    me = lax.axis_index("param")
    core = lax.axis_index("sensor")
    x = lax.rem(me, 2)
    y = lax.rem(me // 2, 2)
    z = me // 4
    plane = 4
    other_chip = me + 1 - 2 * x
    y_chip = me + 2 - 4 * y
    other_core = 1 - core
    z_mate = z + 1 - 2 * lax.rem(z, 2)
    half = steps // 2
    rest = half + 1 - LANES
    rows = points * GROUP
    count = groups * GROUP
    pieces = groups // PIECE
    span = PIECE * 2 * GROUP

    barrier = pltpu.get_barrier_semaphore()

    for neighbour in ((other_chip, core), (other_chip, other_core), (y_chip, core), (me, other_core)):
        pl.semaphore_signal(barrier, inc=1, device_id=neighbour, device_id_type=MESH)

    @pl.when(z > 0)
    def _():
        pl.semaphore_signal(barrier, inc=1, device_id=(me - plane, core), device_id_type=MESH)

    @pl.when(z + 1 < lines)
    def _():
        pl.semaphore_signal(barrier, inc=1, device_id=(me + plane, core), device_id_type=MESH)

    def filled(piece, target):
        known = -(-(freqs - target * GROUP) // (2 * GROUP))
        return min(PIECE, known - piece * PIECE)

    def raw_copy(piece):
        begin = piece * span
        size = min(span, freqs - begin)
        return pltpu.make_async_copy(
            spectra_ref.at[:, pl.ds(begin, size)], raw.at[:, pl.ds(begin, size)], raw_sem.at[piece]
        )

    data_copy = pltpu.make_async_copy(data_ref, series, load_sem.at[0])
    forward_copy = pltpu.make_async_copy(forward_ref.at[core], table, load_sem.at[1])
    backward_copy = pltpu.make_async_copy(
        backward_ref.at[core], inverse.at[:, :, pl.ds(0, backward_ref.shape[3])], load_sem.at[2]
    )
    raw_copy(0).start()
    data_copy.start()
    for piece in range(1, pieces):
        raw_copy(piece).start()
    forward_copy.start()
    backward_copy.start()

    raw[:, freqs:] = jnp.zeros((2, raw.shape[1] - freqs) + tuple(raw.shape[2:]), jnp.float32)
    pad = inverse.shape[2] - backward_ref.shape[3]
    inverse[:, :, inverse.shape[2] - pad :, :] = jnp.zeros((2, 2, pad, wide), jnp.bfloat16)
    short = filled(pieces - 1, 1)
    if short < PIECE:

        @pl.when(core == 1)
        def _():
            begin = (pieces - 1) * PIECE + short
            for owner in range(1, 3):
                kbuf[owner, :, begin:] = jnp.zeros((2, PIECE - short) + tuple(kbuf.shape[3:]), jnp.float32)

    own_val[count:, :] = jnp.zeros((own_val.shape[0] - count, LANES), jnp.float32)

    strip = 64

    @pl.loop(0, fold.shape[1] // strip)
    def _(part):
        begin = pl.multiple_of(part * strip, strip)
        time = lax.broadcasted_iota(jnp.int32, (strip, 4 * LANES), 0) + begin
        for side in range(2):
            direct = jnp.where(time == maps_ref[3 * side : 3 * side + 1, :], 1.0, 0.0)
            sign = maps_ref[3 * side + 2 : 3 * side + 3, :].astype(jnp.float32)
            mirror = jnp.where(time == maps_ref[3 * side + 1 : 3 * side + 2, :], sign, 0.0)
            fold[side, pl.ds(begin, strip), :] = (direct + mirror).astype(jnp.bfloat16)

    upper = lax.broadcasted_iota(jnp.int32, (8, LANES), 0) < points
    stripe = lax.broadcasted_iota(jnp.int32, (8, LANES), 1) // local % 2 == 0

    def sort_piece(piece):
        @pl.loop(0, 2)
        def _(part):
            @pl.loop(piece * PIECE, (piece + 1) * PIECE)
            def _(group):
                for side in range(2):
                    for duo in range(GROUP // 2):
                        begin = group * 2 * GROUP + side * GROUP + 2 * duo
                        first = raw[part, begin]
                        second = raw[part, begin + 1]
                        low = jnp.where(upper, first, pltpu.roll(second, points, 0))
                        high = jnp.where(upper, pltpu.roll(first, points, 0), second)
                        packed[0, part, group, side, duo] = jnp.where(stripe, low, pltpu.roll(high, local, 1))
                        packed[1, part, group, side, duo] = jnp.where(stripe, pltpu.roll(high, LANES - local, 1), low)

    def k_copy(piece, target):
        begin = piece * PIECE
        size = filled(piece, target)
        rel = core if target == 0 else other_core
        return pltpu.make_async_remote_copy(
            src_ref=packed.at[1 - x, :, pl.ds(begin, size), target],
            dst_ref=kbuf.at[1 + rel, :, pl.ds(begin, size)],
            send_sem=k_send.at[piece, target], recv_sem=k_recv.at[piece, 1 + rel],
            device_id=(other_chip, target), device_id_type=MESH,
        )

    def k_keep(piece):
        begin = piece * PIECE
        return pltpu.make_async_remote_copy(
            src_ref=packed.at[x, :, pl.ds(begin, PIECE), other_core],
            dst_ref=kbuf.at[0, :, pl.ds(begin, PIECE)],
            send_sem=k_send.at[piece, 2], recv_sem=k_recv.at[piece, 0],
            device_id=(me, other_core), device_id_type=MESH,
        )

    def k_arrival(piece, slot, size):
        begin = piece * PIECE
        return pltpu.make_async_remote_copy(
            src_ref=packed.at[0, :, pl.ds(begin, size), 0],
            dst_ref=kbuf.at[slot, :, pl.ds(begin, size)],
            send_sem=k_send.at[piece, 2], recv_sem=k_recv.at[piece, slot],
            device_id=(me, other_core), device_id_type=MESH,
        )

    def wait_piece(piece):
        k_arrival(piece, 0, PIECE).wait_recv()
        for target in range(2):

            @pl.when(core == target)
            def _():
                for arrival in range(1, 3):
                    k_arrival(piece, arrival, filled(piece, target)).wait_recv()

    def send_piece(piece):
        for target in range(2):
            k_copy(piece, target).start()
        k_keep(piece).start()

    raw_copy(0).wait()
    sort_piece(0)
    pl.semaphore_wait(barrier, 4 + jnp.minimum(z, 1) + jnp.minimum(lines - 1 - z, 1))
    send_piece(0)

    def slot(line, row, column):
        return line * plane + row * 2 + column

    def place(line, row):
        upper_line = line // 2
        return lax.rem(line, 2) * plane + row * 2 + upper_line + x - 2 * upper_line * x

    def block(chunk, line, row, rel=0):
        position = rel * (n // 2) + place(line, row)
        return gathered.at[chunk, pl.ds(pl.multiple_of(position * local, local), local), :]

    data_copy.wait()
    plain = (((1,), (0,)), ((), ()))
    folded = []
    for side in range(2):
        values = jnp.concatenate([series[2 * chunk + side] for chunk in range(CHUNKS)], axis=0)
        high = values.astype(jnp.bfloat16)
        left = values - high.astype(jnp.float32)
        middle = left.astype(jnp.bfloat16)
        low = (left - middle.astype(jnp.float32)).astype(jnp.bfloat16)
        result = lax.dot_general(
            jnp.concatenate([high, middle, low], axis=0), fold[side, :steps, :], plain,
            preferred_element_type=jnp.float32,
        )
        size = CHUNKS * local
        folded.append(result[:size] + (result[size : 2 * size] + result[2 * size :]))
    own_row = pl.ds(pl.multiple_of(place(z, y) * local, local), local)
    for chunk in range(CHUNKS):
        even = folded[0][chunk * local : (chunk + 1) * local]
        odd = folded[1][chunk * local : (chunk + 1) * local]
        gathered[chunk, own_row, 0 : 2 * LANES] = even[:, : 2 * LANES]
        gathered[chunk, own_row, 2 * LANES : 4 * LANES] = odd[:, : 2 * LANES]
        gathered[chunk, own_row, 4 * LANES : 5 * LANES] = (
            even[:, 2 * LANES : 3 * LANES] + odd[:, 2 * LANES : 3 * LANES]
        )
        gathered[chunk, own_row, 5 * LANES : 6 * LANES] = even[:, 3 * LANES :]
        gathered[chunk, own_row, 6 * LANES :] = odd[:, 3 * LANES :]

    def send(source, target, send_sem, recv_sem):
        return pltpu.make_async_remote_copy(
            src_ref=source, dst_ref=source, send_sem=send_sem, recv_sem=recv_sem,
            device_id=target, device_id_type=MESH,
        )

    def line_copy(chunk, step, way):
        source = jnp.clip(z - way * step, 0, lines - 1)
        target = jnp.clip(z + way, 0, lines - 1)
        index = step if way > 0 else lines + step
        return send(
            block(chunk, source, y), (slot(target, y, x), core), z_send.at[chunk, index], z_recv.at[chunk, index]
        )

    def line_arrival(chunk, step, way):
        source = jnp.clip(z - way * (step + 1), 0, lines - 1)
        target = jnp.clip(z + way, 0, lines - 1)
        index = step if way > 0 else lines + step
        return source, send(
            block(chunk, source, y), (slot(target, y, x), core), z_send.at[chunk, index], z_recv.at[chunk, index]
        )

    def sends(step, way):
        inside = z + 1 < lines if way > 0 else z > 0
        begun = z >= step if way > 0 else z + step < lines
        return jnp.logical_and(inside, begun)

    def receives(step, way):
        return z >= step + 1 if way > 0 else z + step + 1 < lines

    def y_copy(chunk, line):
        return send(block(chunk, line, y), (y_chip, core), y_send.at[chunk, line], y_recv.at[chunk, line])

    def y_arrival(chunk, line):
        return send(block(chunk, line, 1 - y), (y_chip, core), y_send.at[chunk, line], y_recv.at[chunk, line])

    def turn_copy(chunk):
        return send(block(chunk, z, 1 - y), (slot(z_mate, y, x), core), w_send.at[chunk], w_recv.at[chunk])

    def turn_arrival(chunk):
        return send(block(chunk, z_mate, 1 - y), (slot(z_mate, y, x), core), w_send.at[chunk], w_recv.at[chunk])

    def turns(chunk):
        return chunk >= CHUNKS // 2

    def by_row(chunk, line):
        return jnp.logical_not(jnp.logical_and(turns(chunk), line == z_mate))

    def core_copy(chunk, row, line):
        index = row * lines + line
        return pltpu.make_async_remote_copy(
            src_ref=block(chunk, line, row), dst_ref=block(chunk, line, row, 1),
            send_sem=c_send.at[chunk, index], recv_sem=c_recv.at[chunk, index],
            device_id=(me, other_core), device_id_type=MESH,
        )

    def start_lines(chunk):
        for way in (1, -1):

            @pl.when(sends(0, way))
            def _():
                line_copy(chunk, 0, way).start()

        y_copy(chunk, z).start()
        core_copy(chunk, y, z).start()

    def from_lines(chunk, step):
        for way in (1, -1):

            @pl.when(receives(step, way))
            def _():
                source, arrival = line_arrival(chunk, step, way)
                arrival.wait_recv()
                if step + 1 < lines - 1:

                    @pl.when(sends(step + 1, way))
                    def _():
                        line_copy(chunk, step + 1, way).start()

                @pl.when(by_row(chunk, source))
                def _():
                    y_copy(chunk, source).start()

                core_copy(chunk, y, source).start()

    def from_mate(chunk):
        y_arrival(chunk, z).wait_recv()
        core_copy(chunk, 1 - y, z).start()

    def to_mate(chunk):
        @pl.when(turns(chunk))
        def _():
            turn_copy(chunk).start()

    def from_row(chunk):
        for step in range(1, lines):
            line = lax.rem(z + step, lines)

            @pl.when(by_row(chunk, line))
            def _():
                y_arrival(chunk, line).wait_recv()

            @pl.when(jnp.logical_not(by_row(chunk, line)))
            def _():
                turn_arrival(chunk).wait_recv()

            core_copy(chunk, 1 - y, line).start()

    def from_core(chunk):
        for line in range(lines):
            for row in range(2):
                core_copy(chunk, row, line).wait_recv()

    lane_index = lax.broadcasted_iota(jnp.int32, (gathered.shape[1], LANES), 1)

    def transform(chunk):
        def lanes(index):
            return gathered[chunk, :, index * LANES : (index + 1) * LANES]

        for which in range(4):
            odd = which // 2
            position = which % 2
            if which < 2:
                tail = lanes(4 + which)
            elif which == 2:
                tail = lanes(6)
            else:
                tail = jnp.where(lane_index >= rest, lanes(4), lanes(6))
            right = split(jnp.concatenate([lanes(which), tail], axis=1))
            left = jnp.concatenate([table[position], table[2 + which]], axis=1)
            result = split_product(left, count, right)
            for lane in range(2):
                spectrum[lane, pl.ds(position * vectors + 2 * chunk + odd, count, stride=2 * vectors), :] = result[
                    :, lane * LANES : (lane + 1) * LANES
                ]

    pl.loop(0, CHUNKS)(start_lines)

    for piece in range(1, pieces):
        raw_copy(piece).wait()
        sort_piece(piece)
        send_piece(piece)

    forward_copy.wait()
    backward_copy.wait()

    def finish(chunk):
        from_core(chunk)
        transform(chunk)

    stages = [
        (functools.partial(from_lines, step=0), 0), (from_mate, 0),
        (functools.partial(from_lines, step=1), 1), (functools.partial(from_lines, step=2), 2),
        (to_mate, 4), (from_row, 6), (finish, 7),
    ]

    @pl.loop(0, CHUNKS + 7)
    def _(turn):
        for stage, age in stages:
            chunk = turn - age

            @pl.when(jnp.logical_and(chunk >= 0, chunk < CHUNKS))
            def _():
                stage(chunk)

    columns = GROUP * 2 * vectors
    row_freq = lax.broadcasted_iota(jnp.int32, (4 * rows, columns), 0) // points % GROUP
    col_freq = lax.broadcasted_iota(jnp.int32, (4 * rows, columns), 1) // (2 * vectors)
    own = row_freq == col_freq
    lane = lax.broadcasted_iota(jnp.int32, (2 * rows, LANES), 1)
    row = lax.broadcasted_iota(jnp.int32, (2 * rows, LANES), 0) // points % 2
    sign = jnp.where((lane % (2 * vectors) < vectors) == (row == 0), 1.0, -1.0)
    batch = groups // BATCHES
    step_rows = batch * GROUP
    owner_lane = lax.broadcasted_iota(jnp.int32, (step_rows, LANES), 1) // (2 * vectors)

    def value_copy(turn):
        place_rows = pl.ds(pl.multiple_of(turn * step_rows, GROUP), step_rows)
        return pltpu.make_async_remote_copy(
            src_ref=send_val.at[place_rows], dst_ref=recv_val.at[place_rows],
            send_sem=v_send.at[turn], recv_sem=v_recv.at[turn],
            device_id=(other_chip, core), device_id_type=MESH,
        )

    @pl.loop(0, BATCHES)
    def _(turn):
        for which in range(BATCHES):

            @pl.when(turn == which)
            def _():
                for piece in range(which * batch // PIECE, (which + 1) * batch // PIECE):
                    wait_piece(piece)

        for step in range(batch):
            group = turn * batch + step
            begin = pl.multiple_of(group * columns, columns)
            right = split(
                jnp.concatenate([spectrum[0, pl.ds(begin, columns), :], spectrum[1, pl.ds(begin, columns), :]], axis=1)
            )
            parts = []
            for part in range(2):
                for near, far in (
                    (packed[x, part, group, core], kbuf[0, part, group]), (kbuf[1, part, group], kbuf[2, part, group]),
                ):
                    parts.append(jnp.concatenate([near.reshape(rows, LANES), far.reshape(rows, LANES)], axis=1))
            left = jnp.concatenate(parts, axis=0)
            found = jnp.where(own, product(split(left), right, NT_DIMS), 0.0)
            width = columns
            while width > LANES:
                width //= 2
                found = found[:, :width] + found[:, width:]
            hop = LANES // 2
            while hop >= 2 * vectors:
                found = found + pltpu.roll(found, hop, 1)
                hop //= 2
            value = found[: 2 * rows] + sign * pltpu.roll(found[2 * rows :], vectors, 1)
            for owner in range(2):
                product_s[owner, pl.ds(pl.multiple_of(group * rows, rows), rows), :] = value[
                    owner * rows : (owner + 1) * rows
                ]
        begin = turn * batch * rows
        for owner, target in ((1, send_val), (0, own_val)):
            merged = jnp.zeros((step_rows, LANES), jnp.float32)
            for point in range(points):
                merged = jnp.where(
                    owner_lane == point, product_s[owner, pl.ds(begin + point, step_rows, stride=points), :], merged
                )
            target[pl.ds(pl.multiple_of(turn * step_rows, GROUP), step_rows), :] = merged
        value_copy(turn).start()

    @pl.loop(0, BATCHES)
    def _(turn):
        value_copy(turn).wait_recv()

    own_val[:count, :] = own_val[:count, :] + recv_val[...]
    turned = own_val[...].T
    by_position = []
    for position in range(2):
        by_position.append(jnp.concatenate(
            [turned[(2 * point + position) * vectors : (2 * point + position + 1) * vectors] for point in range(points)],
            axis=0,
        ))
    left = split(jnp.concatenate(by_position, axis=1))
    deep = 2 * inverse.shape[2]
    partial[...] = product(left, (inverse[0].reshape(deep, wide), inverse[1].reshape(deep, wide)), plain)

    field_copy = pltpu.make_async_remote_copy(
        src_ref=partial, dst_ref=pair, send_sem=f_send.at[0], recv_sem=f_recv.at[0],
        device_id=(me, other_core), device_id_type=MESH,
    )
    field_copy.start()
    field_copy.wait_recv()

    total = partial[...] + pair[...]
    energy = total * total
    summed = energy[:vectors]
    for point in range(1, points):
        summed = summed + energy[point * vectors : (point + 1) * vectors]
    diagonal = lax.broadcasted_iota(jnp.int32, (vectors, LANES), 0) == lax.broadcasted_iota(
        jnp.int32, (vectors, LANES), 1
    )
    column = jnp.sum(summed, axis=1, keepdims=True)
    flat = jnp.sum(jnp.where(diagonal, column, 0.0), axis=0, keepdims=True)
    flat = jnp.broadcast_to(flat, (8, LANES))
    square[...] = flat
    squares[me] = flat

    def square_copy(step):
        return pltpu.make_async_remote_copy(
            src_ref=square, dst_ref=squares.at[me], send_sem=r_send.at[step], recv_sem=r_recv.at[step],
            device_id=(lax.rem(me + step, n), core), device_id_type=MESH,
        )

    def square_arrival(step):
        return pltpu.make_async_remote_copy(
            src_ref=square, dst_ref=squares.at[lax.rem(me + n - step, n)],
            send_sem=r_send.at[step], recv_sem=r_recv.at[step],
            device_id=(lax.rem(me + step, n), core), device_id_type=MESH,
        )

    @pl.loop(1, n)
    def _(step):
        square_copy(step).start()

    @pl.loop(0, CHUNKS)
    def _(chunk):
        for step in range(lines - 1):
            for way in (1, -1):

                @pl.when(sends(step, way))
                def _():
                    line_copy(chunk, step, way).wait_send()

        for line in range(lines):

            @pl.when(by_row(chunk, line))
            def _():
                y_copy(chunk, line).wait_send()

            for row in range(2):
                core_copy(chunk, row, line).wait_send()

        @pl.when(turns(chunk))
        def _():
            turn_copy(chunk).wait_send()

    for piece in range(pieces):
        for target in range(2):
            k_copy(piece, target).wait_send()
        k_keep(piece).wait_send()
    for turn in range(BATCHES):
        value_copy(turn).wait_send()
    field_copy.wait_send()

    @pl.loop(1, n)
    def _(step):
        square_arrival(step).wait()

    energy_all = squares[0]
    for device in range(1, n):
        energy_all = energy_all + squares[device]
    scale = jnp.sqrt(energy_all / (points * n * steps) + 1e-06)
    rms_ref[...] = scale
    out_ref[...] = total


def finish_kernel(field_ref, scale_ref, out_ref, rms_ref):
    vectors, points, steps = out_ref.shape
    scale = scale_ref[:1]
    rms_ref[...] = scale[0, :vectors]
    diagonal = lax.broadcasted_iota(jnp.int32, (vectors, LANES), 0) == lax.broadcasted_iota(
        jnp.int32, (vectors, LANES), 1
    )
    spread = jnp.broadcast_to(scale, (vectors, LANES))
    divisor = jnp.sum(jnp.where(diagonal, spread, 0.0), axis=1, keepdims=True)
    for point in range(points):
        out_ref[:, point, :] = field_ref[point * vectors : (point + 1) * vectors, :steps] / divisor


def paired_body(data, spectra):
    n = lax.axis_size("param")
    vectors, local, steps = data.shape
    sensors, points, freqs = spectra.shape[1:]
    wide = -(-steps // LANES) * LANES
    groups = -(-freqs // (2 * GROUP))
    count = groups * GROUP
    rows_pad = -(-count // 16) * 16
    deep = -(-count // LANES) * LANES
    pieces = groups // PIECE
    lines = n // 4
    forward, backward = paired_tables(steps, freqs, groups, rows_pad, wide)
    maps = fold_maps(steps)

    turned = jnp.transpose(spectra, (0, 3, 2, 1)).reshape(2, freqs, points, 2, LANES)
    turned = jnp.transpose(turned, (0, 1, 3, 2, 4)).reshape(2, freqs, 2 * points, LANES)

    hbm = pl.BlockSpec(memory_space=pl.ANY)
    vmem = pl.BlockSpec(memory_space=pltpu.VMEM)
    dma = pltpu.SemaphoreType.DMA
    f32, bf16 = jnp.float32, jnp.bfloat16
    fields, scale = pl.pallas_call(
        functools.partial(kernel, n, lines, vectors, local, steps, points, freqs, groups, wide),
        out_shape=(
            jax.ShapeDtypeStruct((points * vectors, wide), f32),
            jax.ShapeDtypeStruct((8, LANES), f32),
        ),
        in_specs=[hbm, hbm, hbm, hbm, vmem],
        out_specs=(vmem, vmem),
        scratch_shapes=[
            pltpu.VMEM((vectors, local, steps), f32),
            pltpu.VMEM((2, wide, 4 * LANES), bf16),
            pltpu.VMEM((2, 2 * count, 2 * points, LANES), f32),
            pltpu.VMEM((2, 2, groups, 2, GROUP // 2, 2 * points, LANES), f32),
            pltpu.VMEM((3, 2, groups, GROUP // 2, 2 * points, LANES), f32),
            pltpu.VMEM((CHUNKS, sensors, 7 * LANES), f32),
            pltpu.VMEM((6, 2 * rows_pad, LANES), bf16),
            pltpu.VMEM((2, 2, deep, wide), bf16),
            pltpu.VMEM((2, count * 2 * vectors, LANES), f32),
            pltpu.VMEM((2, count * points, LANES), f32),
            pltpu.VMEM((deep, LANES), f32),
            pltpu.VMEM((count, LANES), f32),
            pltpu.VMEM((count, LANES), f32),
            pltpu.VMEM((points * vectors, wide), f32),
            pltpu.VMEM((points * vectors, wide), f32),
            pltpu.VMEM((8, LANES), f32),
            pltpu.VMEM((n, 8, LANES), f32),
            dma((3,)),
            dma((pieces,)),
            dma((pieces, 3)), dma((pieces, 3)),
            dma((CHUNKS, 2 * lines)), dma((CHUNKS, 2 * lines)),
            dma((CHUNKS, lines)), dma((CHUNKS, lines)),
            dma((CHUNKS, 2 * lines)), dma((CHUNKS, 2 * lines)),
            dma((CHUNKS,)), dma((CHUNKS,)),
            dma((BATCHES,)), dma((BATCHES,)),
            dma((1,)), dma((1,)),
            dma((n,)), dma((n,)),
        ],
        compiler_params=pltpu.CompilerParams(
            collective_id=0, has_side_effects=True, vmem_limit_bytes=60 * 1024 * 1024
        ),
    )(data, turned, jnp.asarray(forward), jnp.asarray(backward), jnp.asarray(maps))
    return pl.pallas_call(
        finish_kernel,
        out_shape=(jax.ShapeDtypeStruct((vectors, points, steps), f32), jax.ShapeDtypeStruct((vectors,), f32)),
        in_specs=[vmem, vmem],
        out_specs=(vmem, vmem),
    )(fields, scale)


def solution(mesh):
    in_specs = (P(None, ("sensor", "param"), None), P(None, "sensor", "param", None))
    out_specs = (P(None, "param", None), P())
    n = mesh.shape["param"]
    pair = mesh.shape["sensor"] == 2 and n == 16

    def body(data, spectra):
        vectors, local, _ = data.shape
        sensors, points = spectra.shape[1:3]
        fits = local * n * 2 == 2 * sensors and sensors == 2 * LANES and vectors == 2 * CHUNKS
        fits = fits and points * 2 * vectors == LANES and folded_layout_fits(data.shape[2])
        return (paired_body if pair and fits else general_body)(data, spectra)

    return jax.shard_map(body, mesh=mesh, in_specs=in_specs, out_specs=out_specs, check_vma=False)
```

```python
import functools
import math

import jax
import jax.numpy as jnp
import numpy as np
from jax import lax
from jax.experimental import pallas as pl
from jax.experimental.pallas import tpu as pltpu
from jax.sharding import PartitionSpec as P

MESH = pl.DeviceIdType.MESH
LANES = 128
GROUP = 8
CHUNKS = 8
PIECE = 3
BATCHES = 3


def spectral_tables(steps):
    length = 2 * steps
    freqs = steps + 1
    times = lax.broadcasted_iota(jnp.int32, (steps, freqs), 0)
    bins = lax.broadcasted_iota(jnp.int32, (steps, freqs), 1)
    phase = 2.0 * math.pi / length * (times * bins % length).astype(jnp.float32)
    forward = jnp.concatenate([jnp.cos(phase), -jnp.sin(phase)], axis=1)
    weight = jnp.where((bins == 0) | (bins == steps), 1.0, 2.0) / length
    backward = jnp.concatenate([(weight * jnp.cos(phase)).T, (-weight * jnp.sin(phase)).T], axis=0)
    return (forward, backward)


def to_spectrum(series, forward):
    vectors, sensors, steps = series.shape
    flat = jnp.dot(
        series.reshape(vectors * sensors, steps),
        forward,
        precision=lax.Precision.HIGHEST,
        preferred_element_type=jnp.float32,
    )
    return flat.reshape(vectors, sensors, forward.shape[1])


def contract(kernel, spectrum):
    return jnp.einsum(
        "spf,rsf->rpf",
        kernel,
        spectrum,
        precision=lax.Precision.HIGHEST,
        preferred_element_type=jnp.float32,
    )


def general_body(data, spectra):
    steps = data.shape[2]
    freqs = steps + 1
    forward, backward = spectral_tables(steps)
    whole = to_spectrum(lax.all_gather(data, "param", axis=1, tiled=True), forward)
    real_part = whole[..., :freqs]
    imag_part = whole[..., freqs:]
    kernel_re = spectra[0]
    kernel_im = spectra[1]
    out_re = contract(kernel_re, real_part) + contract(kernel_im, imag_part)
    out_im = contract(kernel_re, imag_part) - contract(kernel_im, real_part)
    vectors, points = (out_re.shape[0], out_re.shape[1])
    stacked = jnp.concatenate([out_re, out_im], axis=2).reshape(vectors * points, 2 * freqs)
    partial_field = jnp.dot(
        stacked, backward, precision=lax.Precision.HIGHEST, preferred_element_type=jnp.float32
    ).reshape(vectors, points, steps)
    count = points * lax.axis_size("param") * steps
    share = lax.psum_scatter(partial_field, "sensor", scatter_dimension=0, tiled=True)
    squares = lax.psum(jnp.sum(share * share, axis=(1, 2)), "param")
    scale = jnp.sqrt(squares / count + 1e-06)
    normalized = share / scale[:, None, None]
    gradient, rms_all = (
        lax.all_gather(normalized, "sensor", axis=0, tiled=True),
        lax.all_gather(scale, "sensor", axis=0, tiled=True),
    )
    return (gradient, rms_all)


def split(value):
    high = value.astype(jnp.bfloat16)
    return high, (value - high.astype(jnp.float32)).astype(jnp.bfloat16)


NT_DIMS = (((1,), (1,)), ((), ()))


def product(left, right, dims):
    dot = functools.partial(lax.dot_general, dimension_numbers=dims, preferred_element_type=jnp.float32)
    size = left[0].shape[0]
    both = dot(jnp.concatenate(left, axis=0), right[0])
    return both[:size] + (both[size:] + dot(left[0], right[1]))


def split_product(table, rows, right):
    dot = functools.partial(lax.dot_general, dimension_numbers=NT_DIMS, preferred_element_type=jnp.float32)
    half = table.shape[0] // 2
    both = dot(table, right[0])
    return both[:rows] + (both[half : half + rows] + dot(table[:half], right[1])[:rows])


def folded_layout_fits(steps):
    half = steps // 2
    rest = half + 1 - LANES
    groups = -(-(steps + 1) // (2 * GROUP))
    fits = steps % 2 == 0 and 0 < rest < LANES and half - LANES - (LANES - rest) <= LANES - rest
    return fits and groups % (PIECE * BATCHES) == 0


def frequency_order(freqs, groups):
    bins = np.arange(groups * 2 * GROUP).reshape(groups, 2, GROUP)
    return [bins[:, core].reshape(-1) for core in range(2)]


def lane_times(steps):
    half = steps // 2
    rest = half + 1 - LANES
    room = LANES - rest
    lane = np.arange(LANES)
    first = np.where(lane < rest, LANES + lane, -1)
    first_odd = np.where(lane < rest - 1, LANES + lane, -1)
    second = np.where(lane >= room, LANES + lane - room, -1)
    tail_a = np.where(lane >= rest, LANES + lane - rest, -1)
    tail_b = np.where(lane < rest - 1 - room, LANES + room + lane, -1)
    return lane, first, first_odd, second, tail_a, tail_b


def fold_maps(steps):
    lane, first, first_odd, second, tail_a, tail_b = lane_times(steps)
    shared = np.where(second >= 0, second, tail_b)
    even = np.concatenate([lane, lane, first, first_odd])
    odd = np.concatenate([lane, lane, tail_a, shared])
    ones = np.ones(LANES, np.int64)
    even_sign = np.concatenate([ones, -ones, ones, -ones])
    odd_sign = np.concatenate([ones, -ones, -ones, np.where(second >= 0, 1, -1)])
    maps = np.full((8, 4 * LANES), -1, np.int32)
    for index, (time, sign) in enumerate(((even, even_sign), (odd, odd_sign))):
        mirror = np.where((time > 0) & (2 * time != steps), steps - time, -1)
        maps[3 * index] = time
        maps[3 * index + 1] = np.where(time < 0, -1, mirror)
        maps[3 * index + 2] = sign
    return maps


def halves(values):
    high = values.astype(jnp.bfloat16)
    return high, (values - high.astype(np.float32)).astype(jnp.bfloat16)


def paired_tables(steps, freqs, groups, rows_pad, wide):
    half = steps // 2
    lane, first, first_odd, second, tail_a, tail_b = lane_times(steps)
    tail = np.where(tail_a >= 0, tail_a, tail_b)
    forward, backward = [], []
    for bins in frequency_order(freqs, groups):
        count = bins.shape[0]
        known = (bins < freqs)[:, None]
        even = (bins % 2 == 0)[:, None]
        angle = bins[:, None] * np.arange(steps)[None, :] % (2 * steps)
        phase = np.pi / steps * angle
        sine = np.where(angle % steps == 0, 0.0, np.sin(phase))
        cosine = np.cos(phase)
        symmetric = np.where(known, np.where(even, cosine, -sine), 0.0)
        other = np.where(known, np.where(even, -sine, cosine), 0.0)
        blocks = []
        for table, times in (
            (symmetric, lane), (other, lane), (symmetric, first), (other, first_odd), (symmetric, second), (other, tail),
        ):
            limit = half if table is symmetric else half - 1
            inside = (times >= 0) & (times <= limit)
            value = np.where(inside[None, :], table[:, np.clip(times, 0, limit)], 0.0).astype(np.float32)
            block = np.zeros((2, rows_pad, LANES), jnp.bfloat16)
            block[0, :count], block[1, :count] = halves(value)
            blocks.append(block.reshape(2 * rows_pad, LANES))
        forward.append(np.stack(blocks))
        weight = np.where((bins == 0) | (bins == steps), 0.5, 1.0)[:, None] / steps
        inverse = np.zeros((2, 2, rows_pad, wide), jnp.bfloat16)
        for position, table in enumerate((symmetric, other)):
            value = (table * weight).astype(np.float32)
            inverse[0, position, :count, :steps], inverse[1, position, :count, :steps] = halves(value)
        backward.append(inverse)
    return np.stack(forward), np.stack(backward)


def kernel(
    n, lines, vectors, local, steps, points, freqs, groups, wide,
    data_ref, spectra_ref, forward_ref, backward_ref, maps_ref,
    out_ref, rms_ref,
    series, fold, raw, packed, kbuf, gathered, table, inverse, spectrum, product_s, own_val, send_val, recv_val,
    partial, pair, square, squares,
    load_sem, raw_sem, k_send, k_recv, z_send, z_recv, y_send, y_recv, c_send, c_recv, w_send, w_recv,
    v_send, v_recv, f_send, f_recv, r_send, r_recv,
):
    me = lax.axis_index("param")
    core = lax.axis_index("sensor")
    x = lax.rem(me, 2)
    y = lax.rem(me // 2, 2)
    z = me // 4
    plane = 4
    other_chip = me + 1 - 2 * x
    y_chip = me + 2 - 4 * y
    other_core = 1 - core
    z_mate = z + 1 - 2 * lax.rem(z, 2)
    half = steps // 2
    rest = half + 1 - LANES
    rows = points * GROUP
    count = groups * GROUP
    pieces = groups // PIECE
    span = PIECE * 2 * GROUP
    batch = groups // BATCHES

    barrier = pltpu.get_barrier_semaphore()

    for neighbour in ((other_chip, core), (other_chip, other_core), (y_chip, core), (me, other_core)):
        pl.semaphore_signal(barrier, inc=1, device_id=neighbour, device_id_type=MESH)

    @pl.when(z > 0)
    def _():
        pl.semaphore_signal(barrier, inc=1, device_id=(me - plane, core), device_id_type=MESH)

    @pl.when(z + 1 < lines)
    def _():
        pl.semaphore_signal(barrier, inc=1, device_id=(me + plane, core), device_id_type=MESH)

    def filled(piece, target):
        known = -(-(freqs - target * GROUP) // (2 * GROUP))
        return min(PIECE, known - piece * PIECE)

    def raw_copy(piece):
        begin = piece * span
        size = min(span, freqs - begin)
        return pltpu.make_async_copy(
            spectra_ref.at[:, pl.ds(begin, size)], raw.at[:, pl.ds(begin, size)], raw_sem.at[piece]
        )

    data_copy = pltpu.make_async_copy(data_ref, series, load_sem.at[0])
    forward_copy = pltpu.make_async_copy(forward_ref.at[core], table, load_sem.at[1])
    backward_copy = pltpu.make_async_copy(
        backward_ref.at[core], inverse.at[:, :, pl.ds(0, backward_ref.shape[3])], load_sem.at[2]
    )
    raw_copy(0).start()
    data_copy.start()
    for piece in range(1, pieces):
        raw_copy(piece).start()
    forward_copy.start()
    backward_copy.start()

    raw[:, freqs:] = jnp.zeros((2, raw.shape[1] - freqs) + tuple(raw.shape[2:]), jnp.float32)
    pad = inverse.shape[2] - backward_ref.shape[3]
    inverse[:, :, inverse.shape[2] - pad :, :] = jnp.zeros((2, 2, pad, wide), jnp.bfloat16)
    short = filled(pieces - 1, 1)
    if short < PIECE:

        @pl.when(core == 1)
        def _():
            begin = (pieces - 1) * PIECE + short
            for owner in range(1, 3):
                kbuf[owner, :, begin:] = jnp.zeros((2, PIECE - short) + tuple(kbuf.shape[3:]), jnp.float32)

    own_val[count:, :] = jnp.zeros((own_val.shape[0] - count, LANES), jnp.float32)

    strip = 64

    @pl.loop(0, fold.shape[1] // strip)
    def _(part):
        begin = pl.multiple_of(part * strip, strip)
        time = lax.broadcasted_iota(jnp.int32, (strip, 4 * LANES), 0) + begin
        for side in range(2):
            direct = jnp.where(time == maps_ref[3 * side : 3 * side + 1, :], 1.0, 0.0)
            sign = maps_ref[3 * side + 2 : 3 * side + 3, :].astype(jnp.float32)
            mirror = jnp.where(time == maps_ref[3 * side + 1 : 3 * side + 2, :], sign, 0.0)
            fold[side, pl.ds(begin, strip), :] = (direct + mirror).astype(jnp.bfloat16)

    upper = lax.broadcasted_iota(jnp.int32, (8, LANES), 0) < points
    stripe = lax.broadcasted_iota(jnp.int32, (8, LANES), 1) // local % 2 == 0

    def sort_piece(piece):
        @pl.loop(0, 2)
        def _(part):
            @pl.loop(piece * PIECE, (piece + 1) * PIECE)
            def _(group):
                for side in range(2):
                    for duo in range(GROUP // 2):
                        begin = group * 2 * GROUP + side * GROUP + 2 * duo
                        first = raw[part, begin]
                        second = raw[part, begin + 1]
                        low = jnp.where(upper, first, pltpu.roll(second, points, 0))
                        high = jnp.where(upper, pltpu.roll(first, points, 0), second)
                        packed[0, part, group, side, duo] = jnp.where(stripe, low, pltpu.roll(high, local, 1))
                        packed[1, part, group, side, duo] = jnp.where(stripe, pltpu.roll(high, LANES - local, 1), low)

    def k_copy(piece, target):
        begin = piece * PIECE
        size = filled(piece, target)
        rel = core if target == 0 else other_core
        return pltpu.make_async_remote_copy(
            src_ref=packed.at[1 - x, :, pl.ds(begin, size), target],
            dst_ref=kbuf.at[1 + rel, :, pl.ds(begin, size)],
            send_sem=k_send.at[target], recv_sem=k_recv.at[piece // (pieces // BATCHES)],
            device_id=(other_chip, target), device_id_type=MESH,
        )

    def k_keep(piece):
        begin = piece * PIECE
        return pltpu.make_async_remote_copy(
            src_ref=packed.at[x, :, pl.ds(begin, PIECE), other_core],
            dst_ref=kbuf.at[0, :, pl.ds(begin, PIECE)],
            send_sem=k_send.at[2], recv_sem=k_recv.at[piece // (pieces // BATCHES)],
            device_id=(me, other_core), device_id_type=MESH,
        )

    def all_of(ref, send_sem, recv_sem):
        return pltpu.make_async_remote_copy(
            src_ref=ref, dst_ref=ref, send_sem=send_sem, recv_sem=recv_sem,
            device_id=(me, other_core), device_id_type=MESH,
        )

    def wait_batch(turn):
        begin = turn * batch
        full = all_of(kbuf.at[:, :, pl.ds(begin, batch)], k_send.at[2], k_recv.at[turn])
        missing = 0 if turn + 1 < BATCHES else 2 * (PIECE - filled(pieces - 1, 1))
        if missing:
            short = all_of(packed.at[0, 0, pl.ds(0, 3 * batch - missing)], k_send.at[2], k_recv.at[turn])
            pl.when(core == 0)(full.wait_recv)
            pl.when(core == 1)(short.wait_recv)
        else:
            full.wait_recv()

    def send_piece(piece):
        for target in range(2):
            k_copy(piece, target).start()
        k_keep(piece).start()

    raw_copy(0).wait()
    sort_piece(0)
    pl.semaphore_wait(barrier, 4 + jnp.minimum(z, 1) + jnp.minimum(lines - 1 - z, 1))
    send_piece(0)

    def slot(line, row, column):
        return line * plane + row * 2 + column

    def place(line, row):
        upper_line = line // 2
        return lax.rem(line, 2) * plane + row * 2 + upper_line + x - 2 * upper_line * x

    def block(chunk, line, row, rel=0):
        position = rel * (n // 2) + place(line, row)
        return gathered.at[chunk, pl.ds(pl.multiple_of(position * local, local), local), :]

    data_copy.wait()
    plain = (((1,), (0,)), ((), ()))
    folded = []
    for side in range(2):
        values = jnp.concatenate([series[2 * chunk + side] for chunk in range(CHUNKS)], axis=0)
        high = values.astype(jnp.bfloat16)
        left = values - high.astype(jnp.float32)
        middle = left.astype(jnp.bfloat16)
        low = (left - middle.astype(jnp.float32)).astype(jnp.bfloat16)
        result = lax.dot_general(
            jnp.concatenate([high, middle, low], axis=0), fold[side, :steps, :], plain,
            preferred_element_type=jnp.float32,
        )
        size = CHUNKS * local
        folded.append(result[:size] + (result[size : 2 * size] + result[2 * size :]))
    own_row = pl.ds(pl.multiple_of(place(z, y) * local, local), local)
    for chunk in range(CHUNKS):
        even = folded[0][chunk * local : (chunk + 1) * local]
        odd = folded[1][chunk * local : (chunk + 1) * local]
        gathered[chunk, own_row, 0 : 2 * LANES] = even[:, : 2 * LANES]
        gathered[chunk, own_row, 2 * LANES : 4 * LANES] = odd[:, : 2 * LANES]
        gathered[chunk, own_row, 4 * LANES : 5 * LANES] = (
            even[:, 2 * LANES : 3 * LANES] + odd[:, 2 * LANES : 3 * LANES]
        )
        gathered[chunk, own_row, 5 * LANES : 6 * LANES] = even[:, 3 * LANES :]
        gathered[chunk, own_row, 6 * LANES :] = odd[:, 3 * LANES :]

    def send(source, target, send_sem, recv_sem):
        return pltpu.make_async_remote_copy(
            src_ref=source, dst_ref=source, send_sem=send_sem, recv_sem=recv_sem,
            device_id=target, device_id_type=MESH,
        )

    def some(blocks, send_sem, recv_sem):
        return all_of(gathered.at[0, pl.ds(0, blocks * local)], send_sem, recv_sem)

    def many(blocks, send_sem, recv_sem):
        whole = gathered.shape[1] // local
        if blocks <= whole:
            return some(blocks, send_sem, recv_sem)
        assert blocks % CHUNKS == 0
        return all_of(gathered.at[:, pl.ds(0, blocks // CHUNKS * local)], send_sem, recv_sem)

    def line_index(source, target):
        return jnp.where(source < target, source, source - 1)

    def line_copy(chunk, step, way):
        source = jnp.clip(z - way * step, 0, lines - 1)
        target = jnp.clip(z + way, 0, lines - 1)
        return send(
            block(chunk, source, y), (slot(target, y, x), core),
            z_send.at[0], z_recv.at[chunk, jnp.clip(line_index(source, target), 0, lines - 2)],
        )

    def line_arrival(chunk, step, way):
        source = jnp.clip(z - way * (step + 1), 0, lines - 1)
        target = jnp.clip(z + way, 0, lines - 1)
        return source, send(
            block(chunk, source, y), (slot(target, y, x), core),
            z_send.at[0], z_recv.at[chunk, jnp.clip(line_index(source, z), 0, lines - 2)],
        )

    def sends(step, way):
        inside = z + 1 < lines if way > 0 else z > 0
        begun = z >= step if way > 0 else z + step < lines
        return jnp.logical_and(inside, begun)

    def receives(step, way):
        return z >= step + 1 if way > 0 else z + step + 1 < lines

    def y_copy(chunk, line):
        index = jnp.where(line == z, 0, 1)
        return send(block(chunk, line, y), (y_chip, core), y_send.at[0], y_recv.at[chunk, index])

    def turn_copy(chunk):
        return send(block(chunk, z, 1 - y), (slot(z_mate, y, x), core), w_send.at[0], w_recv.at[chunk])

    def turn_arrival(chunk):
        return send(block(chunk, z_mate, 1 - y), (slot(z_mate, y, x), core), w_send.at[0], w_recv.at[chunk])

    def turns(chunk):
        return chunk >= CHUNKS // 2

    def by_row(chunk, line):
        return jnp.logical_not(jnp.logical_and(turns(chunk), line == z_mate))

    def core_copy(chunk, row, line):
        return pltpu.make_async_remote_copy(
            src_ref=block(chunk, line, row), dst_ref=block(chunk, line, row, 1),
            send_sem=c_send.at[0], recv_sem=c_recv.at[chunk],
            device_id=(me, other_core), device_id_type=MESH,
        )

    def start_lines(chunk):
        for way in (1, -1):

            @pl.when(sends(0, way))
            def _():
                line_copy(chunk, 0, way).start()

        y_copy(chunk, z).start()
        core_copy(chunk, y, z).start()

    def from_lines(chunk, step):
        for way in (1, -1):

            @pl.when(receives(step, way))
            def _():
                source, arrival = line_arrival(chunk, step, way)
                arrival.wait_recv()
                if step + 1 < lines - 1:

                    @pl.when(sends(step + 1, way))
                    def _():
                        line_copy(chunk, step + 1, way).start()

                @pl.when(by_row(chunk, source))
                def _():
                    y_copy(chunk, source).start()

                core_copy(chunk, y, source).start()

    def from_mate(chunk):
        some(1, y_send.at[0], y_recv.at[chunk, 0]).wait_recv()
        core_copy(chunk, 1 - y, z).start()

    def to_mate(chunk):
        @pl.when(turns(chunk))
        def _():
            turn_copy(chunk).start()

    def from_row(chunk):
        @pl.when(turns(chunk))
        def _():
            some(lines - 2, y_send.at[0], y_recv.at[chunk, 1]).wait_recv()
            turn_arrival(chunk).wait_recv()

        @pl.when(jnp.logical_not(turns(chunk)))
        def _():
            some(lines - 1, y_send.at[0], y_recv.at[chunk, 1]).wait_recv()

        for step in range(1, lines):
            core_copy(chunk, 1 - y, lax.rem(z + step, lines)).start()

    def from_core(chunk):
        some(n // 2, c_send.at[0], c_recv.at[chunk]).wait_recv()

    lane_index = lax.broadcasted_iota(jnp.int32, (gathered.shape[1], LANES), 1)

    def transform(chunk):
        def lanes(index):
            return gathered[chunk, :, index * LANES : (index + 1) * LANES]

        for which in range(4):
            odd = which // 2
            position = which % 2
            if which < 2:
                tail = lanes(4 + which)
            elif which == 2:
                tail = lanes(6)
            else:
                tail = jnp.where(lane_index >= rest, lanes(4), lanes(6))
            right = split(jnp.concatenate([lanes(which), tail], axis=1))
            left = jnp.concatenate([table[position], table[2 + which]], axis=1)
            result = split_product(left, count, right)
            for lane in range(2):
                spectrum[lane, pl.ds(position * vectors + 2 * chunk + odd, count, stride=2 * vectors), :] = result[
                    :, lane * LANES : (lane + 1) * LANES
                ]

    pl.loop(0, CHUNKS)(start_lines)

    for piece in range(1, pieces):
        raw_copy(piece).wait()
        sort_piece(piece)
        send_piece(piece)

    forward_copy.wait()
    backward_copy.wait()

    def finish(chunk):
        from_core(chunk)
        transform(chunk)

    stages = [
        (functools.partial(from_lines, step=0), 0), (from_mate, 0),
        (functools.partial(from_lines, step=1), 1), (functools.partial(from_lines, step=2), 2),
        (to_mate, 4), (from_row, 6), (finish, 7),
    ]

    @pl.loop(0, CHUNKS + 7)
    def _(turn):
        for stage, age in stages:
            chunk = turn - age

            @pl.when(jnp.logical_and(chunk >= 0, chunk < CHUNKS))
            def _():
                stage(chunk)

    columns = GROUP * 2 * vectors
    row_freq = lax.broadcasted_iota(jnp.int32, (4 * rows, columns), 0) // points % GROUP
    col_freq = lax.broadcasted_iota(jnp.int32, (4 * rows, columns), 1) // (2 * vectors)
    own = row_freq == col_freq
    lane = lax.broadcasted_iota(jnp.int32, (2 * rows, LANES), 1)
    row = lax.broadcasted_iota(jnp.int32, (2 * rows, LANES), 0) // points % 2
    sign = jnp.where((lane % (2 * vectors) < vectors) == (row == 0), 1.0, -1.0)
    step_rows = batch * GROUP
    owner_lane = lax.broadcasted_iota(jnp.int32, (step_rows, LANES), 1) // (2 * vectors)

    def value_copy(turn):
        place_rows = pl.ds(pl.multiple_of(turn * step_rows, GROUP), step_rows)
        return pltpu.make_async_remote_copy(
            src_ref=send_val.at[place_rows], dst_ref=recv_val.at[place_rows],
            send_sem=v_send.at[0], recv_sem=v_recv.at[0],
            device_id=(other_chip, core), device_id_type=MESH,
        )

    @pl.loop(0, BATCHES)
    def _(turn):
        for which in range(BATCHES):

            @pl.when(turn == which)
            def _():
                wait_batch(which)

        for step in range(batch):
            group = turn * batch + step
            begin = pl.multiple_of(group * columns, columns)
            right = split(
                jnp.concatenate([spectrum[0, pl.ds(begin, columns), :], spectrum[1, pl.ds(begin, columns), :]], axis=1)
            )
            parts = []
            for part in range(2):
                for near, far in (
                    (packed[x, part, group, core], kbuf[0, part, group]), (kbuf[1, part, group], kbuf[2, part, group]),
                ):
                    parts.append(jnp.concatenate([near.reshape(rows, LANES), far.reshape(rows, LANES)], axis=1))
            left = jnp.concatenate(parts, axis=0)
            found = jnp.where(own, product(split(left), right, NT_DIMS), 0.0)
            width = columns
            while width > LANES:
                width //= 2
                found = found[:, :width] + found[:, width:]
            hop = LANES // 2
            while hop >= 2 * vectors:
                found = found + pltpu.roll(found, hop, 1)
                hop //= 2
            value = found[: 2 * rows] + sign * pltpu.roll(found[2 * rows :], vectors, 1)
            for owner in range(2):
                product_s[owner, pl.ds(pl.multiple_of(group * rows, rows), rows), :] = value[
                    owner * rows : (owner + 1) * rows
                ]
        begin = turn * batch * rows
        for owner, target in ((1, send_val), (0, own_val)):
            merged = jnp.zeros((step_rows, LANES), jnp.float32)
            for point in range(points):
                merged = jnp.where(
                    owner_lane == point, product_s[owner, pl.ds(begin + point, step_rows, stride=points), :], merged
                )
            target[pl.ds(pl.multiple_of(turn * step_rows, GROUP), step_rows), :] = merged
        value_copy(turn).start()

    all_of(recv_val, v_send.at[0], v_recv.at[0]).wait_recv()

    own_val[:count, :] = own_val[:count, :] + recv_val[...]
    turned = own_val[...].T
    by_position = []
    for position in range(2):
        by_position.append(jnp.concatenate(
            [turned[(2 * point + position) * vectors : (2 * point + position + 1) * vectors] for point in range(points)],
            axis=0,
        ))
    left = split(jnp.concatenate(by_position, axis=1))
    deep = 2 * inverse.shape[2]
    partial[...] = product(left, (inverse[0].reshape(deep, wide), inverse[1].reshape(deep, wide)), plain)

    field_copy = pltpu.make_async_remote_copy(
        src_ref=partial, dst_ref=pair, send_sem=f_send.at[0], recv_sem=f_recv.at[0],
        device_id=(me, other_core), device_id_type=MESH,
    )
    field_copy.start()
    field_copy.wait_recv()

    total = partial[...] + pair[...]
    energy = total * total
    summed = energy[:vectors]
    for point in range(1, points):
        summed = summed + energy[point * vectors : (point + 1) * vectors]
    diagonal = lax.broadcasted_iota(jnp.int32, (vectors, LANES), 0) == lax.broadcasted_iota(
        jnp.int32, (vectors, LANES), 1
    )
    column = jnp.sum(summed, axis=1, keepdims=True)
    flat = jnp.sum(jnp.where(diagonal, column, 0.0), axis=0, keepdims=True)
    flat = jnp.broadcast_to(flat, (8, LANES))
    square[...] = flat
    squares[me] = flat

    def square_copy(step):
        return pltpu.make_async_remote_copy(
            src_ref=square, dst_ref=squares.at[me], send_sem=r_send.at[0], recv_sem=r_recv.at[0],
            device_id=(lax.rem(me + step, n), core), device_id_type=MESH,
        )

    @pl.loop(1, n)
    def _(step):
        square_copy(step).start()

    for line in range(lines):
        ahead = line + 1 if line + 1 < lines else 0
        back = lines - line if line > 0 else 0

        @pl.when(z == line)
        def _():
            many((ahead + back) * CHUNKS, z_send.at[0], z_recv.at[0, 0]).wait_send()

    late = CHUNKS - CHUNKS // 2
    all_of(
        gathered.at[:, pl.ds(0, (lines * CHUNKS - late) * local // CHUNKS)], y_send.at[0], y_recv.at[0, 0]
    ).wait_send()
    some(late, w_send.at[0], w_recv.at[0]).wait_send()
    all_of(gathered.at[:, pl.ds(0, gathered.shape[1] // 2)], c_send.at[0], c_recv.at[0]).wait_send()
    for target in range(2):
        all_of(packed.at[0, :, pl.ds(0, groups - PIECE + filled(pieces - 1, target)), target],
               k_send.at[target], k_recv.at[0]).wait_send()
    all_of(packed.at[0, :, :, 0], k_send.at[2], k_recv.at[0]).wait_send()
    all_of(send_val, v_send.at[0], v_recv.at[0]).wait_send()
    field_copy.wait_send()

    all_of(squares.at[pl.ds(0, n - 1)], r_send.at[0], r_recv.at[0]).wait()

    energy_all = squares[0]
    for device in range(1, n):
        energy_all = energy_all + squares[device]
    scale = jnp.sqrt(energy_all / (points * n * steps) + 1e-06)
    rms_ref[...] = scale
    out_ref[...] = total


def finish_kernel(field_ref, scale_ref, out_ref, rms_ref):
    vectors, points, steps = out_ref.shape
    scale = scale_ref[:1]
    rms_ref[...] = scale[0, :vectors]
    diagonal = lax.broadcasted_iota(jnp.int32, (vectors, LANES), 0) == lax.broadcasted_iota(
        jnp.int32, (vectors, LANES), 1
    )
    spread = jnp.broadcast_to(scale, (vectors, LANES))
    divisor = jnp.sum(jnp.where(diagonal, spread, 0.0), axis=1, keepdims=True)
    for point in range(points):
        out_ref[:, point, :] = field_ref[point * vectors : (point + 1) * vectors, :steps] / divisor


def paired_body(data, spectra):
    n = lax.axis_size("param")
    vectors, local, steps = data.shape
    sensors, points, freqs = spectra.shape[1:]
    wide = -(-steps // LANES) * LANES
    groups = -(-freqs // (2 * GROUP))
    count = groups * GROUP
    rows_pad = -(-count // 16) * 16
    deep = -(-count // LANES) * LANES
    pieces = groups // PIECE
    lines = n // 4
    forward, backward = paired_tables(steps, freqs, groups, rows_pad, wide)
    maps = fold_maps(steps)

    turned = jnp.transpose(spectra, (0, 3, 2, 1)).reshape(2, freqs, points, 2, LANES)
    turned = jnp.transpose(turned, (0, 1, 3, 2, 4)).reshape(2, freqs, 2 * points, LANES)

    hbm = pl.BlockSpec(memory_space=pl.ANY)
    vmem = pl.BlockSpec(memory_space=pltpu.VMEM)
    dma = pltpu.SemaphoreType.DMA
    f32, bf16 = jnp.float32, jnp.bfloat16
    fields, scale = pl.pallas_call(
        functools.partial(kernel, n, lines, vectors, local, steps, points, freqs, groups, wide),
        out_shape=(
            jax.ShapeDtypeStruct((points * vectors, wide), f32),
            jax.ShapeDtypeStruct((8, LANES), f32),
        ),
        in_specs=[hbm, hbm, hbm, hbm, vmem],
        out_specs=(vmem, vmem),
        scratch_shapes=[
            pltpu.VMEM((vectors, local, steps), f32),
            pltpu.VMEM((2, wide, 4 * LANES), bf16),
            pltpu.VMEM((2, 2 * count, 2 * points, LANES), f32),
            pltpu.VMEM((2, 2, groups, 2, GROUP // 2, 2 * points, LANES), f32),
            pltpu.VMEM((3, 2, groups, GROUP // 2, 2 * points, LANES), f32),
            pltpu.VMEM((CHUNKS, sensors, 7 * LANES), f32),
            pltpu.VMEM((6, 2 * rows_pad, LANES), bf16),
            pltpu.VMEM((2, 2, deep, wide), bf16),
            pltpu.VMEM((2, count * 2 * vectors, LANES), f32),
            pltpu.VMEM((2, count * points, LANES), f32),
            pltpu.VMEM((deep, LANES), f32),
            pltpu.VMEM((count, LANES), f32),
            pltpu.VMEM((count, LANES), f32),
            pltpu.VMEM((points * vectors, wide), f32),
            pltpu.VMEM((points * vectors, wide), f32),
            pltpu.VMEM((8, LANES), f32),
            pltpu.VMEM((n, 8, LANES), f32),
            dma((3,)),
            dma((pieces,)),
            dma((3,)), dma((BATCHES,)),
            dma((1,)), dma((CHUNKS, lines - 1)),
            dma((1,)), dma((CHUNKS, 2)),
            dma((1,)), dma((CHUNKS,)),
            dma((1,)), dma((CHUNKS,)),
            dma((1,)), dma((1,)),
            dma((1,)), dma((1,)),
            dma((1,)), dma((1,)),
        ],
        compiler_params=pltpu.CompilerParams(
            collective_id=0, has_side_effects=True, vmem_limit_bytes=60 * 1024 * 1024
        ),
    )(data, turned, jnp.asarray(forward), jnp.asarray(backward), jnp.asarray(maps))
    return pl.pallas_call(
        finish_kernel,
        out_shape=(jax.ShapeDtypeStruct((vectors, points, steps), f32), jax.ShapeDtypeStruct((vectors,), f32)),
        in_specs=[vmem, vmem],
        out_specs=(vmem, vmem),
    )(fields, scale)


def solution(mesh):
    in_specs = (P(None, ("sensor", "param"), None), P(None, "sensor", "param", None))
    out_specs = (P(None, "param", None), P())
    n = mesh.shape["param"]
    pair = mesh.shape["sensor"] == 2 and n == 16

    def body(data, spectra):
        vectors, local, _ = data.shape
        sensors, points = spectra.shape[1:3]
        fits = local * n == sensors and local % 8 == 0 and sensors == 2 * LANES and vectors == 2 * CHUNKS
        fits = fits and points * 2 * vectors == LANES and folded_layout_fits(data.shape[2])
        return (paired_body if pair and fits else general_body)(data, spectra)

    return jax.shard_map(body, mesh=mesh, in_specs=in_specs, out_specs=out_specs, check_vma=False)
```

```python
import functools
import math

import jax
import jax.numpy as jnp
import numpy as np
from jax import lax
from jax.experimental import pallas as pl
from jax.experimental.pallas import tpu as pltpu
from jax.sharding import PartitionSpec as P

MESH = pl.DeviceIdType.MESH
LANES = 128
GROUP = 8
CHUNKS = 8
PIECE = 3
BATCHES = 3


def spectral_tables(steps):
    length = 2 * steps
    freqs = steps + 1
    times = lax.broadcasted_iota(jnp.int32, (steps, freqs), 0)
    bins = lax.broadcasted_iota(jnp.int32, (steps, freqs), 1)
    phase = 2.0 * math.pi / length * (times * bins % length).astype(jnp.float32)
    forward = jnp.concatenate([jnp.cos(phase), -jnp.sin(phase)], axis=1)
    weight = jnp.where((bins == 0) | (bins == steps), 1.0, 2.0) / length
    backward = jnp.concatenate([(weight * jnp.cos(phase)).T, (-weight * jnp.sin(phase)).T], axis=0)
    return (forward, backward)


def to_spectrum(series, forward):
    vectors, sensors, steps = series.shape
    flat = jnp.dot(
        series.reshape(vectors * sensors, steps),
        forward,
        precision=lax.Precision.HIGHEST,
        preferred_element_type=jnp.float32,
    )
    return flat.reshape(vectors, sensors, forward.shape[1])


def contract(kernel, spectrum):
    return jnp.einsum(
        "spf,rsf->rpf",
        kernel,
        spectrum,
        precision=lax.Precision.HIGHEST,
        preferred_element_type=jnp.float32,
    )


def general_body(data, spectra):
    steps = data.shape[2]
    freqs = steps + 1
    forward, backward = spectral_tables(steps)
    whole = to_spectrum(lax.all_gather(data, "param", axis=1, tiled=True), forward)
    real_part = whole[..., :freqs]
    imag_part = whole[..., freqs:]
    kernel_re = spectra[0]
    kernel_im = spectra[1]
    out_re = contract(kernel_re, real_part) + contract(kernel_im, imag_part)
    out_im = contract(kernel_re, imag_part) - contract(kernel_im, real_part)
    vectors, points = (out_re.shape[0], out_re.shape[1])
    stacked = jnp.concatenate([out_re, out_im], axis=2).reshape(vectors * points, 2 * freqs)
    partial_field = jnp.dot(
        stacked, backward, precision=lax.Precision.HIGHEST, preferred_element_type=jnp.float32
    ).reshape(vectors, points, steps)
    count = points * lax.axis_size("param") * steps
    share = lax.psum_scatter(partial_field, "sensor", scatter_dimension=0, tiled=True)
    squares = lax.psum(jnp.sum(share * share, axis=(1, 2)), "param")
    scale = jnp.sqrt(squares / count + 1e-06)
    normalized = share / scale[:, None, None]
    gradient, rms_all = (
        lax.all_gather(normalized, "sensor", axis=0, tiled=True),
        lax.all_gather(scale, "sensor", axis=0, tiled=True),
    )
    return (gradient, rms_all)


def split(value):
    high = value.astype(jnp.bfloat16)
    return high, (value - high.astype(jnp.float32)).astype(jnp.bfloat16)


NT_DIMS = (((1,), (1,)), ((), ()))


def product(left, right, dims):
    dot = functools.partial(lax.dot_general, dimension_numbers=dims, preferred_element_type=jnp.float32)
    size = left[0].shape[0]
    both = dot(jnp.concatenate(left, axis=0), right[0])
    return both[:size] + (both[size:] + dot(left[0], right[1]))


def split_product(table, rows, right):
    dot = functools.partial(lax.dot_general, dimension_numbers=NT_DIMS, preferred_element_type=jnp.float32)
    half = table.shape[0] // 2
    both = dot(table, right[0])
    return both[:rows] + (both[half : half + rows] + dot(table[:half], right[1])[:rows])


def folded_layout_fits(steps):
    half = steps // 2
    rest = half + 1 - LANES
    groups = -(-(steps + 1) // (2 * GROUP))
    fits = steps % 2 == 0 and 0 < rest < LANES and half - LANES - (LANES - rest) <= LANES - rest
    fits = fits and groups % (PIECE * BATCHES) == 0
    return fits and BATCHES * batch_shares(groups // BATCHES * GROUP)[0][1] <= LANES


def frequency_order(freqs, groups):
    bins = np.arange(groups * 2 * GROUP).reshape(groups, 2, GROUP)
    return [bins[:, core].reshape(-1) for core in range(2)]


def lane_times(steps):
    half = steps // 2
    rest = half + 1 - LANES
    room = LANES - rest
    lane = np.arange(LANES)
    first = np.where(lane < rest, LANES + lane, -1)
    first_odd = np.where(lane < rest - 1, LANES + lane, -1)
    second = np.where(lane >= room, LANES + lane - room, -1)
    tail_a = np.where(lane >= rest, LANES + lane - rest, -1)
    tail_b = np.where(lane < rest - 1 - room, LANES + room + lane, -1)
    return lane, first, first_odd, second, tail_a, tail_b


def fold_maps(steps):
    lane, first, first_odd, second, tail_a, tail_b = lane_times(steps)
    shared = np.where(second >= 0, second, tail_b)
    even = np.concatenate([lane, lane, first, first_odd])
    odd = np.concatenate([lane, lane, tail_a, shared])
    ones = np.ones(LANES, np.int64)
    even_sign = np.concatenate([ones, -ones, ones, -ones])
    odd_sign = np.concatenate([ones, -ones, -ones, np.where(second >= 0, 1, -1)])
    maps = np.full((8, 4 * LANES), -1, np.int32)
    for index, (time, sign) in enumerate(((even, even_sign), (odd, odd_sign))):
        mirror = np.where((time > 0) & (2 * time != steps), steps - time, -1)
        maps[3 * index] = time
        maps[3 * index + 1] = np.where(time < 0, -1, mirror)
        maps[3 * index + 2] = sign
    return maps


def halves(values):
    high = values.astype(jnp.bfloat16)
    return high, (values - high.astype(np.float32)).astype(jnp.bfloat16)


def batch_shares(batch):
    first = -(-batch // (2 * GROUP)) * GROUP
    return ((0, first), (first, batch - first))


def paired_tables(steps, freqs, groups, rows_pad, wide):
    half = steps // 2
    lane, first, first_odd, second, tail_a, tail_b = lane_times(steps)
    tail = np.where(tail_a >= 0, tail_a, tail_b)
    forward, backward = [], []
    for bins in frequency_order(freqs, groups):
        count = bins.shape[0]
        known = (bins < freqs)[:, None]
        even = (bins % 2 == 0)[:, None]
        angle = bins[:, None] * np.arange(steps)[None, :] % (2 * steps)
        phase = np.pi / steps * angle
        sine = np.where(angle % steps == 0, 0.0, np.sin(phase))
        cosine = np.cos(phase)
        symmetric = np.where(known, np.where(even, cosine, -sine), 0.0)
        other = np.where(known, np.where(even, -sine, cosine), 0.0)
        blocks = []
        for table, times in (
            (symmetric, lane), (other, lane), (symmetric, first), (other, first_odd), (symmetric, second), (other, tail),
        ):
            limit = half if table is symmetric else half - 1
            inside = (times >= 0) & (times <= limit)
            value = np.where(inside[None, :], table[:, np.clip(times, 0, limit)], 0.0).astype(np.float32)
            block = np.zeros((2, rows_pad, LANES), jnp.bfloat16)
            block[0, :count], block[1, :count] = halves(value)
            blocks.append(block.reshape(2 * rows_pad, LANES))
        forward.append(np.stack(blocks))
        weight = np.where((bins == 0) | (bins == steps), 0.5, 1.0)[:, None] / steps
        inverse = np.zeros((2, 2, 2, LANES, wide), jnp.bfloat16)
        batch = groups // BATCHES * GROUP
        for position, table in enumerate((symmetric, other)):
            value = (table * weight).astype(np.float32)
            for turn in range(BATCHES):
                for share, (begin, size) in enumerate(batch_shares(batch)):
                    target = slice(turn * batch_shares(batch)[0][1], turn * batch_shares(batch)[0][1] + size)
                    source = slice(turn * batch + begin, turn * batch + begin + size)
                    parts = halves(value[source])
                    for index in range(2):
                        inverse[index, position, share, target, :steps] = parts[index]
        backward.append(inverse)
    return np.stack(forward), np.stack(backward)


def kernel(
    n, lines, vectors, local, steps, points, freqs, groups, wide,
    data_ref, spectra_ref, forward_ref, backward_ref, maps_ref,
    out_ref, rms_ref,
    series, fold, raw, packed, kbuf, gathered, table, inverse, spectrum, product_s, own_val, send_val, recv_val,
    partial, pair, square, squares,
    load_sem, raw_sem, k_send, k_recv, z_send, z_recv, y_send, y_recv, c_send, c_recv, w_send, w_recv,
    v_send, v_recv, f_send, f_recv, r_send, r_recv,
):
    me = lax.axis_index("param")
    core = lax.axis_index("sensor")
    x = lax.rem(me, 2)
    y = lax.rem(me // 2, 2)
    z = me // 4
    plane = 4
    other_chip = me + 1 - 2 * x
    y_chip = me + 2 - 4 * y
    other_core = 1 - core
    z_mate = z + 1 - 2 * lax.rem(z, 2)
    half = steps // 2
    rest = half + 1 - LANES
    rows = points * GROUP
    count = groups * GROUP
    pieces = groups // PIECE
    span = PIECE * 2 * GROUP
    batch = groups // BATCHES

    barrier = pltpu.get_barrier_semaphore()

    for neighbour in ((other_chip, core), (other_chip, other_core), (y_chip, core), (me, other_core)):
        pl.semaphore_signal(barrier, inc=1, device_id=neighbour, device_id_type=MESH)

    @pl.when(z > 0)
    def _():
        pl.semaphore_signal(barrier, inc=1, device_id=(me - plane, core), device_id_type=MESH)

    @pl.when(z + 1 < lines)
    def _():
        pl.semaphore_signal(barrier, inc=1, device_id=(me + plane, core), device_id_type=MESH)

    def filled(piece, target):
        known = -(-(freqs - target * GROUP) // (2 * GROUP))
        return min(PIECE, known - piece * PIECE)

    def raw_copy(piece):
        begin = piece * span
        size = min(span, freqs - begin)
        return pltpu.make_async_copy(
            spectra_ref.at[:, pl.ds(begin, size)], raw.at[:, pl.ds(begin, size)], raw_sem.at[piece]
        )

    data_copy = pltpu.make_async_copy(data_ref, series, load_sem.at[0])
    forward_copy = pltpu.make_async_copy(forward_ref.at[core], table, load_sem.at[1])
    backward_copies = [
        pltpu.make_async_copy(backward_ref.at[source], inverse.at[index], load_sem.at[2 + index])
        for index, source in enumerate((core, other_core))
    ]
    raw_copy(0).start()
    data_copy.start()
    for piece in range(1, pieces):
        raw_copy(piece).start()
    forward_copy.start()
    for backward_copy in backward_copies:
        backward_copy.start()

    raw[:, freqs:] = jnp.zeros((2, raw.shape[1] - freqs) + tuple(raw.shape[2:]), jnp.float32)
    short = filled(pieces - 1, 1)
    if short < PIECE:

        @pl.when(core == 1)
        def _():
            begin = (pieces - 1) * PIECE + short
            for owner in range(1, 3):
                kbuf[owner, :, begin:] = jnp.zeros((2, PIECE - short) + tuple(kbuf.shape[3:]), jnp.float32)


    strip = 64

    @pl.loop(0, fold.shape[1] // strip)
    def _(part):
        begin = pl.multiple_of(part * strip, strip)
        time = lax.broadcasted_iota(jnp.int32, (strip, 4 * LANES), 0) + begin
        for side in range(2):
            direct = jnp.where(time == maps_ref[3 * side : 3 * side + 1, :], 1.0, 0.0)
            sign = maps_ref[3 * side + 2 : 3 * side + 3, :].astype(jnp.float32)
            mirror = jnp.where(time == maps_ref[3 * side + 1 : 3 * side + 2, :], sign, 0.0)
            fold[side, pl.ds(begin, strip), :] = (direct + mirror).astype(jnp.bfloat16)

    upper = lax.broadcasted_iota(jnp.int32, (8, LANES), 0) < points
    stripe = lax.broadcasted_iota(jnp.int32, (8, LANES), 1) // local % 2 == 0

    def sort_piece(piece):
        @pl.loop(0, 2)
        def _(part):
            @pl.loop(piece * PIECE, (piece + 1) * PIECE)
            def _(group):
                for side in range(2):
                    for duo in range(GROUP // 2):
                        begin = group * 2 * GROUP + side * GROUP + 2 * duo
                        first = raw[part, begin]
                        second = raw[part, begin + 1]
                        low = jnp.where(upper, first, pltpu.roll(second, points, 0))
                        high = jnp.where(upper, pltpu.roll(first, points, 0), second)
                        packed[0, part, group, side, duo] = jnp.where(stripe, low, pltpu.roll(high, local, 1))
                        packed[1, part, group, side, duo] = jnp.where(stripe, pltpu.roll(high, LANES - local, 1), low)

    def k_copy(piece, target):
        begin = piece * PIECE
        size = filled(piece, target)
        rel = core if target == 0 else other_core
        return pltpu.make_async_remote_copy(
            src_ref=packed.at[1 - x, :, pl.ds(begin, size), target],
            dst_ref=kbuf.at[1 + rel, :, pl.ds(begin, size)],
            send_sem=k_send.at[target], recv_sem=k_recv.at[piece // (pieces // BATCHES)],
            device_id=(other_chip, target), device_id_type=MESH,
        )

    def k_keep(piece):
        begin = piece * PIECE
        return pltpu.make_async_remote_copy(
            src_ref=packed.at[x, :, pl.ds(begin, PIECE), other_core],
            dst_ref=kbuf.at[0, :, pl.ds(begin, PIECE)],
            send_sem=k_send.at[2], recv_sem=k_recv.at[piece // (pieces // BATCHES)],
            device_id=(me, other_core), device_id_type=MESH,
        )

    def all_of(ref, send_sem, recv_sem):
        return pltpu.make_async_remote_copy(
            src_ref=ref, dst_ref=ref, send_sem=send_sem, recv_sem=recv_sem,
            device_id=(me, other_core), device_id_type=MESH,
        )

    def wait_batch(turn):
        begin = turn * batch
        full = all_of(kbuf.at[:, :, pl.ds(begin, batch)], k_send.at[2], k_recv.at[turn])
        missing = 0 if turn + 1 < BATCHES else 2 * (PIECE - filled(pieces - 1, 1))
        if missing:
            short = all_of(packed.at[0, 0, pl.ds(0, 3 * batch - missing)], k_send.at[2], k_recv.at[turn])
            pl.when(core == 0)(full.wait_recv)
            pl.when(core == 1)(short.wait_recv)
        else:
            full.wait_recv()

    def send_piece(piece):
        for target in range(2):
            k_copy(piece, target).start()
        k_keep(piece).start()

    raw_copy(0).wait()
    sort_piece(0)
    pl.semaphore_wait(barrier, 4 + jnp.minimum(z, 1) + jnp.minimum(lines - 1 - z, 1))
    send_piece(0)

    def slot(line, row, column):
        return line * plane + row * 2 + column

    def place(line, row):
        upper_line = line // 2
        return lax.rem(line, 2) * plane + row * 2 + upper_line + x - 2 * upper_line * x

    def block(chunk, line, row, rel=0):
        position = rel * (n // 2) + place(line, row)
        return gathered.at[chunk, pl.ds(pl.multiple_of(position * local, local), local), :]

    data_copy.wait()
    plain = (((1,), (0,)), ((), ()))
    folded = []
    for side in range(2):
        values = jnp.concatenate([series[side * CHUNKS + chunk] for chunk in range(CHUNKS)], axis=0)
        high = values.astype(jnp.bfloat16)
        left = values - high.astype(jnp.float32)
        middle = left.astype(jnp.bfloat16)
        low = (left - middle.astype(jnp.float32)).astype(jnp.bfloat16)
        result = lax.dot_general(
            jnp.concatenate([high, middle, low], axis=0), fold[side, :steps, :], plain,
            preferred_element_type=jnp.float32,
        )
        size = CHUNKS * local
        folded.append(result[:size] + (result[size : 2 * size] + result[2 * size :]))
    own_row = pl.ds(pl.multiple_of(place(z, y) * local, local), local)
    for chunk in range(CHUNKS):
        even = folded[0][chunk * local : (chunk + 1) * local]
        odd = folded[1][chunk * local : (chunk + 1) * local]
        gathered[chunk, own_row, 0 : 2 * LANES] = even[:, : 2 * LANES]
        gathered[chunk, own_row, 2 * LANES : 4 * LANES] = odd[:, : 2 * LANES]
        gathered[chunk, own_row, 4 * LANES : 5 * LANES] = (
            even[:, 2 * LANES : 3 * LANES] + odd[:, 2 * LANES : 3 * LANES]
        )
        gathered[chunk, own_row, 5 * LANES : 6 * LANES] = even[:, 3 * LANES :]
        gathered[chunk, own_row, 6 * LANES :] = odd[:, 3 * LANES :]

    def send(source, target, send_sem, recv_sem):
        return pltpu.make_async_remote_copy(
            src_ref=source, dst_ref=source, send_sem=send_sem, recv_sem=recv_sem,
            device_id=target, device_id_type=MESH,
        )

    def some(blocks, send_sem, recv_sem):
        return all_of(gathered.at[0, pl.ds(0, blocks * local)], send_sem, recv_sem)

    def many(blocks, send_sem, recv_sem):
        whole = gathered.shape[1] // local
        if blocks <= whole:
            return some(blocks, send_sem, recv_sem)
        assert blocks % CHUNKS == 0
        return all_of(gathered.at[:, pl.ds(0, blocks // CHUNKS * local)], send_sem, recv_sem)

    def line_index(source, target):
        return jnp.where(source < target, source, source - 1)

    def line_copy(chunk, step, way):
        source = jnp.clip(z - way * step, 0, lines - 1)
        target = jnp.clip(z + way, 0, lines - 1)
        return send(
            block(chunk, source, y), (slot(target, y, x), core),
            z_send.at[0], z_recv.at[chunk, jnp.clip(line_index(source, target), 0, lines - 2)],
        )

    def line_arrival(chunk, step, way):
        source = jnp.clip(z - way * (step + 1), 0, lines - 1)
        target = jnp.clip(z + way, 0, lines - 1)
        return source, send(
            block(chunk, source, y), (slot(target, y, x), core),
            z_send.at[0], z_recv.at[chunk, jnp.clip(line_index(source, z), 0, lines - 2)],
        )

    def sends(step, way):
        inside = z + 1 < lines if way > 0 else z > 0
        begun = z >= step if way > 0 else z + step < lines
        return jnp.logical_and(inside, begun)

    def receives(step, way):
        return z >= step + 1 if way > 0 else z + step + 1 < lines

    def y_copy(chunk, line):
        index = jnp.where(line == z, 0, 1)
        return send(block(chunk, line, y), (y_chip, core), y_send.at[0], y_recv.at[chunk, index])

    def turn_copy(chunk):
        return send(block(chunk, z, 1 - y), (slot(z_mate, y, x), core), w_send.at[0], w_recv.at[chunk])

    def turn_arrival(chunk):
        return send(block(chunk, z_mate, 1 - y), (slot(z_mate, y, x), core), w_send.at[0], w_recv.at[chunk])

    def turns(chunk):
        return chunk >= CHUNKS // 2

    def by_row(chunk, line):
        return jnp.logical_not(jnp.logical_and(turns(chunk), line == z_mate))

    def core_copy(chunk, row, line):
        return pltpu.make_async_remote_copy(
            src_ref=block(chunk, line, row), dst_ref=block(chunk, line, row, 1),
            send_sem=c_send.at[0], recv_sem=c_recv.at[chunk],
            device_id=(me, other_core), device_id_type=MESH,
        )

    def start_lines(chunk):
        for way in (1, -1):

            @pl.when(sends(0, way))
            def _():
                line_copy(chunk, 0, way).start()

        y_copy(chunk, z).start()
        core_copy(chunk, y, z).start()

    def from_lines(chunk, step):
        for way in (1, -1):

            @pl.when(receives(step, way))
            def _():
                source, arrival = line_arrival(chunk, step, way)
                arrival.wait_recv()
                if step + 1 < lines - 1:

                    @pl.when(sends(step + 1, way))
                    def _():
                        line_copy(chunk, step + 1, way).start()

                @pl.when(by_row(chunk, source))
                def _():
                    y_copy(chunk, source).start()

                core_copy(chunk, y, source).start()

    def from_mate(chunk):
        some(1, y_send.at[0], y_recv.at[chunk, 0]).wait_recv()
        core_copy(chunk, 1 - y, z).start()

    def to_mate(chunk):
        @pl.when(turns(chunk))
        def _():
            turn_copy(chunk).start()

    def from_row(chunk):
        @pl.when(turns(chunk))
        def _():
            some(lines - 2, y_send.at[0], y_recv.at[chunk, 1]).wait_recv()
            turn_arrival(chunk).wait_recv()

        @pl.when(jnp.logical_not(turns(chunk)))
        def _():
            some(lines - 1, y_send.at[0], y_recv.at[chunk, 1]).wait_recv()

        for step in range(1, lines):
            core_copy(chunk, 1 - y, lax.rem(z + step, lines)).start()

    def from_core(chunk):
        some(n // 2, c_send.at[0], c_recv.at[chunk]).wait_recv()

    lane_index = lax.broadcasted_iota(jnp.int32, (gathered.shape[1], LANES), 1)

    def transform(chunk):
        def lanes(index):
            return gathered[chunk, :, index * LANES : (index + 1) * LANES]

        for which in range(4):
            odd = which // 2
            position = which % 2
            if which < 2:
                tail = lanes(4 + which)
            elif which == 2:
                tail = lanes(6)
            else:
                tail = jnp.where(lane_index >= rest, lanes(4), lanes(6))
            right = split(jnp.concatenate([lanes(which), tail], axis=1))
            left = jnp.concatenate([table[position], table[2 + which]], axis=1)
            result = split_product(left, count, right)
            for lane in range(2):
                spectrum[lane, pl.ds(odd * vectors + position * CHUNKS + chunk, count, stride=2 * vectors), :] = result[
                    :, lane * LANES : (lane + 1) * LANES
                ]

    pl.loop(0, CHUNKS)(start_lines)

    for piece in range(1, pieces):
        raw_copy(piece).wait()
        sort_piece(piece)
        send_piece(piece)

    forward_copy.wait()
    for backward_copy in backward_copies:
        backward_copy.wait()

    def finish(chunk):
        from_core(chunk)
        transform(chunk)

    stages = [
        (functools.partial(from_lines, step=0), 0), (from_mate, 0),
        (functools.partial(from_lines, step=1), 1), (functools.partial(from_lines, step=2), 2),
        (to_mate, 4), (from_row, 6), (finish, 7),
    ]

    @pl.loop(0, CHUNKS + 7)
    def _(turn):
        for stage, age in stages:
            chunk = turn - age

            @pl.when(jnp.logical_and(chunk >= 0, chunk < CHUNKS))
            def _():
                stage(chunk)

    columns = GROUP * 2 * vectors
    row_freq = lax.broadcasted_iota(jnp.int32, (4 * rows, columns), 0) // points % GROUP
    col_freq = lax.broadcasted_iota(jnp.int32, (4 * rows, columns), 1) // (2 * vectors)
    own = row_freq == col_freq
    lane = lax.broadcasted_iota(jnp.int32, (2 * rows, LANES), 1)
    row = lax.broadcasted_iota(jnp.int32, (2 * rows, LANES), 0) // points % 2
    first_half = lane % vectors < vectors // 2
    sign = jnp.where(first_half == (row == 0), 1.0, -1.0)
    shares = batch_shares(batch * GROUP)
    step_rows = shares[0][1]
    lane_group = lax.broadcasted_iota(jnp.int32, (step_rows, LANES), 1) // vectors
    known_rows = lax.broadcasted_iota(jnp.int32, (step_rows, LANES), 0) < shares[1][1]

    def value_rows(turn):
        return pl.ds(pl.multiple_of(turn * step_rows, GROUP), step_rows)

    def value_copy(turn, target):
        place_rows = value_rows(turn)
        return pltpu.make_async_remote_copy(
            src_ref=send_val.at[target, place_rows],
            dst_ref=recv_val.at[jnp.where(core == target, 0, 2), place_rows],
            send_sem=v_send.at[0], recv_sem=v_recv.at[0],
            device_id=(other_chip, target), device_id_type=MESH,
        )

    def value_keep(turn):
        place_rows = value_rows(turn)
        return pltpu.make_async_remote_copy(
            src_ref=send_val.at[2, place_rows], dst_ref=recv_val.at[1, place_rows],
            send_sem=v_send.at[0], recv_sem=v_recv.at[0],
            device_id=(me, other_core), device_id_type=MESH,
        )

    @pl.loop(0, BATCHES)
    def _(turn):
        for which in range(BATCHES):

            @pl.when(turn == which)
            def _():
                wait_batch(which)

        for step in range(batch):
            group = turn * batch + step
            begin = pl.multiple_of(group * columns, columns)
            right = split(
                jnp.concatenate([spectrum[0, pl.ds(begin, columns), :], spectrum[1, pl.ds(begin, columns), :]], axis=1)
            )
            parts = []
            for part in range(2):
                for near, far in (
                    (packed[x, part, group, core], kbuf[0, part, group]), (kbuf[1, part, group], kbuf[2, part, group]),
                ):
                    parts.append(jnp.concatenate([near.reshape(rows, LANES), far.reshape(rows, LANES)], axis=1))
            left = jnp.concatenate(parts, axis=0)
            found = jnp.where(own, product(split(left), right, NT_DIMS), 0.0)
            width = columns
            while width > LANES:
                width //= 2
                found = found[:, :width] + found[:, width:]
            hop = LANES // 2
            while hop >= 2 * vectors:
                found = found + pltpu.roll(found, hop, 1)
                hop //= 2
            turned = found[2 * rows :]
            turned = jnp.where(
                first_half, pltpu.roll(turned, LANES - vectors // 2, 1), pltpu.roll(turned, vectors // 2, 1)
            )
            value = found[: 2 * rows] + sign * turned
            for owner in range(2):
                product_s[owner, pl.ds(pl.multiple_of(group * rows, rows), rows), :] = value[
                    owner * rows : (owner + 1) * rows
                ]
        for owner in (1, 0):
            merged = [jnp.zeros((step_rows, LANES), jnp.float32)] * 2
            for share in range(2):
                for point in range(points):
                    begin = (turn * batch * GROUP + shares[share][0]) * points + point
                    value = product_s[owner, pl.ds(begin, step_rows, stride=points), :]
                    if share == 1:
                        value = jnp.where(known_rows, value, 0.0)
                    shifted = pltpu.roll(value, vectors, 1)
                    index = share * points + point
                    for target in range(2):
                        chosen = value if index % 2 == target else shifted
                        merged[target] = jnp.where(lane_group == index, chosen, merged[target])
            if owner == 1:
                for target in range(2):
                    send_val[target, value_rows(turn), :] = merged[target]
                for target in range(2):
                    value_copy(turn, target).start()
            else:
                send_val[2, value_rows(turn), :] = jnp.where(core == 0, merged[1], merged[0])
                own_val[value_rows(turn), :] = jnp.where(core == 0, merged[0], merged[1])
                value_keep(turn).start()

    sent = BATCHES * step_rows
    all_of(recv_val.at[:, pl.ds(0, sent)], v_send.at[0], v_recv.at[0]).wait_recv()

    own_half = vectors // 2
    blocks = []
    for near in (own_val[:sent, :] + recv_val[0, :sent, :], recv_val[1, :sent, :] + recv_val[2, :sent, :]):
        turned = jnp.concatenate([near, jnp.zeros((LANES - sent, LANES), jnp.float32)], axis=0).T
        for position in range(2):
            for share in range(2):
                begins = [
                    ((share * points + point) * 2 + position) * own_half for point in range(points)
                ]
                blocks.append(jnp.concatenate([turned[begin : begin + own_half] for begin in begins], axis=0))
    left = split(jnp.concatenate(blocks, axis=1))
    right = []
    for index in range(2):
        right.append(jnp.concatenate([inverse[near, index].reshape(4 * LANES, wide) for near in range(2)], axis=0))
    total = product(left, right, plain)
    partial[...] = total

    field_copy = pltpu.make_async_remote_copy(
        src_ref=partial, dst_ref=pair, send_sem=f_send.at[0], recv_sem=f_recv.at[0],
        device_id=(me, other_core), device_id_type=MESH,
    )

    energy = total * total
    summed = energy[:own_half]
    for point in range(1, points):
        summed = summed + energy[point * own_half : (point + 1) * own_half]
    column = jnp.sum(summed, axis=1, keepdims=True)
    lane8 = lax.broadcasted_iota(jnp.int32, (own_half, LANES), 1)
    row8 = lax.broadcasted_iota(jnp.int32, (own_half, LANES), 0)
    flat = jnp.sum(jnp.where(lane8 == row8 + core * own_half, column, 0.0), axis=0, keepdims=True)
    square[...] = flat
    mine = core * n + me
    squares[mine] = flat

    def square_copy(target, target_core):
        return pltpu.make_async_remote_copy(
            src_ref=square, dst_ref=squares.at[mine], send_sem=r_send.at[0], recv_sem=r_recv.at[0],
            device_id=(target, target_core), device_id_type=MESH,
        )

    @pl.loop(1, n)
    def _(step):
        square_copy(lax.rem(me + step, n), core).start()
        square_copy(lax.rem(me + step, n), other_core).start()

    square_copy(me, other_core).start()
    field_copy.start()

    for line in range(lines):
        ahead = line + 1 if line + 1 < lines else 0
        back = lines - line if line > 0 else 0

        @pl.when(z == line)
        def _():
            many((ahead + back) * CHUNKS, z_send.at[0], z_recv.at[0, 0]).wait_send()

    late = CHUNKS - CHUNKS // 2
    all_of(
        gathered.at[:, pl.ds(0, (lines * CHUNKS - late) * local // CHUNKS)], y_send.at[0], y_recv.at[0, 0]
    ).wait_send()
    some(late, w_send.at[0], w_recv.at[0]).wait_send()
    all_of(gathered.at[:, pl.ds(0, gathered.shape[1] // 2)], c_send.at[0], c_recv.at[0]).wait_send()
    for target in range(2):
        all_of(packed.at[0, :, pl.ds(0, groups - PIECE + filled(pieces - 1, target)), target],
               k_send.at[target], k_recv.at[0]).wait_send()
    all_of(packed.at[0, :, :, 0], k_send.at[2], k_recv.at[0]).wait_send()
    all_of(send_val.at[:, pl.ds(0, sent)], v_send.at[0], v_recv.at[0]).wait_send()
    field_copy.wait_send()

    field_copy.wait_recv()
    tall = points * own_half
    out_ref[pl.ds(pl.multiple_of(core * tall, tall), tall), :] = total
    out_ref[pl.ds(pl.multiple_of(other_core * tall, tall), tall), :] = pair[...]
    all_of(squares.at[pl.ds(0, 2 * n - 1)], r_send.at[0], r_recv.at[0]).wait()

    energy_all = squares[0]
    for device in range(1, 2 * n):
        energy_all = energy_all + squares[device]
    scale = jnp.sqrt(energy_all / (points * n * steps) + 1e-06)
    rms_ref[...] = jnp.broadcast_to(scale, rms_ref.shape)


def finish_kernel(field_ref, scale_ref, out_ref, rms_ref):
    vectors, points, steps = out_ref.shape
    scale = scale_ref[:1]
    rms_ref[...] = scale[0, :vectors]
    diagonal = lax.broadcasted_iota(jnp.int32, (vectors, LANES), 0) == lax.broadcasted_iota(
        jnp.int32, (vectors, LANES), 1
    )
    spread = jnp.broadcast_to(scale, (vectors, LANES))
    divisor = jnp.sum(jnp.where(diagonal, spread, 0.0), axis=1, keepdims=True)
    half = vectors // 2
    for point in range(points):
        near = field_ref[point * half : (point + 1) * half, :steps]
        far = field_ref[(points + point) * half : (points + point + 1) * half, :steps]
        out_ref[:, point, :] = jnp.concatenate([near, far], axis=0) / divisor


def paired_body(data, spectra):
    n = lax.axis_size("param")
    vectors, local, steps = data.shape
    sensors, points, freqs = spectra.shape[1:]
    wide = -(-steps // LANES) * LANES
    groups = -(-freqs // (2 * GROUP))
    count = groups * GROUP
    rows_pad = -(-count // 16) * 16
    pieces = groups // PIECE
    lines = n // 4
    forward, backward = paired_tables(steps, freqs, groups, rows_pad, wide)
    maps = fold_maps(steps)

    turned = jnp.transpose(spectra, (0, 3, 2, 1)).reshape(2, freqs, points, 2, LANES)
    turned = jnp.transpose(turned, (0, 1, 3, 2, 4)).reshape(2, freqs, 2 * points, LANES)

    hbm = pl.BlockSpec(memory_space=pl.ANY)
    vmem = pl.BlockSpec(memory_space=pltpu.VMEM)
    dma = pltpu.SemaphoreType.DMA
    f32, bf16 = jnp.float32, jnp.bfloat16
    fields, scale = pl.pallas_call(
        functools.partial(kernel, n, lines, vectors, local, steps, points, freqs, groups, wide),
        out_shape=(
            pltpu.VMEM((points * vectors, wide), f32),
            pltpu.VMEM((8, LANES), f32),
        ),
        in_specs=[hbm, hbm, hbm, hbm, vmem],
        out_specs=(vmem, vmem),
        scratch_shapes=[
            pltpu.VMEM((vectors, local, steps), f32),
            pltpu.VMEM((2, wide, 4 * LANES), bf16),
            pltpu.VMEM((2, 2 * count, 2 * points, LANES), f32),
            pltpu.VMEM((2, 2, groups, 2, GROUP // 2, 2 * points, LANES), f32),
            pltpu.VMEM((3, 2, groups, GROUP // 2, 2 * points, LANES), f32),
            pltpu.VMEM((CHUNKS, sensors, 7 * LANES), f32),
            pltpu.VMEM((6, 2 * rows_pad, LANES), bf16),
            pltpu.VMEM((2, 2, 2, 2, LANES, wide), bf16),
            pltpu.VMEM((2, count * 2 * vectors, LANES), f32),
            pltpu.VMEM((2, (count + GROUP) * points, LANES), f32),
            pltpu.VMEM((LANES, LANES), f32),
            pltpu.VMEM((3, LANES, LANES), f32),
            pltpu.VMEM((3, LANES, LANES), f32),
            pltpu.VMEM((points * vectors // 2, wide), f32),
            pltpu.VMEM((points * vectors // 2, wide), f32),
            pltpu.VMEM((1, LANES), f32),
            pltpu.VMEM((2 * n, 1, LANES), f32),
            dma((4,)),
            dma((pieces,)),
            dma((3,)), dma((BATCHES,)),
            dma((1,)), dma((CHUNKS, lines - 1)),
            dma((1,)), dma((CHUNKS, 2)),
            dma((1,)), dma((CHUNKS,)),
            dma((1,)), dma((CHUNKS,)),
            dma((1,)), dma((1,)),
            dma((1,)), dma((1,)),
            dma((1,)), dma((1,)),
        ],
        compiler_params=pltpu.CompilerParams(
            collective_id=0, has_side_effects=True, vmem_limit_bytes=60 * 1024 * 1024
        ),
    )(data, turned, jnp.asarray(forward), jnp.asarray(backward), jnp.asarray(maps))
    return pl.pallas_call(
        finish_kernel,
        out_shape=(jax.ShapeDtypeStruct((vectors, points, steps), f32), jax.ShapeDtypeStruct((vectors,), f32)),
        in_specs=[vmem, vmem],
        out_specs=(vmem, vmem),
    )(pltpu.with_memory_space_constraint(fields, pltpu.VMEM), pltpu.with_memory_space_constraint(scale, pltpu.VMEM))


def solution(mesh):
    in_specs = (P(None, ("sensor", "param"), None), P(None, "sensor", "param", None))
    out_specs = (P(None, "param", None), P())
    n = mesh.shape["param"]
    pair = mesh.shape["sensor"] == 2 and n == 16

    def body(data, spectra):
        vectors, local, _ = data.shape
        sensors, points = spectra.shape[1:3]
        fits = local * n == sensors and local % 8 == 0 and sensors == 2 * LANES and vectors == 2 * CHUNKS
        fits = fits and points * 2 * vectors == LANES and folded_layout_fits(data.shape[2])
        return (paired_body if pair and fits else general_body)(data, spectra)

    return jax.shard_map(body, mesh=mesh, in_specs=in_specs, out_specs=out_specs, check_vma=False)
```

```python
import functools
import math

import jax
import jax.numpy as jnp
import numpy as np
from jax import lax
from jax.experimental import pallas as pl
from jax.experimental.pallas import tpu as pltpu
from jax.sharding import PartitionSpec as P

MESH = pl.DeviceIdType.MESH
LANES = 128
GROUP = 8
CHUNKS = 8
PIECE = 3
BATCHES = 3


def spectral_tables(steps):
    length = 2 * steps
    freqs = steps + 1
    times = lax.broadcasted_iota(jnp.int32, (steps, freqs), 0)
    bins = lax.broadcasted_iota(jnp.int32, (steps, freqs), 1)
    phase = 2.0 * math.pi / length * (times * bins % length).astype(jnp.float32)
    forward = jnp.concatenate([jnp.cos(phase), -jnp.sin(phase)], axis=1)
    weight = jnp.where((bins == 0) | (bins == steps), 1.0, 2.0) / length
    backward = jnp.concatenate([(weight * jnp.cos(phase)).T, (-weight * jnp.sin(phase)).T], axis=0)
    return (forward, backward)


def to_spectrum(series, forward):
    vectors, sensors, steps = series.shape
    flat = jnp.dot(
        series.reshape(vectors * sensors, steps),
        forward,
        precision=lax.Precision.HIGHEST,
        preferred_element_type=jnp.float32,
    )
    return flat.reshape(vectors, sensors, forward.shape[1])


def contract(kernel, spectrum):
    return jnp.einsum(
        "spf,rsf->rpf",
        kernel,
        spectrum,
        precision=lax.Precision.HIGHEST,
        preferred_element_type=jnp.float32,
    )


def general_body(data, spectra):
    steps = data.shape[2]
    freqs = steps + 1
    forward, backward = spectral_tables(steps)
    whole = to_spectrum(lax.all_gather(data, "param", axis=1, tiled=True), forward)
    real_part = whole[..., :freqs]
    imag_part = whole[..., freqs:]
    kernel_re = spectra[0]
    kernel_im = spectra[1]
    out_re = contract(kernel_re, real_part) + contract(kernel_im, imag_part)
    out_im = contract(kernel_re, imag_part) - contract(kernel_im, real_part)
    vectors, points = (out_re.shape[0], out_re.shape[1])
    stacked = jnp.concatenate([out_re, out_im], axis=2).reshape(vectors * points, 2 * freqs)
    partial_field = jnp.dot(
        stacked, backward, precision=lax.Precision.HIGHEST, preferred_element_type=jnp.float32
    ).reshape(vectors, points, steps)
    count = points * lax.axis_size("param") * steps
    share = lax.psum_scatter(partial_field, "sensor", scatter_dimension=0, tiled=True)
    squares = lax.psum(jnp.sum(share * share, axis=(1, 2)), "param")
    scale = jnp.sqrt(squares / count + 1e-06)
    normalized = share / scale[:, None, None]
    gradient, rms_all = (
        lax.all_gather(normalized, "sensor", axis=0, tiled=True),
        lax.all_gather(scale, "sensor", axis=0, tiled=True),
    )
    return (gradient, rms_all)


def split(value):
    high = value.astype(jnp.bfloat16)
    return high, (value - high.astype(jnp.float32)).astype(jnp.bfloat16)


NT_DIMS = (((1,), (1,)), ((), ()))


def product(left, right, dims):
    dot = functools.partial(lax.dot_general, dimension_numbers=dims, preferred_element_type=jnp.float32)
    size = left[0].shape[0]
    both = dot(jnp.concatenate(left, axis=0), right[0])
    return both[:size] + (both[size:] + dot(left[0], right[1]))


def split_product(table, rows, right):
    dot = functools.partial(lax.dot_general, dimension_numbers=NT_DIMS, preferred_element_type=jnp.float32)
    half = table.shape[0] // 2
    both = dot(table, right[0])
    return both[:rows] + (both[half : half + rows] + dot(table[:half], right[1])[:rows])


def folded_layout_fits(steps):
    half = steps // 2
    rest = half + 1 - LANES
    groups = -(-(steps + 1) // (2 * GROUP))
    fits = steps % 2 == 0 and 0 < rest < LANES and half - LANES - (LANES - rest) <= LANES - rest
    fits = fits and groups % (PIECE * BATCHES) == 0
    return fits and BATCHES * batch_shares(groups // BATCHES * GROUP)[0][1] <= LANES


def frequency_order(freqs, groups):
    bins = np.arange(groups * 2 * GROUP).reshape(groups, 2, GROUP)
    return [bins[:, core].reshape(-1) for core in range(2)]


def lane_times(steps):
    half = steps // 2
    rest = half + 1 - LANES
    room = LANES - rest
    lane = np.arange(LANES)
    first = np.where(lane < rest, LANES + lane, -1)
    first_odd = np.where(lane < rest - 1, LANES + lane, -1)
    second = np.where(lane >= room, LANES + lane - room, -1)
    tail_a = np.where(lane >= rest, LANES + lane - rest, -1)
    tail_b = np.where(lane < rest - 1 - room, LANES + room + lane, -1)
    return lane, first, first_odd, second, tail_a, tail_b


def fold_maps(steps):
    lane, first, first_odd, second, tail_a, tail_b = lane_times(steps)
    shared = np.where(second >= 0, second, tail_b)
    even = np.concatenate([lane, lane, first, first_odd])
    odd = np.concatenate([lane, lane, tail_a, shared])
    ones = np.ones(LANES, np.int64)
    even_sign = np.concatenate([ones, -ones, ones, -ones])
    odd_sign = np.concatenate([ones, -ones, -ones, np.where(second >= 0, 1, -1)])
    maps = np.full((8, 4 * LANES), -1, np.int32)
    for index, (time, sign) in enumerate(((even, even_sign), (odd, odd_sign))):
        mirror = np.where((time > 0) & (2 * time != steps), steps - time, -1)
        maps[3 * index] = time
        maps[3 * index + 1] = np.where(time < 0, -1, mirror)
        maps[3 * index + 2] = sign
    return maps


def halves(values):
    high = values.astype(jnp.bfloat16)
    return high, (values - high.astype(np.float32)).astype(jnp.bfloat16)


def batch_shares(batch):
    first = -(-batch // (2 * GROUP)) * GROUP
    return ((0, first), (first, batch - first))


def paired_tables(steps, freqs, groups, rows_pad, wide):
    half = steps // 2
    lane, first, first_odd, second, tail_a, tail_b = lane_times(steps)
    tail = np.where(tail_a >= 0, tail_a, tail_b)
    forward, backward = [], []
    for bins in frequency_order(freqs, groups):
        count = bins.shape[0]
        known = (bins < freqs)[:, None]
        even = (bins % 2 == 0)[:, None]
        angle = bins[:, None] * np.arange(steps)[None, :] % (2 * steps)
        phase = np.pi / steps * angle
        sine = np.where(angle % steps == 0, 0.0, np.sin(phase))
        cosine = np.cos(phase)
        symmetric = np.where(known, np.where(even, cosine, -sine), 0.0)
        other = np.where(known, np.where(even, -sine, cosine), 0.0)
        blocks = []
        for table, times in (
            (symmetric, lane), (other, lane), (symmetric, first), (other, first_odd), (symmetric, second), (other, tail),
        ):
            limit = half if table is symmetric else half - 1
            inside = (times >= 0) & (times <= limit)
            value = np.where(inside[None, :], table[:, np.clip(times, 0, limit)], 0.0).astype(np.float32)
            block = np.zeros((2, rows_pad, LANES), jnp.bfloat16)
            block[0, :count], block[1, :count] = halves(value)
            blocks.append(block.reshape(2 * rows_pad, LANES))
        forward.append(np.stack(blocks))
        weight = np.where((bins == 0) | (bins == steps), 0.5, 1.0)[:, None] / steps
        inverse = np.zeros((2, 2, 2, LANES, wide), jnp.bfloat16)
        batch = groups // BATCHES * GROUP
        for position, table in enumerate((symmetric, other)):
            value = (table * weight).astype(np.float32)
            for turn in range(BATCHES):
                for share, (begin, size) in enumerate(batch_shares(batch)):
                    target = slice(turn * batch_shares(batch)[0][1], turn * batch_shares(batch)[0][1] + size)
                    source = slice(turn * batch + begin, turn * batch + begin + size)
                    parts = halves(value[source])
                    for index in range(2):
                        inverse[index, position, share, target, :steps] = parts[index]
        backward.append(inverse)
    return np.stack(forward), np.stack(backward)


def kernel(
    n, lines, vectors, local, steps, points, freqs, groups, wide,
    data_ref, spectra_ref, forward_ref, backward_ref, maps_ref,
    out_ref, rms_ref,
    series, fold, raw, packed, kbuf, gathered, table, inverse, spectrum, product_s, own_val, send_val, recv_val,
    partial, pair, square, squares,
    load_sem, raw_sem, k_send, k_recv, z_send, z_recv, y_send, y_recv, c_send, c_recv, w_send, w_recv,
    v_send, v_recv, f_send, f_recv, r_send, r_recv,
):
    me = lax.axis_index("param")
    core = lax.axis_index("sensor")
    x = lax.rem(me, 2)
    y = lax.rem(me // 2, 2)
    z = me // 4
    plane = 4
    other_chip = me + 1 - 2 * x
    y_chip = me + 2 - 4 * y
    other_core = 1 - core
    z_mate = z + 1 - 2 * lax.rem(z, 2)
    half = steps // 2
    rest = half + 1 - LANES
    rows = points * GROUP
    count = groups * GROUP
    pieces = groups // PIECE
    span = PIECE * 2 * GROUP
    batch = groups // BATCHES

    barrier = pltpu.get_barrier_semaphore()

    for neighbour in ((other_chip, core), (other_chip, other_core), (y_chip, core), (me, other_core)):
        pl.semaphore_signal(barrier, inc=1, device_id=neighbour, device_id_type=MESH)

    @pl.when(z > 0)
    def _():
        pl.semaphore_signal(barrier, inc=1, device_id=(me - plane, core), device_id_type=MESH)

    @pl.when(z + 1 < lines)
    def _():
        pl.semaphore_signal(barrier, inc=1, device_id=(me + plane, core), device_id_type=MESH)

    def filled(piece, target):
        known = -(-(freqs - target * GROUP) // (2 * GROUP))
        return min(PIECE, known - piece * PIECE)

    def raw_copy(piece):
        begin = piece * span
        size = min(span, freqs - begin)
        return pltpu.make_async_copy(
            spectra_ref.at[:, pl.ds(begin, size)], raw.at[:, pl.ds(begin, size)], raw_sem.at[piece]
        )

    data_copy = pltpu.make_async_copy(data_ref, series, load_sem.at[0])
    forward_copy = pltpu.make_async_copy(forward_ref.at[core], table, load_sem.at[1])
    backward_copies = [
        pltpu.make_async_copy(backward_ref.at[source], inverse.at[index], load_sem.at[2 + index])
        for index, source in enumerate((core, other_core))
    ]
    data_copy.start()
    raw_copy(0).start()
    for piece in range(1, pieces):
        raw_copy(piece).start()
    forward_copy.start()
    for backward_copy in backward_copies:
        backward_copy.start()

    strip = 64

    @pl.loop(0, fold.shape[1] // strip)
    def _(part):
        begin = pl.multiple_of(part * strip, strip)
        time = lax.broadcasted_iota(jnp.int32, (strip, 4 * LANES), 0) + begin
        for side in range(2):
            direct = jnp.where(time == maps_ref[3 * side : 3 * side + 1, :], 1.0, 0.0)
            sign = maps_ref[3 * side + 2 : 3 * side + 3, :].astype(jnp.float32)
            mirror = jnp.where(time == maps_ref[3 * side + 1 : 3 * side + 2, :], sign, 0.0)
            fold[side, pl.ds(begin, strip), :] = (direct + mirror).astype(jnp.bfloat16)

    upper = lax.broadcasted_iota(jnp.int32, (8, LANES), 0) < points
    stripe = lax.broadcasted_iota(jnp.int32, (8, LANES), 1) // local % 2 == 0

    def sort_piece(piece):
        @pl.loop(0, 2)
        def _(part):
            @pl.loop(piece * PIECE, (piece + 1) * PIECE)
            def _(group):
                for side in range(2):
                    for duo in range(GROUP // 2):
                        begin = group * 2 * GROUP + side * GROUP + 2 * duo
                        first = raw[part, begin]
                        second = raw[part, begin + 1]
                        low = jnp.where(upper, first, pltpu.roll(second, points, 0))
                        high = jnp.where(upper, pltpu.roll(first, points, 0), second)
                        packed[0, part, group, side, duo] = jnp.where(stripe, low, pltpu.roll(high, local, 1))
                        packed[1, part, group, side, duo] = jnp.where(stripe, pltpu.roll(high, LANES - local, 1), low)

    def k_copy(piece, target):
        begin = piece * PIECE
        size = filled(piece, target)
        rel = core if target == 0 else other_core
        return pltpu.make_async_remote_copy(
            src_ref=packed.at[1 - x, :, pl.ds(begin, size), target],
            dst_ref=kbuf.at[1 + rel, :, pl.ds(begin, size)],
            send_sem=k_send.at[target], recv_sem=k_recv.at[piece // (pieces // BATCHES)],
            device_id=(other_chip, target), device_id_type=MESH,
        )

    def k_keep(piece):
        begin = piece * PIECE
        return pltpu.make_async_remote_copy(
            src_ref=packed.at[x, :, pl.ds(begin, PIECE), other_core],
            dst_ref=kbuf.at[0, :, pl.ds(begin, PIECE)],
            send_sem=k_send.at[2], recv_sem=k_recv.at[piece // (pieces // BATCHES)],
            device_id=(me, other_core), device_id_type=MESH,
        )

    def all_of(ref, send_sem, recv_sem):
        return pltpu.make_async_remote_copy(
            src_ref=ref, dst_ref=ref, send_sem=send_sem, recv_sem=recv_sem,
            device_id=(me, other_core), device_id_type=MESH,
        )

    def wait_batch(turn):
        begin = turn * batch
        full = all_of(kbuf.at[:, :, pl.ds(begin, batch)], k_send.at[2], k_recv.at[turn])
        missing = 0 if turn + 1 < BATCHES else 2 * (PIECE - filled(pieces - 1, 1))
        if missing:
            short = all_of(packed.at[0, 0, pl.ds(0, 3 * batch - missing)], k_send.at[2], k_recv.at[turn])
            pl.when(core == 0)(full.wait_recv)
            pl.when(core == 1)(short.wait_recv)
        else:
            full.wait_recv()

    def send_piece(piece):
        for target in range(2):
            k_copy(piece, target).start()
        k_keep(piece).start()

    def slot(line, row, column):
        return line * plane + row * 2 + column

    def place(line, row):
        upper_line = line // 2
        return lax.rem(line, 2) * plane + row * 2 + upper_line + x - 2 * upper_line * x

    def block(chunk, line, row, rel=0):
        position = rel * (n // 2) + place(line, row)
        return gathered.at[chunk, pl.ds(pl.multiple_of(position * local, local), local), :]

    data_copy.wait()
    plain = (((1,), (0,)), ((), ()))
    folded = []
    for side in range(2):
        values = jnp.concatenate([series[side * CHUNKS + chunk] for chunk in range(CHUNKS)], axis=0)
        high = values.astype(jnp.bfloat16)
        left = values - high.astype(jnp.float32)
        middle = left.astype(jnp.bfloat16)
        low = (left - middle.astype(jnp.float32)).astype(jnp.bfloat16)
        result = lax.dot_general(
            jnp.concatenate([high, middle, low], axis=0), fold[side, :steps, :], plain,
            preferred_element_type=jnp.float32,
        )
        size = CHUNKS * local
        folded.append(result[:size] + (result[size : 2 * size] + result[2 * size :]))
    own_row = pl.ds(pl.multiple_of(place(z, y) * local, local), local)
    for chunk in range(CHUNKS):
        even = folded[0][chunk * local : (chunk + 1) * local]
        odd = folded[1][chunk * local : (chunk + 1) * local]
        gathered[chunk, own_row, 0 : 2 * LANES] = even[:, : 2 * LANES]
        gathered[chunk, own_row, 2 * LANES : 4 * LANES] = odd[:, : 2 * LANES]
        gathered[chunk, own_row, 4 * LANES : 5 * LANES] = (
            even[:, 2 * LANES : 3 * LANES] + odd[:, 2 * LANES : 3 * LANES]
        )
        gathered[chunk, own_row, 5 * LANES : 6 * LANES] = even[:, 3 * LANES :]
        gathered[chunk, own_row, 6 * LANES :] = odd[:, 3 * LANES :]

    def send(source, target, send_sem, recv_sem):
        return pltpu.make_async_remote_copy(
            src_ref=source, dst_ref=source, send_sem=send_sem, recv_sem=recv_sem,
            device_id=target, device_id_type=MESH,
        )

    def some(blocks, send_sem, recv_sem):
        return all_of(gathered.at[0, pl.ds(0, blocks * local)], send_sem, recv_sem)

    def many(blocks, send_sem, recv_sem):
        whole = gathered.shape[1] // local
        if blocks <= whole:
            return some(blocks, send_sem, recv_sem)
        assert blocks % CHUNKS == 0
        return all_of(gathered.at[:, pl.ds(0, blocks // CHUNKS * local)], send_sem, recv_sem)

    def line_index(source, target):
        return jnp.where(source < target, source, source - 1)

    def line_copy(chunk, step, way):
        source = jnp.clip(z - way * step, 0, lines - 1)
        target = jnp.clip(z + way, 0, lines - 1)
        return send(
            block(chunk, source, y), (slot(target, y, x), core),
            z_send.at[0], z_recv.at[chunk, jnp.clip(line_index(source, target), 0, lines - 2)],
        )

    def line_arrival(chunk, step, way):
        source = jnp.clip(z - way * (step + 1), 0, lines - 1)
        target = jnp.clip(z + way, 0, lines - 1)
        return source, send(
            block(chunk, source, y), (slot(target, y, x), core),
            z_send.at[0], z_recv.at[chunk, jnp.clip(line_index(source, z), 0, lines - 2)],
        )

    def sends(step, way):
        inside = z + 1 < lines if way > 0 else z > 0
        begun = z >= step if way > 0 else z + step < lines
        return jnp.logical_and(inside, begun)

    def receives(step, way):
        return z >= step + 1 if way > 0 else z + step + 1 < lines

    def y_copy(chunk, line):
        index = jnp.where(line == z, 0, 1)
        return send(block(chunk, line, y), (y_chip, core), y_send.at[0], y_recv.at[chunk, index])

    def turn_copy(chunk):
        return send(block(chunk, z, 1 - y), (slot(z_mate, y, x), core), w_send.at[0], w_recv.at[chunk])

    def turn_arrival(chunk):
        return send(block(chunk, z_mate, 1 - y), (slot(z_mate, y, x), core), w_send.at[0], w_recv.at[chunk])

    def turns(chunk):
        return chunk >= CHUNKS // 2

    def by_row(chunk, line):
        return jnp.logical_not(jnp.logical_and(turns(chunk), line == z_mate))

    def core_copy(chunk, row, line):
        return pltpu.make_async_remote_copy(
            src_ref=block(chunk, line, row), dst_ref=block(chunk, line, row, 1),
            send_sem=c_send.at[0], recv_sem=c_recv.at[chunk],
            device_id=(me, other_core), device_id_type=MESH,
        )

    def start_lines(chunk):
        for way in (1, -1):

            @pl.when(sends(0, way))
            def _():
                line_copy(chunk, 0, way).start()

        y_copy(chunk, z).start()
        core_copy(chunk, y, z).start()

    def from_lines(chunk, step):
        for way in (1, -1):

            @pl.when(receives(step, way))
            def _():
                source, arrival = line_arrival(chunk, step, way)
                arrival.wait_recv()
                if step + 1 < lines - 1:

                    @pl.when(sends(step + 1, way))
                    def _():
                        line_copy(chunk, step + 1, way).start()

                @pl.when(by_row(chunk, source))
                def _():
                    y_copy(chunk, source).start()

                core_copy(chunk, y, source).start()

    def from_mate(chunk):
        some(1, y_send.at[0], y_recv.at[chunk, 0]).wait_recv()
        core_copy(chunk, 1 - y, z).start()

    def to_mate(chunk):
        @pl.when(turns(chunk))
        def _():
            turn_copy(chunk).start()

    def from_row(chunk):
        @pl.when(turns(chunk))
        def _():
            some(lines - 2, y_send.at[0], y_recv.at[chunk, 1]).wait_recv()
            turn_arrival(chunk).wait_recv()

        @pl.when(jnp.logical_not(turns(chunk)))
        def _():
            some(lines - 1, y_send.at[0], y_recv.at[chunk, 1]).wait_recv()

        for step in range(1, lines):
            core_copy(chunk, 1 - y, lax.rem(z + step, lines)).start()

    def from_core(chunk):
        some(n // 2, c_send.at[0], c_recv.at[chunk]).wait_recv()

    lane_index = lax.broadcasted_iota(jnp.int32, (gathered.shape[1], LANES), 1)

    def transform(chunk):
        def lanes(index):
            return gathered[chunk, :, index * LANES : (index + 1) * LANES]

        for which in range(4):
            odd = which // 2
            position = which % 2
            if which < 2:
                tail = lanes(4 + which)
            elif which == 2:
                tail = lanes(6)
            else:
                tail = jnp.where(lane_index >= rest, lanes(4), lanes(6))
            right = split(jnp.concatenate([lanes(which), tail], axis=1))
            left = jnp.concatenate([table[position], table[2 + which]], axis=1)
            result = split_product(left, count, right)
            for lane in range(2):
                spectrum[lane, pl.ds(odd * vectors + position * CHUNKS + chunk, count, stride=2 * vectors), :] = result[
                    :, lane * LANES : (lane + 1) * LANES
                ]

    pl.semaphore_wait(barrier, 4 + jnp.minimum(z, 1) + jnp.minimum(lines - 1 - z, 1))
    pl.loop(0, CHUNKS)(start_lines)

    raw[:, freqs:] = jnp.zeros((2, raw.shape[1] - freqs) + tuple(raw.shape[2:]), jnp.float32)
    short = filled(pieces - 1, 1)
    if short < PIECE:

        @pl.when(core == 1)
        def _():
            begin = (pieces - 1) * PIECE + short
            for owner in range(1, 3):
                kbuf[owner, :, begin:] = jnp.zeros((2, PIECE - short) + tuple(kbuf.shape[3:]), jnp.float32)


    for piece in range(pieces):
        raw_copy(piece).wait()
        sort_piece(piece)
        send_piece(piece)

    forward_copy.wait()
    for backward_copy in backward_copies:
        backward_copy.wait()

    def finish(chunk):
        from_core(chunk)
        transform(chunk)

    stages = [
        (functools.partial(from_lines, step=0), 0), (from_mate, 0),
        (functools.partial(from_lines, step=1), 1), (functools.partial(from_lines, step=2), 2), (to_mate, 3),
        (from_row, 5), (finish, 6),
    ]

    @pl.loop(0, CHUNKS + stages[-1][1])
    def _(turn):
        for stage, age in stages:
            chunk = turn - age

            @pl.when(jnp.logical_and(chunk >= 0, chunk < CHUNKS))
            def _():
                stage(chunk)

    columns = GROUP * 2 * vectors
    row_freq = lax.broadcasted_iota(jnp.int32, (4 * rows, columns), 0) // points % GROUP
    col_freq = lax.broadcasted_iota(jnp.int32, (4 * rows, columns), 1) // (2 * vectors)
    own = row_freq == col_freq
    lane = lax.broadcasted_iota(jnp.int32, (2 * rows, LANES), 1)
    row = lax.broadcasted_iota(jnp.int32, (2 * rows, LANES), 0) // points % 2
    first_half = lane % vectors < vectors // 2
    sign = jnp.where(first_half == (row == 0), 1.0, -1.0)
    shares = batch_shares(batch * GROUP)
    step_rows = shares[0][1]
    lane_group = lax.broadcasted_iota(jnp.int32, (step_rows, LANES), 1) // vectors
    known_rows = lax.broadcasted_iota(jnp.int32, (step_rows, LANES), 0) < shares[1][1]

    def value_rows(turn):
        return pl.ds(pl.multiple_of(turn * step_rows, GROUP), step_rows)

    def value_copy(turn, target):
        place_rows = value_rows(turn)
        return pltpu.make_async_remote_copy(
            src_ref=send_val.at[target, place_rows],
            dst_ref=recv_val.at[jnp.where(core == target, 0, 2), place_rows],
            send_sem=v_send.at[0], recv_sem=v_recv.at[0],
            device_id=(other_chip, target), device_id_type=MESH,
        )

    def value_keep(turn):
        place_rows = value_rows(turn)
        return pltpu.make_async_remote_copy(
            src_ref=send_val.at[2, place_rows], dst_ref=recv_val.at[1, place_rows],
            send_sem=v_send.at[0], recv_sem=v_recv.at[0],
            device_id=(me, other_core), device_id_type=MESH,
        )

    @pl.loop(0, BATCHES)
    def _(turn):
        for which in range(BATCHES):

            @pl.when(turn == which)
            def _():
                wait_batch(which)

        for step in range(batch):
            group = turn * batch + step
            begin = pl.multiple_of(group * columns, columns)
            right = split(
                jnp.concatenate([spectrum[0, pl.ds(begin, columns), :], spectrum[1, pl.ds(begin, columns), :]], axis=1)
            )
            parts = []
            for part in range(2):
                for near, far in (
                    (packed[x, part, group, core], kbuf[0, part, group]), (kbuf[1, part, group], kbuf[2, part, group]),
                ):
                    parts.append(jnp.concatenate([near.reshape(rows, LANES), far.reshape(rows, LANES)], axis=1))
            left = jnp.concatenate(parts, axis=0)
            found = jnp.where(own, product(split(left), right, NT_DIMS), 0.0)
            width = columns
            while width > LANES:
                width //= 2
                found = found[:, :width] + found[:, width:]
            hop = LANES // 2
            while hop >= 2 * vectors:
                found = found + pltpu.roll(found, hop, 1)
                hop //= 2
            turned = found[2 * rows :]
            turned = jnp.where(
                first_half, pltpu.roll(turned, LANES - vectors // 2, 1), pltpu.roll(turned, vectors // 2, 1)
            )
            value = found[: 2 * rows] + sign * turned
            for owner in range(2):
                product_s[owner, pl.ds(pl.multiple_of(group * rows, rows), rows), :] = value[
                    owner * rows : (owner + 1) * rows
                ]
        for owner in (1, 0):
            merged = [jnp.zeros((step_rows, LANES), jnp.float32)] * 2
            for share in range(2):
                for point in range(points):
                    begin = (turn * batch * GROUP + shares[share][0]) * points + point
                    value = product_s[owner, pl.ds(begin, step_rows, stride=points), :]
                    if share == 1:
                        value = jnp.where(known_rows, value, 0.0)
                    shifted = pltpu.roll(value, vectors, 1)
                    index = share * points + point
                    for target in range(2):
                        chosen = value if index % 2 == target else shifted
                        merged[target] = jnp.where(lane_group == index, chosen, merged[target])
            if owner == 1:
                for target in range(2):
                    send_val[target, value_rows(turn), :] = merged[target]
                for target in range(2):
                    value_copy(turn, target).start()
            else:
                send_val[2, value_rows(turn), :] = jnp.where(core == 0, merged[1], merged[0])
                own_val[value_rows(turn), :] = jnp.where(core == 0, merged[0], merged[1])
                value_keep(turn).start()

    sent = BATCHES * step_rows
    all_of(recv_val.at[:, pl.ds(0, sent)], v_send.at[0], v_recv.at[0]).wait_recv()

    own_half = vectors // 2
    blocks = []
    for near in (own_val[:sent, :] + recv_val[0, :sent, :], recv_val[1, :sent, :] + recv_val[2, :sent, :]):
        turned = jnp.concatenate([near, jnp.zeros((LANES - sent, LANES), jnp.float32)], axis=0).T
        for position in range(2):
            for share in range(2):
                begins = [
                    ((share * points + point) * 2 + position) * own_half for point in range(points)
                ]
                blocks.append(jnp.concatenate([turned[begin : begin + own_half] for begin in begins], axis=0))
    left = split(jnp.concatenate(blocks, axis=1))
    right = []
    for index in range(2):
        right.append(jnp.concatenate([inverse[near, index].reshape(4 * LANES, wide) for near in range(2)], axis=0))
    total = product(left, right, plain)
    partial[...] = total

    field_copy = pltpu.make_async_remote_copy(
        src_ref=partial, dst_ref=pair, send_sem=f_send.at[0], recv_sem=f_recv.at[0],
        device_id=(me, other_core), device_id_type=MESH,
    )

    energy = total * total
    summed = energy[:own_half]
    for point in range(1, points):
        summed = summed + energy[point * own_half : (point + 1) * own_half]
    column = jnp.sum(summed, axis=1, keepdims=True)
    lane8 = lax.broadcasted_iota(jnp.int32, (own_half, LANES), 1)
    row8 = lax.broadcasted_iota(jnp.int32, (own_half, LANES), 0)
    flat = jnp.sum(jnp.where(lane8 == row8 + core * own_half, column, 0.0), axis=0, keepdims=True)
    square[...] = flat
    mine = core * n + me
    squares[mine] = flat

    def square_copy(target, target_core):
        return pltpu.make_async_remote_copy(
            src_ref=square, dst_ref=squares.at[mine], send_sem=r_send.at[0], recv_sem=r_recv.at[0],
            device_id=(target, target_core), device_id_type=MESH,
        )

    @pl.loop(1, n)
    def _(step):
        square_copy(lax.rem(me + step, n), core).start()
        square_copy(lax.rem(me + step, n), other_core).start()

    square_copy(me, other_core).start()
    field_copy.start()

    for line in range(lines):
        ahead = line + 1 if line + 1 < lines else 0
        back = lines - line if line > 0 else 0

        @pl.when(z == line)
        def _():
            many((ahead + back) * CHUNKS, z_send.at[0], z_recv.at[0, 0]).wait_send()

    late = CHUNKS - CHUNKS // 2
    all_of(
        gathered.at[:, pl.ds(0, (lines * CHUNKS - late) * local // CHUNKS)], y_send.at[0], y_recv.at[0, 0]
    ).wait_send()
    some(late, w_send.at[0], w_recv.at[0]).wait_send()
    all_of(gathered.at[:, pl.ds(0, gathered.shape[1] // 2)], c_send.at[0], c_recv.at[0]).wait_send()
    for target in range(2):
        all_of(packed.at[0, :, pl.ds(0, groups - PIECE + filled(pieces - 1, target)), target],
               k_send.at[target], k_recv.at[0]).wait_send()
    all_of(packed.at[0, :, :, 0], k_send.at[2], k_recv.at[0]).wait_send()
    all_of(send_val.at[:, pl.ds(0, sent)], v_send.at[0], v_recv.at[0]).wait_send()
    field_copy.wait_send()

    field_copy.wait_recv()
    tall = points * own_half
    out_ref[pl.ds(pl.multiple_of(core * tall, tall), tall), :] = total
    out_ref[pl.ds(pl.multiple_of(other_core * tall, tall), tall), :] = pair[...]
    all_of(squares.at[pl.ds(0, 2 * n - 1)], r_send.at[0], r_recv.at[0]).wait()

    energy_all = squares[0]
    for device in range(1, 2 * n):
        energy_all = energy_all + squares[device]
    scale = jnp.sqrt(energy_all / (points * n * steps) + 1e-06)
    rms_ref[...] = jnp.broadcast_to(scale, rms_ref.shape)


def finish_kernel(field_ref, scale_ref, out_ref, rms_ref):
    vectors, points, steps = out_ref.shape
    scale = scale_ref[:1]
    rms_ref[...] = scale[0, :vectors]
    diagonal = lax.broadcasted_iota(jnp.int32, (vectors, LANES), 0) == lax.broadcasted_iota(
        jnp.int32, (vectors, LANES), 1
    )
    spread = jnp.broadcast_to(scale, (vectors, LANES))
    divisor = jnp.sum(jnp.where(diagonal, spread, 0.0), axis=1, keepdims=True)
    half = vectors // 2
    for point in range(points):
        near = field_ref[point * half : (point + 1) * half, :steps]
        far = field_ref[(points + point) * half : (points + point + 1) * half, :steps]
        out_ref[:, point, :] = jnp.concatenate([near, far], axis=0) / divisor


def paired_body(data, spectra):
    n = lax.axis_size("param")
    vectors, local, steps = data.shape
    sensors, points, freqs = spectra.shape[1:]
    wide = -(-steps // LANES) * LANES
    groups = -(-freqs // (2 * GROUP))
    count = groups * GROUP
    rows_pad = -(-count // 16) * 16
    pieces = groups // PIECE
    lines = n // 4
    forward, backward = paired_tables(steps, freqs, groups, rows_pad, wide)
    maps = fold_maps(steps)

    turned = jnp.transpose(spectra, (0, 3, 2, 1)).reshape(2, freqs, points, 2, LANES)
    turned = jnp.transpose(turned, (0, 1, 3, 2, 4)).reshape(2, freqs, 2 * points, LANES)

    hbm = pl.BlockSpec(memory_space=pl.ANY)
    vmem = pl.BlockSpec(memory_space=pltpu.VMEM)
    dma = pltpu.SemaphoreType.DMA
    f32, bf16 = jnp.float32, jnp.bfloat16
    fields, scale = pl.pallas_call(
        functools.partial(kernel, n, lines, vectors, local, steps, points, freqs, groups, wide),
        out_shape=(
            pltpu.VMEM((points * vectors, wide), f32),
            pltpu.VMEM((8, LANES), f32),
        ),
        in_specs=[hbm, hbm, hbm, hbm, vmem],
        out_specs=(vmem, vmem),
        scratch_shapes=[
            pltpu.VMEM((vectors, local, steps), f32),
            pltpu.VMEM((2, wide, 4 * LANES), bf16),
            pltpu.VMEM((2, 2 * count, 2 * points, LANES), f32),
            pltpu.VMEM((2, 2, groups, 2, GROUP // 2, 2 * points, LANES), f32),
            pltpu.VMEM((3, 2, groups, GROUP // 2, 2 * points, LANES), f32),
            pltpu.VMEM((CHUNKS, sensors, 7 * LANES), f32),
            pltpu.VMEM((6, 2 * rows_pad, LANES), bf16),
            pltpu.VMEM((2, 2, 2, 2, LANES, wide), bf16),
            pltpu.VMEM((2, count * 2 * vectors, LANES), f32),
            pltpu.VMEM((2, (count + GROUP) * points, LANES), f32),
            pltpu.VMEM((LANES, LANES), f32),
            pltpu.VMEM((3, LANES, LANES), f32),
            pltpu.VMEM((3, LANES, LANES), f32),
            pltpu.VMEM((points * vectors // 2, wide), f32),
            pltpu.VMEM((points * vectors // 2, wide), f32),
            pltpu.VMEM((1, LANES), f32),
            pltpu.VMEM((2 * n, 1, LANES), f32),
            dma((4,)),
            dma((pieces,)),
            dma((3,)), dma((BATCHES,)),
            dma((1,)), dma((CHUNKS, lines - 1)),
            dma((1,)), dma((CHUNKS, 2)),
            dma((1,)), dma((CHUNKS,)),
            dma((1,)), dma((CHUNKS,)),
            dma((1,)), dma((1,)),
            dma((1,)), dma((1,)),
            dma((1,)), dma((1,)),
        ],
        compiler_params=pltpu.CompilerParams(
            collective_id=0, has_side_effects=True, vmem_limit_bytes=60 * 1024 * 1024
        ),
    )(data, turned, jnp.asarray(forward), jnp.asarray(backward), jnp.asarray(maps))
    return pl.pallas_call(
        finish_kernel,
        out_shape=(jax.ShapeDtypeStruct((vectors, points, steps), f32), jax.ShapeDtypeStruct((vectors,), f32)),
        in_specs=[vmem, vmem],
        out_specs=(vmem, vmem),
    )(pltpu.with_memory_space_constraint(fields, pltpu.VMEM), pltpu.with_memory_space_constraint(scale, pltpu.VMEM))


def solution(mesh):
    in_specs = (P(None, ("sensor", "param"), None), P(None, "sensor", "param", None))
    out_specs = (P(None, "param", None), P())
    n = mesh.shape["param"]
    pair = mesh.shape["sensor"] == 2 and n == 16

    def body(data, spectra):
        vectors, local, _ = data.shape
        sensors, points = spectra.shape[1:3]
        fits = local * n == sensors and local % 8 == 0 and sensors == 2 * LANES and vectors == 2 * CHUNKS
        fits = fits and points * 2 * vectors == LANES and folded_layout_fits(data.shape[2])
        return (paired_body if pair and fits else general_body)(data, spectra)

    return jax.shard_map(body, mesh=mesh, in_specs=in_specs, out_specs=out_specs, check_vma=False)
```

```python
import functools
import math

import jax
import jax.numpy as jnp
import numpy as np
from jax import lax
from jax.experimental import pallas as pl
from jax.experimental.pallas import tpu as pltpu
from jax.sharding import PartitionSpec as P

MESH = pl.DeviceIdType.MESH
LANES = 128
GROUP = 8
CHUNKS = 8
PIECE = 3
BATCHES = 3
PAD_ROWS = 4


def spectral_tables(steps):
    length = 2 * steps
    freqs = steps + 1
    times = lax.broadcasted_iota(jnp.int32, (steps, freqs), 0)
    bins = lax.broadcasted_iota(jnp.int32, (steps, freqs), 1)
    phase = 2.0 * math.pi / length * (times * bins % length).astype(jnp.float32)
    forward = jnp.concatenate([jnp.cos(phase), -jnp.sin(phase)], axis=1)
    weight = jnp.where((bins == 0) | (bins == steps), 1.0, 2.0) / length
    backward = jnp.concatenate([(weight * jnp.cos(phase)).T, (-weight * jnp.sin(phase)).T], axis=0)
    return (forward, backward)


def to_spectrum(series, forward):
    vectors, sensors, steps = series.shape
    flat = jnp.dot(
        series.reshape(vectors * sensors, steps),
        forward,
        precision=lax.Precision.HIGHEST,
        preferred_element_type=jnp.float32,
    )
    return flat.reshape(vectors, sensors, forward.shape[1])


def contract(kernel, spectrum):
    return jnp.einsum(
        "spf,rsf->rpf",
        kernel,
        spectrum,
        precision=lax.Precision.HIGHEST,
        preferred_element_type=jnp.float32,
    )


def general_body(data, spectra):
    steps = data.shape[2]
    freqs = steps + 1
    forward, backward = spectral_tables(steps)
    whole = to_spectrum(lax.all_gather(data, "param", axis=1, tiled=True), forward)
    real_part = whole[..., :freqs]
    imag_part = whole[..., freqs:]
    kernel_re = spectra[0]
    kernel_im = spectra[1]
    out_re = contract(kernel_re, real_part) + contract(kernel_im, imag_part)
    out_im = contract(kernel_re, imag_part) - contract(kernel_im, real_part)
    vectors, points = (out_re.shape[0], out_re.shape[1])
    stacked = jnp.concatenate([out_re, out_im], axis=2).reshape(vectors * points, 2 * freqs)
    partial_field = jnp.dot(
        stacked, backward, precision=lax.Precision.HIGHEST, preferred_element_type=jnp.float32
    ).reshape(vectors, points, steps)
    count = points * lax.axis_size("param") * steps
    share = lax.psum_scatter(partial_field, "sensor", scatter_dimension=0, tiled=True)
    squares = lax.psum(jnp.sum(share * share, axis=(1, 2)), "param")
    scale = jnp.sqrt(squares / count + 1e-06)
    normalized = share / scale[:, None, None]
    gradient, rms_all = (
        lax.all_gather(normalized, "sensor", axis=0, tiled=True),
        lax.all_gather(scale, "sensor", axis=0, tiled=True),
    )
    return (gradient, rms_all)


def split(value):
    high = value.astype(jnp.bfloat16)
    return high, (value - high.astype(jnp.float32)).astype(jnp.bfloat16)


NT_DIMS = (((1,), (1,)), ((), ()))


def product(left, right, dims):
    dot = functools.partial(lax.dot_general, dimension_numbers=dims, preferred_element_type=jnp.float32)
    size = left[0].shape[0]
    both = dot(jnp.concatenate(left, axis=0), right[0])
    return both[:size] + (both[size:] + dot(left[0], right[1]))


def split_product(table, rows, right):
    dot = functools.partial(lax.dot_general, dimension_numbers=NT_DIMS, preferred_element_type=jnp.float32)
    half = table.shape[0] // 2
    both = dot(table, right[0])
    return both[:rows] + (both[half : half + rows] + dot(table[:half], right[1])[:rows])


def folded_layout_fits(steps):
    half = steps // 2
    rest = half + 1 - LANES
    groups = -(-(steps + 1) // (2 * GROUP))
    fits = steps % 2 == 0 and 0 < rest < LANES and half - LANES - (LANES - rest) <= LANES - rest
    fits = fits and groups % (PIECE * BATCHES) == 0
    return fits and BATCHES * batch_shares(groups // BATCHES * GROUP)[0][1] <= LANES


def frequency_order(freqs, groups):
    bins = np.arange(groups * 2 * GROUP).reshape(groups, 2, GROUP)
    return [bins[:, core].reshape(-1) for core in range(2)]


def lane_times(steps):
    half = steps // 2
    rest = half + 1 - LANES
    room = LANES - rest
    lane = np.arange(LANES)
    first = np.where(lane < rest, LANES + lane, -1)
    first_odd = np.where(lane < rest - 1, LANES + lane, -1)
    second = np.where(lane >= room, LANES + lane - room, -1)
    tail_a = np.where(lane >= rest, LANES + lane - rest, -1)
    tail_b = np.where(lane < rest - 1 - room, LANES + room + lane, -1)
    return lane, first, first_odd, second, tail_a, tail_b


def fold_maps(steps):
    lane, first, first_odd, second, tail_a, tail_b = lane_times(steps)
    shared = np.where(second >= 0, second, tail_b)
    even = np.concatenate([lane, lane, first, first_odd])
    odd = np.concatenate([lane, lane, tail_a, shared])
    ones = np.ones(LANES, np.int64)
    even_sign = np.concatenate([ones, -ones, ones, -ones])
    odd_sign = np.concatenate([ones, -ones, -ones, np.where(second >= 0, 1, -1)])
    maps = np.full((8, 4 * LANES), -1, np.int32)
    for index, (time, sign) in enumerate(((even, even_sign), (odd, odd_sign))):
        mirror = np.where((time > 0) & (2 * time != steps), steps - time, -1)
        maps[3 * index] = time
        maps[3 * index + 1] = np.where(time < 0, -1, mirror)
        maps[3 * index + 2] = sign
    return maps


def halves(values):
    high = values.astype(jnp.bfloat16)
    return high, (values - high.astype(np.float32)).astype(jnp.bfloat16)


def batch_shares(batch):
    first = -(-batch // (2 * GROUP)) * GROUP
    return ((0, first), (first, batch - first))


def paired_tables(steps, freqs, groups, rows_pad, wide):
    half = steps // 2
    lane, first, first_odd, second, tail_a, tail_b = lane_times(steps)
    tail = np.where(tail_a >= 0, tail_a, tail_b)
    forward, backward = [], []
    for bins in frequency_order(freqs, groups):
        count = bins.shape[0]
        known = (bins < freqs)[:, None]
        even = (bins % 2 == 0)[:, None]
        angle = bins[:, None] * np.arange(steps)[None, :] % (2 * steps)
        phase = np.pi / steps * angle
        sine = np.where(angle % steps == 0, 0.0, np.sin(phase))
        cosine = np.cos(phase)
        symmetric = np.where(known, np.where(even, cosine, -sine), 0.0)
        other = np.where(known, np.where(even, -sine, cosine), 0.0)
        blocks = []
        for table, times in (
            (symmetric, lane), (other, lane), (symmetric, first), (other, first_odd), (symmetric, second), (other, tail),
        ):
            limit = half if table is symmetric else half - 1
            inside = (times >= 0) & (times <= limit)
            value = np.where(inside[None, :], table[:, np.clip(times, 0, limit)], 0.0).astype(np.float32)
            block = np.zeros((2, rows_pad, LANES), jnp.bfloat16)
            block[0, :count], block[1, :count] = halves(value)
            blocks.append(block.reshape(2 * rows_pad, LANES))
        forward.append(np.stack(blocks))
        weight = np.where((bins == 0) | (bins == steps), 0.5, 1.0)[:, None] / steps
        inverse = np.zeros((2, 2, 2, LANES, wide), jnp.bfloat16)
        batch = groups // BATCHES * GROUP
        for position, table in enumerate((symmetric, other)):
            value = (table * weight).astype(np.float32)
            for turn in range(BATCHES):
                for share, (begin, size) in enumerate(batch_shares(batch)):
                    target = slice(turn * batch_shares(batch)[0][1], turn * batch_shares(batch)[0][1] + size)
                    source = slice(turn * batch + begin, turn * batch + begin + size)
                    parts = halves(value[source])
                    for index in range(2):
                        inverse[index, position, share, target, :steps] = parts[index]
        backward.append(inverse)
    return np.stack(forward), np.stack(backward)


def kernel(
    n, lines, vectors, local, steps, points, freqs, groups, wide,
    data_ref, spectra_ref, forward_ref, backward_ref, maps_ref,
    out_ref, rms_ref,
    series, fold, raw, packed, kbuf, gathered, table, inverse, spectrum, product_s, own_val, send_val, recv_val,
    partial, pair, square, squares,
    load_sem, raw_sem, k_send, k_recv, z_send, z_recv, y_send, y_recv, c_send, c_recv, w_send, w_recv,
    v_send, v_recv, f_send, f_recv, r_send, r_recv,
):
    me = lax.axis_index("param")
    core = lax.axis_index("sensor")
    x = lax.rem(me, 2)
    y = lax.rem(me // 2, 2)
    z = me // 4
    plane = 4
    other_chip = me + 1 - 2 * x
    y_chip = me + 2 - 4 * y
    other_core = 1 - core
    z_mate = z + 1 - 2 * lax.rem(z, 2)
    half = steps // 2
    rest = half + 1 - LANES
    rows = points * GROUP
    count = groups * GROUP
    pieces = groups // PIECE
    span = PIECE * 2 * GROUP
    pitch = 2 * vectors + PAD_ROWS
    batch = groups // BATCHES

    barrier = pltpu.get_barrier_semaphore()

    for neighbour in ((other_chip, core), (other_chip, other_core), (y_chip, core), (me, other_core)):
        pl.semaphore_signal(barrier, inc=1, device_id=neighbour, device_id_type=MESH)

    @pl.when(z > 0)
    def _():
        pl.semaphore_signal(barrier, inc=1, device_id=(me - plane, core), device_id_type=MESH)

    @pl.when(z + 1 < lines)
    def _():
        pl.semaphore_signal(barrier, inc=1, device_id=(me + plane, core), device_id_type=MESH)

    def filled(piece, target):
        known = -(-(freqs - target * GROUP) // (2 * GROUP))
        return min(PIECE, known - piece * PIECE)

    def raw_copy(piece):
        begin = piece * span
        size = min(span, freqs - begin)
        return pltpu.make_async_copy(
            spectra_ref.at[:, pl.ds(begin, size)], raw.at[:, pl.ds(begin, size)], raw_sem.at[piece]
        )

    data_copy = pltpu.make_async_copy(data_ref, series, load_sem.at[0])
    forward_copy = pltpu.make_async_copy(forward_ref.at[core], table, load_sem.at[1])
    backward_copies = [
        pltpu.make_async_copy(backward_ref.at[source], inverse.at[index], load_sem.at[2 + index])
        for index, source in enumerate((core, other_core))
    ]
    data_copy.start()
    raw_copy(0).start()
    for piece in range(1, pieces):
        raw_copy(piece).start()
    forward_copy.start()
    for backward_copy in backward_copies:
        backward_copy.start()

    strip = 64

    @pl.loop(0, fold.shape[1] // strip)
    def _(part):
        begin = pl.multiple_of(part * strip, strip)
        time = lax.broadcasted_iota(jnp.int32, (strip, 4 * LANES), 0) + begin
        for side in range(2):
            direct = jnp.where(time == maps_ref[3 * side : 3 * side + 1, :], 1.0, 0.0)
            sign = maps_ref[3 * side + 2 : 3 * side + 3, :].astype(jnp.float32)
            mirror = jnp.where(time == maps_ref[3 * side + 1 : 3 * side + 2, :], sign, 0.0)
            fold[side, pl.ds(begin, strip), :] = (direct + mirror).astype(jnp.bfloat16)

    upper = lax.broadcasted_iota(jnp.int32, (8, LANES), 0) < points
    stripe = lax.broadcasted_iota(jnp.int32, (8, LANES), 1) // local % 2 == 0

    def sort_piece(piece):
        @pl.loop(0, 2)
        def _(part):
            @pl.loop(piece * PIECE, (piece + 1) * PIECE)
            def _(group):
                for side in range(2):
                    for duo in range(GROUP // 2):
                        begin = group * 2 * GROUP + side * GROUP + 2 * duo
                        first = raw[part, begin]
                        second = raw[part, begin + 1]
                        low = jnp.where(upper, first, pltpu.roll(second, points, 0))
                        high = jnp.where(upper, pltpu.roll(first, points, 0), second)
                        packed[0, part, group, side, duo] = jnp.where(stripe, low, pltpu.roll(high, local, 1))
                        packed[1, part, group, side, duo] = jnp.where(stripe, pltpu.roll(high, LANES - local, 1), low)

    def k_copy(piece, target):
        begin = piece * PIECE
        size = filled(piece, target)
        rel = core if target == 0 else other_core
        return pltpu.make_async_remote_copy(
            src_ref=packed.at[1 - x, :, pl.ds(begin, size), target],
            dst_ref=kbuf.at[1 + rel, :, pl.ds(begin, size)],
            send_sem=k_send.at[target], recv_sem=k_recv.at[piece // (pieces // BATCHES)],
            device_id=(other_chip, target), device_id_type=MESH,
        )

    def k_keep(piece):
        begin = piece * PIECE
        return pltpu.make_async_remote_copy(
            src_ref=packed.at[x, :, pl.ds(begin, PIECE), other_core],
            dst_ref=kbuf.at[0, :, pl.ds(begin, PIECE)],
            send_sem=k_send.at[2], recv_sem=k_recv.at[piece // (pieces // BATCHES)],
            device_id=(me, other_core), device_id_type=MESH,
        )

    def all_of(ref, send_sem, recv_sem):
        return pltpu.make_async_remote_copy(
            src_ref=ref, dst_ref=ref, send_sem=send_sem, recv_sem=recv_sem,
            device_id=(me, other_core), device_id_type=MESH,
        )

    def wait_batch(turn):
        begin = turn * batch
        full = all_of(kbuf.at[:, :, pl.ds(begin, batch)], k_send.at[2], k_recv.at[turn])
        missing = 0 if turn + 1 < BATCHES else 2 * (PIECE - filled(pieces - 1, 1))
        if missing:
            short = all_of(packed.at[0, 0, pl.ds(0, 3 * batch - missing)], k_send.at[2], k_recv.at[turn])
            pl.when(core == 0)(full.wait_recv)
            pl.when(core == 1)(short.wait_recv)
        else:
            full.wait_recv()

    def send_piece(piece):
        for target in range(2):
            k_copy(piece, target).start()
        k_keep(piece).start()

    def slot(line, row, column):
        return line * plane + row * 2 + column

    def place(line, row):
        upper_line = line // 2
        return lax.rem(line, 2) * plane + row * 2 + upper_line + x - 2 * upper_line * x

    def block(chunk, line, row, rel=0):
        position = rel * (n // 2) + place(line, row)
        return gathered.at[chunk, pl.ds(pl.multiple_of(position * local, local), local), :]

    data_copy.wait()
    plain = (((1,), (0,)), ((), ()))
    folded = []
    for side in range(2):
        values = jnp.concatenate([series[side * CHUNKS + chunk] for chunk in range(CHUNKS)], axis=0)
        high = values.astype(jnp.bfloat16)
        left = values - high.astype(jnp.float32)
        middle = left.astype(jnp.bfloat16)
        low = (left - middle.astype(jnp.float32)).astype(jnp.bfloat16)
        result = lax.dot_general(
            jnp.concatenate([high, middle, low], axis=0), fold[side, :steps, :], plain,
            preferred_element_type=jnp.float32,
        )
        size = CHUNKS * local
        folded.append(result[:size] + (result[size : 2 * size] + result[2 * size :]))
    own_row = pl.ds(pl.multiple_of(place(z, y) * local, local), local)
    for chunk in range(CHUNKS):
        even = folded[0][chunk * local : (chunk + 1) * local]
        odd = folded[1][chunk * local : (chunk + 1) * local]
        gathered[chunk, own_row, 0 : 2 * LANES] = even[:, : 2 * LANES]
        gathered[chunk, own_row, 2 * LANES : 4 * LANES] = odd[:, : 2 * LANES]
        gathered[chunk, own_row, 4 * LANES : 5 * LANES] = (
            even[:, 2 * LANES : 3 * LANES] + odd[:, 2 * LANES : 3 * LANES]
        )
        gathered[chunk, own_row, 5 * LANES : 6 * LANES] = even[:, 3 * LANES :]
        gathered[chunk, own_row, 6 * LANES :] = odd[:, 3 * LANES :]

    def send(source, target, send_sem, recv_sem):
        return pltpu.make_async_remote_copy(
            src_ref=source, dst_ref=source, send_sem=send_sem, recv_sem=recv_sem,
            device_id=target, device_id_type=MESH,
        )

    def some(blocks, send_sem, recv_sem):
        return all_of(gathered.at[0, pl.ds(0, blocks * local)], send_sem, recv_sem)

    def many(blocks, send_sem, recv_sem):
        whole = gathered.shape[1] // local
        if blocks <= whole:
            return some(blocks, send_sem, recv_sem)
        assert blocks % CHUNKS == 0
        return all_of(gathered.at[:, pl.ds(0, blocks // CHUNKS * local)], send_sem, recv_sem)

    def line_index(source, target):
        return jnp.where(source < target, source, source - 1)

    def line_copy(chunk, step, way):
        source = jnp.clip(z - way * step, 0, lines - 1)
        target = jnp.clip(z + way, 0, lines - 1)
        return send(
            block(chunk, source, y), (slot(target, y, x), core),
            z_send.at[0], z_recv.at[chunk, jnp.clip(line_index(source, target), 0, lines - 2)],
        )

    def line_arrival(chunk, step, way):
        source = jnp.clip(z - way * (step + 1), 0, lines - 1)
        target = jnp.clip(z + way, 0, lines - 1)
        return source, send(
            block(chunk, source, y), (slot(target, y, x), core),
            z_send.at[0], z_recv.at[chunk, jnp.clip(line_index(source, z), 0, lines - 2)],
        )

    def sends(step, way):
        inside = z + 1 < lines if way > 0 else z > 0
        begun = z >= step if way > 0 else z + step < lines
        return jnp.logical_and(inside, begun)

    def receives(step, way):
        return z >= step + 1 if way > 0 else z + step + 1 < lines

    def y_copy(chunk, line):
        index = jnp.where(line == z, 0, 1)
        return send(block(chunk, line, y), (y_chip, core), y_send.at[0], y_recv.at[chunk, index])

    def turn_copy(chunk):
        return send(block(chunk, z, 1 - y), (slot(z_mate, y, x), core), w_send.at[0], w_recv.at[chunk])

    def turn_arrival(chunk):
        return send(block(chunk, z_mate, 1 - y), (slot(z_mate, y, x), core), w_send.at[0], w_recv.at[chunk])

    def turns(chunk):
        return chunk >= CHUNKS // 2

    def by_row(chunk, line):
        return jnp.logical_not(jnp.logical_and(turns(chunk), line == z_mate))

    def core_copy(chunk, row, line):
        return pltpu.make_async_remote_copy(
            src_ref=block(chunk, line, row), dst_ref=block(chunk, line, row, 1),
            send_sem=c_send.at[0], recv_sem=c_recv.at[chunk],
            device_id=(me, other_core), device_id_type=MESH,
        )

    def start_lines(chunk):
        for way in (1, -1):

            @pl.when(sends(0, way))
            def _():
                line_copy(chunk, 0, way).start()

        y_copy(chunk, z).start()
        core_copy(chunk, y, z).start()

    def from_lines(chunk, step):
        for way in (1, -1):

            @pl.when(receives(step, way))
            def _():
                source, arrival = line_arrival(chunk, step, way)
                arrival.wait_recv()
                if step + 1 < lines - 1:

                    @pl.when(sends(step + 1, way))
                    def _():
                        line_copy(chunk, step + 1, way).start()

                @pl.when(by_row(chunk, source))
                def _():
                    y_copy(chunk, source).start()

                core_copy(chunk, y, source).start()

    def from_mate(chunk):
        some(1, y_send.at[0], y_recv.at[chunk, 0]).wait_recv()
        core_copy(chunk, 1 - y, z).start()

    def to_mate(chunk):
        @pl.when(turns(chunk))
        def _():
            turn_copy(chunk).start()

    def from_row(chunk):
        @pl.when(turns(chunk))
        def _():
            some(lines - 2, y_send.at[0], y_recv.at[chunk, 1]).wait_recv()
            turn_arrival(chunk).wait_recv()

        @pl.when(jnp.logical_not(turns(chunk)))
        def _():
            some(lines - 1, y_send.at[0], y_recv.at[chunk, 1]).wait_recv()

        for step in range(1, lines):
            core_copy(chunk, 1 - y, lax.rem(z + step, lines)).start()

    def from_core(chunk):
        some(n // 2, c_send.at[0], c_recv.at[chunk]).wait_recv()

    lane_index = lax.broadcasted_iota(jnp.int32, (gathered.shape[1], LANES), 1)

    def transform(chunk):
        def lanes(index):
            return gathered[chunk, :, index * LANES : (index + 1) * LANES]

        for which in range(4):
            odd = which // 2
            position = which % 2
            if which < 2:
                tail = lanes(4 + which)
            elif which == 2:
                tail = lanes(6)
            else:
                tail = jnp.where(lane_index >= rest, lanes(4), lanes(6))
            right = split(jnp.concatenate([lanes(which), tail], axis=1))
            left = jnp.concatenate([table[position], table[2 + which]], axis=1)
            result = split_product(left, count, right)
            for lane in range(2):
                spectrum[lane, pl.ds(odd * vectors + position * CHUNKS + chunk, count, stride=pitch), :] = result[
                    :, lane * LANES : (lane + 1) * LANES
                ]

    pl.semaphore_wait(barrier, 4 + jnp.minimum(z, 1) + jnp.minimum(lines - 1 - z, 1))
    pl.loop(0, CHUNKS)(start_lines)

    raw[:, freqs:] = jnp.zeros((2, raw.shape[1] - freqs) + tuple(raw.shape[2:]), jnp.float32)
    short = filled(pieces - 1, 1)
    if short < PIECE:

        @pl.when(core == 1)
        def _():
            begin = (pieces - 1) * PIECE + short
            for owner in range(1, 3):
                kbuf[owner, :, begin:] = jnp.zeros((2, PIECE - short) + tuple(kbuf.shape[3:]), jnp.float32)


    for piece in range(pieces):
        raw_copy(piece).wait()
        sort_piece(piece)
        send_piece(piece)

    forward_copy.wait()
    for backward_copy in backward_copies:
        backward_copy.wait()

    def finish(chunk):
        from_core(chunk)
        transform(chunk)

    stages = [
        (functools.partial(from_lines, step=0), 0), (from_mate, 0),
        (functools.partial(from_lines, step=1), 2), (functools.partial(from_lines, step=2), 3), (to_mate, 4),
        (from_row, 6), (finish, 7),
    ]

    @pl.loop(0, CHUNKS + stages[-1][1])
    def _(turn):
        for stage, age in stages:
            chunk = turn - age

            @pl.when(jnp.logical_and(chunk >= 0, chunk < CHUNKS))
            def _():
                stage(chunk)

    columns = GROUP * 2 * vectors
    row_freq = lax.broadcasted_iota(jnp.int32, (4 * rows, columns), 0) // points % GROUP
    col_freq = lax.broadcasted_iota(jnp.int32, (4 * rows, columns), 1) // (2 * vectors)
    own = row_freq == col_freq
    lane = lax.broadcasted_iota(jnp.int32, (2 * rows, LANES), 1)
    row = lax.broadcasted_iota(jnp.int32, (2 * rows, LANES), 0) // points % 2
    first_half = lane % vectors < vectors // 2
    sign = jnp.where(first_half == (row == 0), 1.0, -1.0)
    shares = batch_shares(batch * GROUP)
    step_rows = shares[0][1]
    lane_group = lax.broadcasted_iota(jnp.int32, (step_rows, LANES), 1) // vectors
    known_rows = lax.broadcasted_iota(jnp.int32, (step_rows, LANES), 0) < shares[1][1]

    def value_rows(turn):
        return pl.ds(pl.multiple_of(turn * step_rows, GROUP), step_rows)

    def value_copy(turn, target):
        place_rows = value_rows(turn)
        return pltpu.make_async_remote_copy(
            src_ref=send_val.at[target, place_rows],
            dst_ref=recv_val.at[jnp.where(core == target, 0, 2), place_rows],
            send_sem=v_send.at[0], recv_sem=v_recv.at[0],
            device_id=(other_chip, target), device_id_type=MESH,
        )

    def value_keep(turn):
        place_rows = value_rows(turn)
        return pltpu.make_async_remote_copy(
            src_ref=send_val.at[2, place_rows], dst_ref=recv_val.at[1, place_rows],
            send_sem=v_send.at[0], recv_sem=v_recv.at[0],
            device_id=(me, other_core), device_id_type=MESH,
        )

    @pl.loop(0, BATCHES)
    def _(turn):
        for which in range(BATCHES):

            @pl.when(turn == which)
            def _():
                wait_batch(which)

        for step in range(batch):
            group = turn * batch + step
            begin = pl.multiple_of(group * GROUP * pitch, GROUP)
            sides = []
            for side in range(2):
                pieces_of = [spectrum[side, pl.ds(begin + step_f * pitch, 2 * vectors), :] for step_f in range(GROUP)]
                sides.append(jnp.concatenate(pieces_of, axis=0))
            right = split(jnp.concatenate(sides, axis=1))
            parts = []
            for part in range(2):
                for near, far in (
                    (packed[x, part, group, core], kbuf[0, part, group]), (kbuf[1, part, group], kbuf[2, part, group]),
                ):
                    parts.append(jnp.concatenate([near.reshape(rows, LANES), far.reshape(rows, LANES)], axis=1))
            left = jnp.concatenate(parts, axis=0)
            found = jnp.where(own, product(split(left), right, NT_DIMS), 0.0)
            width = columns
            while width > LANES:
                width //= 2
                found = found[:, :width] + found[:, width:]
            hop = LANES // 2
            while hop >= 2 * vectors:
                found = found + pltpu.roll(found, hop, 1)
                hop //= 2
            turned = found[2 * rows :]
            turned = jnp.where(
                first_half, pltpu.roll(turned, LANES - vectors // 2, 1), pltpu.roll(turned, vectors // 2, 1)
            )
            value = found[: 2 * rows] + sign * turned
            for owner in range(2):
                product_s[owner, pl.ds(pl.multiple_of(group * rows, rows), rows), :] = value[
                    owner * rows : (owner + 1) * rows
                ]
        for owner in (1, 0):
            merged = [jnp.zeros((step_rows, LANES), jnp.float32)] * 2
            for share in range(2):
                for point in range(points):
                    begin = (turn * batch * GROUP + shares[share][0]) * points + point
                    value = product_s[owner, pl.ds(begin, step_rows, stride=points), :]
                    if share == 1:
                        value = jnp.where(known_rows, value, 0.0)
                    shifted = pltpu.roll(value, vectors, 1)
                    index = share * points + point
                    for target in range(2):
                        chosen = value if index % 2 == target else shifted
                        merged[target] = jnp.where(lane_group == index, chosen, merged[target])
            if owner == 1:
                for target in range(2):
                    send_val[target, value_rows(turn), :] = merged[target]
                for target in range(2):
                    value_copy(turn, target).start()
            else:
                send_val[2, value_rows(turn), :] = jnp.where(core == 0, merged[1], merged[0])
                own_val[value_rows(turn), :] = jnp.where(core == 0, merged[0], merged[1])
                value_keep(turn).start()

    sent = BATCHES * step_rows
    all_of(recv_val.at[:, pl.ds(0, sent)], v_send.at[0], v_recv.at[0]).wait_recv()

    own_half = vectors // 2
    blocks = []
    for near in (own_val[:sent, :] + recv_val[0, :sent, :], recv_val[1, :sent, :] + recv_val[2, :sent, :]):
        turned = jnp.concatenate([near, jnp.zeros((LANES - sent, LANES), jnp.float32)], axis=0).T
        for position in range(2):
            for share in range(2):
                begins = [
                    ((share * points + point) * 2 + position) * own_half for point in range(points)
                ]
                blocks.append(jnp.concatenate([turned[begin : begin + own_half] for begin in begins], axis=0))
    left = split(jnp.concatenate(blocks, axis=1))
    right = []
    for index in range(2):
        right.append(jnp.concatenate([inverse[near, index].reshape(4 * LANES, wide) for near in range(2)], axis=0))
    total = product(left, right, plain)
    partial[...] = total

    field_copy = pltpu.make_async_remote_copy(
        src_ref=partial, dst_ref=pair, send_sem=f_send.at[0], recv_sem=f_recv.at[0],
        device_id=(me, other_core), device_id_type=MESH,
    )

    energy = total * total
    summed = energy[:own_half]
    for point in range(1, points):
        summed = summed + energy[point * own_half : (point + 1) * own_half]
    column = jnp.sum(summed, axis=1, keepdims=True)
    lane8 = lax.broadcasted_iota(jnp.int32, (own_half, LANES), 1)
    row8 = lax.broadcasted_iota(jnp.int32, (own_half, LANES), 0)
    flat = jnp.sum(jnp.where(lane8 == row8 + core * own_half, column, 0.0), axis=0, keepdims=True)
    square[...] = flat
    mine = core * n + me
    squares[mine] = flat

    def square_copy(target, target_core):
        return pltpu.make_async_remote_copy(
            src_ref=square, dst_ref=squares.at[mine], send_sem=r_send.at[0], recv_sem=r_recv.at[0],
            device_id=(target, target_core), device_id_type=MESH,
        )

    @pl.loop(1, n)
    def _(step):
        square_copy(lax.rem(me + step, n), core).start()
        square_copy(lax.rem(me + step, n), other_core).start()

    square_copy(me, other_core).start()
    field_copy.start()

    for line in range(lines):
        ahead = line + 1 if line + 1 < lines else 0
        back = lines - line if line > 0 else 0

        @pl.when(z == line)
        def _():
            many((ahead + back) * CHUNKS, z_send.at[0], z_recv.at[0, 0]).wait_send()

    late = CHUNKS - CHUNKS // 2
    all_of(
        gathered.at[:, pl.ds(0, (lines * CHUNKS - late) * local // CHUNKS)], y_send.at[0], y_recv.at[0, 0]
    ).wait_send()
    some(late, w_send.at[0], w_recv.at[0]).wait_send()
    all_of(gathered.at[:, pl.ds(0, gathered.shape[1] // 2)], c_send.at[0], c_recv.at[0]).wait_send()
    for target in range(2):
        all_of(packed.at[0, :, pl.ds(0, groups - PIECE + filled(pieces - 1, target)), target],
               k_send.at[target], k_recv.at[0]).wait_send()
    all_of(packed.at[0, :, :, 0], k_send.at[2], k_recv.at[0]).wait_send()
    all_of(send_val.at[:, pl.ds(0, sent)], v_send.at[0], v_recv.at[0]).wait_send()
    field_copy.wait_send()

    field_copy.wait_recv()
    tall = points * own_half
    out_ref[pl.ds(pl.multiple_of(core * tall, tall), tall), :] = total
    out_ref[pl.ds(pl.multiple_of(other_core * tall, tall), tall), :] = pair[...]
    all_of(squares.at[pl.ds(0, 2 * n - 1)], r_send.at[0], r_recv.at[0]).wait()

    energy_all = squares[0]
    for device in range(1, 2 * n):
        energy_all = energy_all + squares[device]
    scale = jnp.sqrt(energy_all / (points * n * steps) + 1e-06)
    rms_ref[...] = jnp.broadcast_to(scale, rms_ref.shape)


def finish_kernel(field_ref, scale_ref, out_ref, rms_ref):
    vectors, points, steps = out_ref.shape
    scale = scale_ref[:1]
    rms_ref[...] = scale[0, :vectors]
    diagonal = lax.broadcasted_iota(jnp.int32, (vectors, LANES), 0) == lax.broadcasted_iota(
        jnp.int32, (vectors, LANES), 1
    )
    spread = jnp.broadcast_to(scale, (vectors, LANES))
    divisor = jnp.sum(jnp.where(diagonal, spread, 0.0), axis=1, keepdims=True)
    half = vectors // 2
    for point in range(points):
        near = field_ref[point * half : (point + 1) * half, :steps]
        far = field_ref[(points + point) * half : (points + point + 1) * half, :steps]
        out_ref[:, point, :] = jnp.concatenate([near, far], axis=0) / divisor


def paired_body(data, spectra):
    n = lax.axis_size("param")
    vectors, local, steps = data.shape
    sensors, points, freqs = spectra.shape[1:]
    wide = -(-steps // LANES) * LANES
    groups = -(-freqs // (2 * GROUP))
    count = groups * GROUP
    rows_pad = -(-count // 16) * 16
    pieces = groups // PIECE
    lines = n // 4
    forward, backward = paired_tables(steps, freqs, groups, rows_pad, wide)
    maps = fold_maps(steps)

    turned = jnp.transpose(spectra, (0, 3, 2, 1)).reshape(2, freqs, points, 2, LANES)
    turned = jnp.transpose(turned, (0, 1, 3, 2, 4)).reshape(2, freqs, 2 * points, LANES)

    hbm = pl.BlockSpec(memory_space=pl.ANY)
    vmem = pl.BlockSpec(memory_space=pltpu.VMEM)
    dma = pltpu.SemaphoreType.DMA
    f32, bf16 = jnp.float32, jnp.bfloat16
    fields, scale = pl.pallas_call(
        functools.partial(kernel, n, lines, vectors, local, steps, points, freqs, groups, wide),
        out_shape=(
            pltpu.VMEM((points * vectors, wide), f32),
            pltpu.VMEM((8, LANES), f32),
        ),
        in_specs=[hbm, hbm, hbm, hbm, vmem],
        out_specs=(vmem, vmem),
        scratch_shapes=[
            pltpu.VMEM((vectors, local, steps), f32),
            pltpu.VMEM((2, wide, 4 * LANES), bf16),
            pltpu.VMEM((2, 2 * count, 2 * points, LANES), f32),
            pltpu.VMEM((2, 2, groups, 2, GROUP // 2, 2 * points, LANES), f32),
            pltpu.VMEM((3, 2, groups, GROUP // 2, 2 * points, LANES), f32),
            pltpu.VMEM((CHUNKS, sensors, 7 * LANES), f32),
            pltpu.VMEM((6, 2 * rows_pad, LANES), bf16),
            pltpu.VMEM((2, 2, 2, 2, LANES, wide), bf16),
            pltpu.VMEM((2, count * (2 * vectors + PAD_ROWS), LANES), f32),
            pltpu.VMEM((2, (count + GROUP) * points, LANES), f32),
            pltpu.VMEM((LANES, LANES), f32),
            pltpu.VMEM((3, LANES, LANES), f32),
            pltpu.VMEM((3, LANES, LANES), f32),
            pltpu.VMEM((points * vectors // 2, wide), f32),
            pltpu.VMEM((points * vectors // 2, wide), f32),
            pltpu.VMEM((1, LANES), f32),
            pltpu.VMEM((2 * n, 1, LANES), f32),
            dma((4,)),
            dma((pieces,)),
            dma((3,)), dma((BATCHES,)),
            dma((1,)), dma((CHUNKS, lines - 1)),
            dma((1,)), dma((CHUNKS, 2)),
            dma((1,)), dma((CHUNKS,)),
            dma((1,)), dma((CHUNKS,)),
            dma((1,)), dma((1,)),
            dma((1,)), dma((1,)),
            dma((1,)), dma((1,)),
        ],
        compiler_params=pltpu.CompilerParams(
            collective_id=0, has_side_effects=True, vmem_limit_bytes=60 * 1024 * 1024
        ),
    )(data, turned, jnp.asarray(forward), jnp.asarray(backward), jnp.asarray(maps))
    return pl.pallas_call(
        finish_kernel,
        out_shape=(jax.ShapeDtypeStruct((vectors, points, steps), f32), jax.ShapeDtypeStruct((vectors,), f32)),
        in_specs=[vmem, vmem],
        out_specs=(vmem, vmem),
    )(pltpu.with_memory_space_constraint(fields, pltpu.VMEM), pltpu.with_memory_space_constraint(scale, pltpu.VMEM))


def solution(mesh):
    in_specs = (P(None, ("sensor", "param"), None), P(None, "sensor", "param", None))
    out_specs = (P(None, "param", None), P())
    n = mesh.shape["param"]
    pair = mesh.shape["sensor"] == 2 and n == 16

    def body(data, spectra):
        vectors, local, _ = data.shape
        sensors, points = spectra.shape[1:3]
        fits = local * n == sensors and local % 8 == 0 and sensors == 2 * LANES and vectors == 2 * CHUNKS
        fits = fits and points * 2 * vectors == LANES and folded_layout_fits(data.shape[2])
        return (paired_body if pair and fits else general_body)(data, spectra)

    return jax.shard_map(body, mesh=mesh, in_specs=in_specs, out_specs=out_specs, check_vma=False)
```

```python
import functools
import math

import jax
import jax.numpy as jnp
import numpy as np
from jax import lax
from jax.experimental import pallas as pl
from jax.experimental.pallas import tpu as pltpu
from jax.sharding import PartitionSpec as P

MESH = pl.DeviceIdType.MESH
LANES = 128
GROUP = 8
CHUNKS = 8
PIECE = 3
BATCHES = 3
PAD_ROWS = 4
NARROW = 2


def spectral_tables(steps):
    length = 2 * steps
    freqs = steps + 1
    times = lax.broadcasted_iota(jnp.int32, (steps, freqs), 0)
    bins = lax.broadcasted_iota(jnp.int32, (steps, freqs), 1)
    phase = 2.0 * math.pi / length * (times * bins % length).astype(jnp.float32)
    forward = jnp.concatenate([jnp.cos(phase), -jnp.sin(phase)], axis=1)
    weight = jnp.where((bins == 0) | (bins == steps), 1.0, 2.0) / length
    backward = jnp.concatenate([(weight * jnp.cos(phase)).T, (-weight * jnp.sin(phase)).T], axis=0)
    return (forward, backward)


def to_spectrum(series, forward):
    vectors, sensors, steps = series.shape
    flat = jnp.dot(
        series.reshape(vectors * sensors, steps),
        forward,
        precision=lax.Precision.HIGHEST,
        preferred_element_type=jnp.float32,
    )
    return flat.reshape(vectors, sensors, forward.shape[1])


def contract(kernel, spectrum):
    return jnp.einsum(
        "spf,rsf->rpf",
        kernel,
        spectrum,
        precision=lax.Precision.HIGHEST,
        preferred_element_type=jnp.float32,
    )


def general_body(data, spectra):
    steps = data.shape[2]
    freqs = steps + 1
    forward, backward = spectral_tables(steps)
    whole = to_spectrum(lax.all_gather(data, "param", axis=1, tiled=True), forward)
    real_part = whole[..., :freqs]
    imag_part = whole[..., freqs:]
    kernel_re = spectra[0]
    kernel_im = spectra[1]
    out_re = contract(kernel_re, real_part) + contract(kernel_im, imag_part)
    out_im = contract(kernel_re, imag_part) - contract(kernel_im, real_part)
    vectors, points = (out_re.shape[0], out_re.shape[1])
    stacked = jnp.concatenate([out_re, out_im], axis=2).reshape(vectors * points, 2 * freqs)
    partial_field = jnp.dot(
        stacked, backward, precision=lax.Precision.HIGHEST, preferred_element_type=jnp.float32
    ).reshape(vectors, points, steps)
    count = points * lax.axis_size("param") * steps
    share = lax.psum_scatter(partial_field, "sensor", scatter_dimension=0, tiled=True)
    squares = lax.psum(jnp.sum(share * share, axis=(1, 2)), "param")
    scale = jnp.sqrt(squares / count + 1e-06)
    normalized = share / scale[:, None, None]
    gradient, rms_all = (
        lax.all_gather(normalized, "sensor", axis=0, tiled=True),
        lax.all_gather(scale, "sensor", axis=0, tiled=True),
    )
    return (gradient, rms_all)


def split(value):
    high = value.astype(jnp.bfloat16)
    return high, (value - high.astype(jnp.float32)).astype(jnp.bfloat16)


NT_DIMS = (((1,), (1,)), ((), ()))


def product(left, right, dims):
    dot = functools.partial(lax.dot_general, dimension_numbers=dims, preferred_element_type=jnp.float32)
    size = left[0].shape[0]
    both = dot(jnp.concatenate(left, axis=0), right[0])
    return both[:size] + (both[size:] + dot(left[0], right[1]))


def split_product(table, rows, right):
    dot = functools.partial(lax.dot_general, dimension_numbers=NT_DIMS, preferred_element_type=jnp.float32)
    half = table.shape[0] // 2
    both = dot(table, right[0])
    return both[:rows] + (both[half : half + rows] + dot(table[:half], right[1])[:rows])


def folded_layout_fits(steps):
    half = steps // 2
    rest = half + 1 - LANES
    groups = -(-(steps + 1) // (2 * GROUP))
    fits = rest - 1 <= 2 * (LANES - (rest - 1)) and steps % 2 == 0 and 0 < rest < LANES and half - LANES - (LANES - rest) <= LANES - rest
    fits = fits and groups % (PIECE * BATCHES) == 0
    return fits and BATCHES * batch_shares(groups // BATCHES * GROUP)[0][1] <= LANES


def frequency_order(freqs, groups):
    bins = np.arange(groups * 2 * GROUP).reshape(groups, 2, GROUP)
    return [bins[:, core].reshape(-1) for core in range(2)]


def lane_times(steps):
    half = steps // 2
    rest = half + 1 - LANES
    room = LANES - rest
    lane = np.arange(LANES)
    first = np.where(lane < rest, LANES + lane, -1)
    first_odd = np.where(lane < rest - 1, LANES + lane, -1)
    second = np.where(lane >= room, LANES + lane - room, -1)
    tail_a = np.where(lane >= rest, LANES + lane - rest, -1)
    tail_b = np.where(lane < rest - 1 - room, LANES + room + lane, -1)
    return lane, first, first_odd, second, tail_a, tail_b


def fold_maps(steps):
    lane, first, first_odd, second, tail_a, tail_b = lane_times(steps)
    shared = np.where(second >= 0, second, tail_b)
    even = np.concatenate([lane, lane, first, first_odd])
    odd = np.concatenate([lane, lane, tail_a, shared])
    ones = np.ones(LANES, np.int64)
    even_sign = np.concatenate([ones, -ones, ones, -ones])
    odd_sign = np.concatenate([ones, -ones, -ones, np.where(second >= 0, 1, -1)])
    maps = np.full((8, 4 * LANES), -1, np.int32)
    for index, (time, sign) in enumerate(((even, even_sign), (odd, odd_sign))):
        mirror = np.where((time > 0) & (2 * time != steps), steps - time, -1)
        maps[3 * index] = time
        maps[3 * index + 1] = np.where(time < 0, -1, mirror)
        maps[3 * index + 2] = sign
    return maps


def halves(values):
    high = values.astype(jnp.bfloat16)
    return high, (values - high.astype(np.float32)).astype(jnp.bfloat16)


def batch_shares(batch):
    first = -(-batch // (2 * GROUP)) * GROUP
    return ((0, first), (first, batch - first))


def paired_tables(steps, freqs, groups, rows_pad, wide):
    half = steps // 2
    lane, first, first_odd, second, tail_a, tail_b = lane_times(steps)
    tail = np.where(tail_a >= 0, tail_a, tail_b)
    forward, backward = [], []
    for bins in frequency_order(freqs, groups):
        count = bins.shape[0]
        known = (bins < freqs)[:, None]
        even = (bins % 2 == 0)[:, None]
        angle = bins[:, None] * np.arange(steps)[None, :] % (2 * steps)
        phase = np.pi / steps * angle
        sine = np.where(angle % steps == 0, 0.0, np.sin(phase))
        cosine = np.cos(phase)
        symmetric = np.where(known, np.where(even, cosine, -sine), 0.0)
        other = np.where(known, np.where(even, -sine, cosine), 0.0)
        blocks = []
        for table, times in (
            (symmetric, lane), (other, lane), (symmetric, first), (other, first_odd), (symmetric, second), (other, tail),
        ):
            limit = half if table is symmetric else half - 1
            inside = (times >= 0) & (times <= limit)
            value = np.where(inside[None, :], table[:, np.clip(times, 0, limit)], 0.0).astype(np.float32)
            block = np.zeros((2, rows_pad, LANES), jnp.bfloat16)
            block[0, :count], block[1, :count] = halves(value)
            blocks.append(block.reshape(2 * rows_pad, LANES))
        forward.append(np.stack(blocks))
        weight = np.where((bins == 0) | (bins == steps), 0.5, 1.0)[:, None] / steps
        inverse = np.zeros((2, 2, 2, LANES, wide), jnp.bfloat16)
        batch = groups // BATCHES * GROUP
        for position, table in enumerate((symmetric, other)):
            value = (table * weight).astype(np.float32)
            for turn in range(BATCHES):
                for share, (begin, size) in enumerate(batch_shares(batch)):
                    target = slice(turn * batch_shares(batch)[0][1], turn * batch_shares(batch)[0][1] + size)
                    source = slice(turn * batch + begin, turn * batch + begin + size)
                    parts = halves(value[source])
                    for index in range(2):
                        inverse[index, position, share, target, :steps] = parts[index]
        backward.append(inverse)
    return np.stack(forward), np.stack(backward)


def kernel(
    n, lines, vectors, local, steps, points, freqs, groups, wide,
    data_ref, spectra_ref, forward_ref, backward_ref, maps_ref,
    out_ref, rms_ref,
    series, fold, raw, packed, kbuf, gathered, table, inverse, spectrum, product_s, own_val, send_val, recv_val,
    partial, pair, square, squares,
    load_sem, raw_sem, k_send, k_recv, z_send, z_recv, y_send, y_recv, c_send, c_recv, w_send, w_recv,
    v_send, v_recv, f_send, f_recv, r_send, r_recv,
):
    me = lax.axis_index("param")
    core = lax.axis_index("sensor")
    x = lax.rem(me, 2)
    y = lax.rem(me // 2, 2)
    z = me // 4
    plane = 4
    other_chip = me + 1 - 2 * x
    y_chip = me + 2 - 4 * y
    other_core = 1 - core
    z_mate = z + 1 - 2 * lax.rem(z, 2)
    half = steps // 2
    rest = half + 1 - LANES
    rows = points * GROUP
    count = groups * GROUP
    pieces = groups // PIECE
    span = PIECE * 2 * GROUP
    pitch = 2 * vectors + PAD_ROWS
    batch = groups // BATCHES

    barrier = pltpu.get_barrier_semaphore()

    for neighbour in ((other_chip, core), (other_chip, other_core), (y_chip, core), (me, other_core)):
        pl.semaphore_signal(barrier, inc=1, device_id=neighbour, device_id_type=MESH)

    @pl.when(z > 0)
    def _():
        pl.semaphore_signal(barrier, inc=1, device_id=(me - plane, core), device_id_type=MESH)

    @pl.when(z + 1 < lines)
    def _():
        pl.semaphore_signal(barrier, inc=1, device_id=(me + plane, core), device_id_type=MESH)

    def filled(piece, target):
        known = -(-(freqs - target * GROUP) // (2 * GROUP))
        return min(PIECE, known - piece * PIECE)

    def raw_copy(piece):
        begin = piece * span
        size = min(span, freqs - begin)
        return pltpu.make_async_copy(
            spectra_ref.at[:, pl.ds(begin, size)], raw.at[:, pl.ds(begin, size)], raw_sem.at[piece]
        )

    data_copy = pltpu.make_async_copy(data_ref, series, load_sem.at[0])
    forward_copy = pltpu.make_async_copy(forward_ref.at[core], table, load_sem.at[1])
    backward_copies = [
        pltpu.make_async_copy(backward_ref.at[source], inverse.at[index], load_sem.at[2 + index])
        for index, source in enumerate((core, other_core))
    ]
    data_copy.start()
    raw_copy(0).start()
    for piece in range(1, pieces):
        raw_copy(piece).start()
    forward_copy.start()
    for backward_copy in backward_copies:
        backward_copy.start()

    strip = 64

    @pl.loop(0, fold.shape[1] // strip)
    def _(part):
        begin = pl.multiple_of(part * strip, strip)
        time = lax.broadcasted_iota(jnp.int32, (strip, 4 * LANES), 0) + begin
        for side in range(2):
            direct = jnp.where(time == maps_ref[3 * side : 3 * side + 1, :], 1.0, 0.0)
            sign = maps_ref[3 * side + 2 : 3 * side + 3, :].astype(jnp.float32)
            mirror = jnp.where(time == maps_ref[3 * side + 1 : 3 * side + 2, :], sign, 0.0)
            fold[side, pl.ds(begin, strip), :] = (direct + mirror).astype(jnp.bfloat16)

    upper = lax.broadcasted_iota(jnp.int32, (8, LANES), 0) < points
    stripe = lax.broadcasted_iota(jnp.int32, (8, LANES), 1) // local % 2 == 0

    def sort_piece(piece):
        @pl.loop(0, 2)
        def _(part):
            @pl.loop(piece * PIECE, (piece + 1) * PIECE)
            def _(group):
                for side in range(2):
                    for duo in range(GROUP // 2):
                        begin = group * 2 * GROUP + side * GROUP + 2 * duo
                        first = raw[part, begin]
                        second = raw[part, begin + 1]
                        low = jnp.where(upper, first, pltpu.roll(second, points, 0))
                        high = jnp.where(upper, pltpu.roll(first, points, 0), second)
                        packed[0, part, group, side, duo] = jnp.where(stripe, low, pltpu.roll(high, local, 1))
                        packed[1, part, group, side, duo] = jnp.where(stripe, pltpu.roll(high, LANES - local, 1), low)

    def k_copy(piece, target):
        begin = piece * PIECE
        size = filled(piece, target)
        rel = core if target == 0 else other_core
        return pltpu.make_async_remote_copy(
            src_ref=packed.at[1 - x, :, pl.ds(begin, size), target],
            dst_ref=kbuf.at[1 + rel, :, pl.ds(begin, size)],
            send_sem=k_send.at[target], recv_sem=k_recv.at[piece // (pieces // BATCHES)],
            device_id=(other_chip, target), device_id_type=MESH,
        )

    def k_keep(piece):
        begin = piece * PIECE
        return pltpu.make_async_remote_copy(
            src_ref=packed.at[x, :, pl.ds(begin, PIECE), other_core],
            dst_ref=kbuf.at[0, :, pl.ds(begin, PIECE)],
            send_sem=k_send.at[2], recv_sem=k_recv.at[piece // (pieces // BATCHES)],
            device_id=(me, other_core), device_id_type=MESH,
        )

    def all_of(ref, send_sem, recv_sem):
        return pltpu.make_async_remote_copy(
            src_ref=ref, dst_ref=ref, send_sem=send_sem, recv_sem=recv_sem,
            device_id=(me, other_core), device_id_type=MESH,
        )

    def wait_batch(turn):
        begin = turn * batch
        full = all_of(kbuf.at[:, :, pl.ds(begin, batch)], k_send.at[2], k_recv.at[turn])
        missing = 0 if turn + 1 < BATCHES else 2 * (PIECE - filled(pieces - 1, 1))
        if missing:
            short = all_of(packed.at[0, 0, pl.ds(0, 3 * batch - missing)], k_send.at[2], k_recv.at[turn])
            pl.when(core == 0)(full.wait_recv)
            pl.when(core == 1)(short.wait_recv)
        else:
            full.wait_recv()

    def send_piece(piece):
        for target in range(2):
            k_copy(piece, target).start()
        k_keep(piece).start()

    def slot(line, row, column):
        return line * plane + row * 2 + column

    def place(line, row):
        upper_line = line // 2
        return lax.rem(line, 2) * plane + row * 2 + upper_line + x - 2 * upper_line * x

    def block(chunk, line, row, rel=0):
        position = rel * (n // 2) + place(line, row)
        row_range = pl.ds(pl.multiple_of(position * local, local), local)
        return gathered.at[chunk, row_range, pl.ds(0, wide_now[0] * LANES)]

    data_copy.wait()
    plain = (((1,), (0,)), ((), ()))
    folded = []
    for side in range(2):
        values = jnp.concatenate([series[side * CHUNKS + chunk] for chunk in range(CHUNKS)], axis=0)
        high = values.astype(jnp.bfloat16)
        left = values - high.astype(jnp.float32)
        middle = left.astype(jnp.bfloat16)
        low = (left - middle.astype(jnp.float32)).astype(jnp.bfloat16)
        result = lax.dot_general(
            jnp.concatenate([high, middle, low], axis=0), fold[side, :steps, :], plain,
            preferred_element_type=jnp.float32,
        )
        size = CHUNKS * local
        folded.append(result[:size] + (result[size : 2 * size] + result[2 * size :]))
    own_row = pl.ds(pl.multiple_of(place(z, y) * local, local), local)
    lane_index = lax.broadcasted_iota(jnp.int32, (gathered.shape[1], LANES), 1)
    lane_small = lax.broadcasted_iota(jnp.int32, (local, LANES), 1)
    spare = LANES - (rest - 1)

    def folded_block(side, chunk, index):
        return folded[side][chunk * local : (chunk + 1) * local, index * LANES : (index + 1) * LANES]

    for chunk in range(CHUNKS):
        for index in range(2):
            gathered[chunk, own_row, index * LANES : (index + 1) * LANES] = folded_block(0, chunk, index)
            gathered[chunk, own_row, (2 + index) * LANES : (3 + index) * LANES] = folded_block(1, chunk, index)
        gathered[chunk, own_row, 4 * LANES : 5 * LANES] = folded_block(0, chunk, 2) + folded_block(1, chunk, 2)
        gathered[chunk, own_row, 5 * LANES : 6 * LANES] = folded_block(1, chunk, 3)
        if chunk < CHUNKS - NARROW:
            last = folded_block(0, chunk, 3)
            if chunk < 2 * NARROW:
                guest = folded_block(0, CHUNKS - NARROW + chunk // 2, 3)
                shift = rest - 1 - chunk % 2 * spare
                last = jnp.where(lane_small >= rest - 1, pltpu.roll(guest, shift, 1), last)
            gathered[chunk, own_row, 6 * LANES :] = last

    def unpack(chunk):
        source = 2 * (chunk - (CHUNKS - NARROW))
        begin = 6 * LANES
        near = pltpu.roll(gathered[source, :, begin:], spare, 1)
        far = pltpu.roll(gathered[source + 1, :, begin:], LANES - (rest - 1 - spare), 1)
        gathered[chunk, :, begin:] = jnp.where(lane_index < spare, near, far)

    wide_now = [7]

    def send(source, target, send_sem, recv_sem):
        return pltpu.make_async_remote_copy(
            src_ref=source, dst_ref=source, send_sem=send_sem, recv_sem=recv_sem,
            device_id=target, device_id_type=MESH,
        )

    def some(blocks, send_sem, recv_sem):
        return all_of(gathered.at[0, pl.ds(0, blocks * local), pl.ds(0, wide_now[0] * LANES)], send_sem, recv_sem)

    def tiles(number, send_sem, recv_sem):
        if number <= raw.shape[1]:
            return all_of(raw.at[0, pl.ds(0, number)], send_sem, recv_sem)
        assert number % 2 == 0
        return all_of(raw.at[:, pl.ds(0, number // 2)], send_sem, recv_sem)

    def line_index(source, target):
        return jnp.where(source < target, source, source - 1)

    def line_copy(chunk, step, way):
        source = jnp.clip(z - way * step, 0, lines - 1)
        target = jnp.clip(z + way, 0, lines - 1)
        return send(
            block(chunk, source, y), (slot(target, y, x), core),
            z_send.at[0], z_recv.at[chunk, jnp.clip(line_index(source, target), 0, lines - 2)],
        )

    def line_arrival(chunk, step, way):
        source = jnp.clip(z - way * (step + 1), 0, lines - 1)
        target = jnp.clip(z + way, 0, lines - 1)
        return source, send(
            block(chunk, source, y), (slot(target, y, x), core),
            z_send.at[0], z_recv.at[chunk, jnp.clip(line_index(source, z), 0, lines - 2)],
        )

    def sends(step, way):
        inside = z + 1 < lines if way > 0 else z > 0
        begun = z >= step if way > 0 else z + step < lines
        return jnp.logical_and(inside, begun)

    def receives(step, way):
        return z >= step + 1 if way > 0 else z + step + 1 < lines

    def y_copy(chunk, line):
        index = jnp.where(line == z, 0, 1)
        return send(block(chunk, line, y), (y_chip, core), y_send.at[0], y_recv.at[chunk, index])

    def turn_copy(chunk):
        return send(block(chunk, z, 1 - y), (slot(z_mate, y, x), core), w_send.at[0], w_recv.at[chunk])

    def turn_arrival(chunk):
        return send(block(chunk, z_mate, 1 - y), (slot(z_mate, y, x), core), w_send.at[0], w_recv.at[chunk])

    def turns(chunk):
        return chunk >= CHUNKS // 2

    def by_row(chunk, line):
        return jnp.logical_not(jnp.logical_and(turns(chunk), line == z_mate))

    def core_copy(chunk, row, line):
        return pltpu.make_async_remote_copy(
            src_ref=block(chunk, line, row), dst_ref=block(chunk, line, row, 1),
            send_sem=c_send.at[0], recv_sem=c_recv.at[chunk],
            device_id=(me, other_core), device_id_type=MESH,
        )

    def start_lines(chunk):
        for way in (1, -1):

            @pl.when(sends(0, way))
            def _():
                line_copy(chunk, 0, way).start()

        y_copy(chunk, z).start()
        core_copy(chunk, y, z).start()

    def from_lines(chunk, step):
        for way in (1, -1):

            @pl.when(receives(step, way))
            def _():
                source, arrival = line_arrival(chunk, step, way)
                arrival.wait_recv()
                if step + 1 < lines - 1:

                    @pl.when(sends(step + 1, way))
                    def _():
                        line_copy(chunk, step + 1, way).start()

                @pl.when(by_row(chunk, source))
                def _():
                    y_copy(chunk, source).start()

                core_copy(chunk, y, source).start()

    def from_mate(chunk):
        some(1, y_send.at[0], y_recv.at[chunk, 0]).wait_recv()
        core_copy(chunk, 1 - y, z).start()

    def to_mate(chunk):
        @pl.when(turns(chunk))
        def _():
            turn_copy(chunk).start()

    def from_row(chunk):
        @pl.when(turns(chunk))
        def _():
            some(lines - 2, y_send.at[0], y_recv.at[chunk, 1]).wait_recv()
            turn_arrival(chunk).wait_recv()

        @pl.when(jnp.logical_not(turns(chunk)))
        def _():
            some(lines - 1, y_send.at[0], y_recv.at[chunk, 1]).wait_recv()

        for step in range(1, lines):
            core_copy(chunk, 1 - y, lax.rem(z + step, lines)).start()

    def from_core(chunk):
        some(n // 2, c_send.at[0], c_recv.at[chunk]).wait_recv()


    def transform(chunk):
        def lanes(index):
            return gathered[chunk, :, index * LANES : (index + 1) * LANES]

        for which in range(4):
            odd = which // 2
            position = which % 2
            if which < 2:
                tail = lanes(4 + 2 * which)
            elif which == 2:
                tail = lanes(5)
            else:
                tail = jnp.where(lane_index >= rest, lanes(4), lanes(5))
            right = split(jnp.concatenate([lanes(which), tail], axis=1))
            left = jnp.concatenate([table[position], table[2 + which]], axis=1)
            result = split_product(left, count, right)
            for lane in range(2):
                spectrum[lane, pl.ds(odd * vectors + position * CHUNKS + chunk, count, stride=pitch), :] = result[
                    :, lane * LANES : (lane + 1) * LANES
                ]

    pl.semaphore_wait(barrier, 4 + jnp.minimum(z, 1) + jnp.minimum(lines - 1 - z, 1))
    def at_width(blocks, action):
        def run(chunk):
            wide_now[0] = blocks
            action(chunk)

        return run

    pl.loop(0, CHUNKS - NARROW)(at_width(7, start_lines))
    pl.loop(CHUNKS - NARROW, CHUNKS)(at_width(6, start_lines))

    raw[:, freqs:] = jnp.zeros((2, raw.shape[1] - freqs) + tuple(raw.shape[2:]), jnp.float32)
    short = filled(pieces - 1, 1)
    if short < PIECE:

        @pl.when(core == 1)
        def _():
            begin = (pieces - 1) * PIECE + short
            for owner in range(1, 3):
                kbuf[owner, :, begin:] = jnp.zeros((2, PIECE - short) + tuple(kbuf.shape[3:]), jnp.float32)


    for piece in range(pieces):
        raw_copy(piece).wait()
        sort_piece(piece)
        send_piece(piece)

    forward_copy.wait()
    for backward_copy in backward_copies:
        backward_copy.wait()

    def finish(chunk):
        @pl.when(chunk >= CHUNKS - NARROW)
        def _():
            unpack(chunk)

        transform(chunk)

    stages = [
        (functools.partial(from_lines, step=0), 0), (from_mate, 0),
        (functools.partial(from_lines, step=1), 2), (functools.partial(from_lines, step=2), 3), (to_mate, 4),
        (from_row, 6), (from_core, 7),
    ]
    last_age = stages[-1][1]

    @pl.loop(0, CHUNKS + last_age)
    def _(turn):
        for stage, age in stages:
            chunk = turn - age
            for blocks, begin, end in ((7, 0, CHUNKS - NARROW), (6, CHUNKS - NARROW, CHUNKS)):

                @pl.when(jnp.logical_and(chunk >= begin, chunk < end))
                def _():
                    at_width(blocks, stage)(chunk)

        pl.when(turn >= last_age)(lambda: finish(turn - last_age))

    columns = GROUP * 2 * vectors
    row_freq = lax.broadcasted_iota(jnp.int32, (4 * rows, columns), 0) // points % GROUP
    col_freq = lax.broadcasted_iota(jnp.int32, (4 * rows, columns), 1) // (2 * vectors)
    own = row_freq == col_freq
    lane = lax.broadcasted_iota(jnp.int32, (2 * rows, LANES), 1)
    row = lax.broadcasted_iota(jnp.int32, (2 * rows, LANES), 0) // points % 2
    first_half = lane % vectors < vectors // 2
    sign = jnp.where(first_half == (row == 0), 1.0, -1.0)
    shares = batch_shares(batch * GROUP)
    step_rows = shares[0][1]
    lane_group = lax.broadcasted_iota(jnp.int32, (step_rows, LANES), 1) // vectors
    known_rows = lax.broadcasted_iota(jnp.int32, (step_rows, LANES), 0) < shares[1][1]

    def value_rows(turn):
        return pl.ds(pl.multiple_of(turn * step_rows, GROUP), step_rows)

    def value_copy(turn, target):
        place_rows = value_rows(turn)
        return pltpu.make_async_remote_copy(
            src_ref=send_val.at[target, place_rows],
            dst_ref=recv_val.at[jnp.where(core == target, 0, 2), place_rows],
            send_sem=v_send.at[0], recv_sem=v_recv.at[0],
            device_id=(other_chip, target), device_id_type=MESH,
        )

    def value_keep(turn):
        place_rows = value_rows(turn)
        return pltpu.make_async_remote_copy(
            src_ref=send_val.at[2, place_rows], dst_ref=recv_val.at[1, place_rows],
            send_sem=v_send.at[0], recv_sem=v_recv.at[0],
            device_id=(me, other_core), device_id_type=MESH,
        )

    @pl.loop(0, BATCHES)
    def _(turn):
        for which in range(BATCHES):

            @pl.when(turn == which)
            def _():
                wait_batch(which)

        for step in range(batch):
            group = turn * batch + step
            begin = pl.multiple_of(group * GROUP * pitch, GROUP)
            sides = []
            for side in range(2):
                pieces_of = [spectrum[side, pl.ds(begin + step_f * pitch, 2 * vectors), :] for step_f in range(GROUP)]
                sides.append(jnp.concatenate(pieces_of, axis=0))
            right = split(jnp.concatenate(sides, axis=1))
            parts = []
            for part in range(2):
                for near, far in (
                    (packed[x, part, group, core], kbuf[0, part, group]), (kbuf[1, part, group], kbuf[2, part, group]),
                ):
                    parts.append(jnp.concatenate([near.reshape(rows, LANES), far.reshape(rows, LANES)], axis=1))
            left = jnp.concatenate(parts, axis=0)
            found = jnp.where(own, product(split(left), right, NT_DIMS), 0.0)
            width = columns
            while width > LANES:
                width //= 2
                found = found[:, :width] + found[:, width:]
            hop = LANES // 2
            while hop >= 2 * vectors:
                found = found + pltpu.roll(found, hop, 1)
                hop //= 2
            turned = found[2 * rows :]
            turned = jnp.where(
                first_half, pltpu.roll(turned, LANES - vectors // 2, 1), pltpu.roll(turned, vectors // 2, 1)
            )
            value = found[: 2 * rows] + sign * turned
            for owner in range(2):
                product_s[owner, pl.ds(pl.multiple_of(group * rows, rows), rows), :] = value[
                    owner * rows : (owner + 1) * rows
                ]
        for owner in (1, 0):
            merged = [jnp.zeros((step_rows, LANES), jnp.float32)] * 2
            for share in range(2):
                for point in range(points):
                    begin = (turn * batch * GROUP + shares[share][0]) * points + point
                    value = product_s[owner, pl.ds(begin, step_rows, stride=points), :]
                    if share == 1:
                        value = jnp.where(known_rows, value, 0.0)
                    shifted = pltpu.roll(value, vectors, 1)
                    index = share * points + point
                    for target in range(2):
                        chosen = value if index % 2 == target else shifted
                        merged[target] = jnp.where(lane_group == index, chosen, merged[target])
            if owner == 1:
                for target in range(2):
                    send_val[target, value_rows(turn), :] = merged[target]
                for target in range(2):
                    value_copy(turn, target).start()
            else:
                send_val[2, value_rows(turn), :] = jnp.where(core == 0, merged[1], merged[0])
                own_val[value_rows(turn), :] = jnp.where(core == 0, merged[0], merged[1])
                value_keep(turn).start()

    sent = BATCHES * step_rows
    all_of(recv_val.at[:, pl.ds(0, sent)], v_send.at[0], v_recv.at[0]).wait_recv()

    own_half = vectors // 2
    blocks = []
    for near in (own_val[:sent, :] + recv_val[0, :sent, :], recv_val[1, :sent, :] + recv_val[2, :sent, :]):
        turned = jnp.concatenate([near, jnp.zeros((LANES - sent, LANES), jnp.float32)], axis=0).T
        for position in range(2):
            for share in range(2):
                begins = [
                    ((share * points + point) * 2 + position) * own_half for point in range(points)
                ]
                blocks.append(jnp.concatenate([turned[begin : begin + own_half] for begin in begins], axis=0))
    left = split(jnp.concatenate(blocks, axis=1))
    right = []
    for index in range(2):
        right.append(jnp.concatenate([inverse[near, index].reshape(4 * LANES, wide) for near in range(2)], axis=0))
    total = product(left, right, plain)
    partial[...] = total

    field_copy = pltpu.make_async_remote_copy(
        src_ref=partial, dst_ref=pair, send_sem=f_send.at[0], recv_sem=f_recv.at[0],
        device_id=(me, other_core), device_id_type=MESH,
    )

    energy = total * total
    summed = energy[:own_half]
    for point in range(1, points):
        summed = summed + energy[point * own_half : (point + 1) * own_half]
    column = jnp.sum(summed, axis=1, keepdims=True)
    lane8 = lax.broadcasted_iota(jnp.int32, (own_half, LANES), 1)
    row8 = lax.broadcasted_iota(jnp.int32, (own_half, LANES), 0)
    flat = jnp.sum(jnp.where(lane8 == row8 + core * own_half, column, 0.0), axis=0, keepdims=True)
    square[...] = flat
    mine = core * n + me
    squares[mine] = flat

    def square_copy(target, target_core):
        return pltpu.make_async_remote_copy(
            src_ref=square, dst_ref=squares.at[mine], send_sem=r_send.at[0], recv_sem=r_recv.at[0],
            device_id=(target, target_core), device_id_type=MESH,
        )

    @pl.loop(1, n)
    def _(step):
        square_copy(lax.rem(me + step, n), core).start()
        square_copy(lax.rem(me + step, n), other_core).start()

    square_copy(me, other_core).start()
    field_copy.start()

    block_tiles = local // 8
    every = sum(7 if chunk < CHUNKS - NARROW else 6 for chunk in range(CHUNKS)) * block_tiles
    late = sum(7 if chunk < CHUNKS - NARROW else 6 for chunk in range(CHUNKS // 2, CHUNKS)) * block_tiles
    for line in range(lines):
        ahead = line + 1 if line + 1 < lines else 0
        back = lines - line if line > 0 else 0

        @pl.when(z == line)
        def _():
            tiles((ahead + back) * every, z_send.at[0], z_recv.at[0, 0]).wait_send()

    tiles(lines * every - late, y_send.at[0], y_recv.at[0, 0]).wait_send()
    tiles(late, w_send.at[0], w_recv.at[0]).wait_send()
    tiles(n // 2 * every, c_send.at[0], c_recv.at[0]).wait_send()
    for target in range(2):
        all_of(packed.at[0, :, pl.ds(0, groups - PIECE + filled(pieces - 1, target)), target],
               k_send.at[target], k_recv.at[0]).wait_send()
    all_of(packed.at[0, :, :, 0], k_send.at[2], k_recv.at[0]).wait_send()
    all_of(send_val.at[:, pl.ds(0, sent)], v_send.at[0], v_recv.at[0]).wait_send()
    field_copy.wait_send()

    field_copy.wait_recv()
    tall = points * own_half
    out_ref[pl.ds(pl.multiple_of(core * tall, tall), tall), :] = total
    out_ref[pl.ds(pl.multiple_of(other_core * tall, tall), tall), :] = pair[...]
    all_of(squares.at[pl.ds(0, 2 * n - 1)], r_send.at[0], r_recv.at[0]).wait()

    energy_all = squares[0]
    for device in range(1, 2 * n):
        energy_all = energy_all + squares[device]
    scale = jnp.sqrt(energy_all / (points * n * steps) + 1e-06)
    rms_ref[...] = jnp.broadcast_to(scale, rms_ref.shape)


def finish_kernel(field_ref, scale_ref, out_ref, rms_ref):
    vectors, points, steps = out_ref.shape
    scale = scale_ref[:1]
    rms_ref[...] = scale[0, :vectors]
    diagonal = lax.broadcasted_iota(jnp.int32, (vectors, LANES), 0) == lax.broadcasted_iota(
        jnp.int32, (vectors, LANES), 1
    )
    spread = jnp.broadcast_to(scale, (vectors, LANES))
    divisor = jnp.sum(jnp.where(diagonal, spread, 0.0), axis=1, keepdims=True)
    half = vectors // 2
    for point in range(points):
        near = field_ref[point * half : (point + 1) * half, :steps]
        far = field_ref[(points + point) * half : (points + point + 1) * half, :steps]
        out_ref[:, point, :] = jnp.concatenate([near, far], axis=0) / divisor


def paired_body(data, spectra):
    n = lax.axis_size("param")
    vectors, local, steps = data.shape
    sensors, points, freqs = spectra.shape[1:]
    wide = -(-steps // LANES) * LANES
    groups = -(-freqs // (2 * GROUP))
    count = groups * GROUP
    rows_pad = -(-count // 16) * 16
    pieces = groups // PIECE
    lines = n // 4
    forward, backward = paired_tables(steps, freqs, groups, rows_pad, wide)
    maps = fold_maps(steps)

    turned = jnp.transpose(spectra, (0, 3, 2, 1)).reshape(2, freqs, points, 2, LANES)
    turned = jnp.transpose(turned, (0, 1, 3, 2, 4)).reshape(2, freqs, 2 * points, LANES)

    hbm = pl.BlockSpec(memory_space=pl.ANY)
    vmem = pl.BlockSpec(memory_space=pltpu.VMEM)
    dma = pltpu.SemaphoreType.DMA
    f32, bf16 = jnp.float32, jnp.bfloat16
    fields, scale = pl.pallas_call(
        functools.partial(kernel, n, lines, vectors, local, steps, points, freqs, groups, wide),
        out_shape=(
            pltpu.VMEM((points * vectors, wide), f32),
            pltpu.VMEM((8, LANES), f32),
        ),
        in_specs=[hbm, hbm, hbm, hbm, vmem],
        out_specs=(vmem, vmem),
        scratch_shapes=[
            pltpu.VMEM((vectors, local, steps), f32),
            pltpu.VMEM((2, wide, 4 * LANES), bf16),
            pltpu.VMEM((2, 2 * count, 2 * points, LANES), f32),
            pltpu.VMEM((2, 2, groups, 2, GROUP // 2, 2 * points, LANES), f32),
            pltpu.VMEM((3, 2, groups, GROUP // 2, 2 * points, LANES), f32),
            pltpu.VMEM((CHUNKS, sensors, 7 * LANES), f32),
            pltpu.VMEM((6, 2 * rows_pad, LANES), bf16),
            pltpu.VMEM((2, 2, 2, 2, LANES, wide), bf16),
            pltpu.VMEM((2, count * (2 * vectors + PAD_ROWS), LANES), f32),
            pltpu.VMEM((2, (count + GROUP) * points, LANES), f32),
            pltpu.VMEM((LANES, LANES), f32),
            pltpu.VMEM((3, LANES, LANES), f32),
            pltpu.VMEM((3, LANES, LANES), f32),
            pltpu.VMEM((points * vectors // 2, wide), f32),
            pltpu.VMEM((points * vectors // 2, wide), f32),
            pltpu.VMEM((1, LANES), f32),
            pltpu.VMEM((2 * n, 1, LANES), f32),
            dma((4,)),
            dma((pieces,)),
            dma((3,)), dma((BATCHES,)),
            dma((1,)), dma((CHUNKS, lines - 1)),
            dma((1,)), dma((CHUNKS, 2)),
            dma((1,)), dma((CHUNKS,)),
            dma((1,)), dma((CHUNKS,)),
            dma((1,)), dma((1,)),
            dma((1,)), dma((1,)),
            dma((1,)), dma((1,)),
        ],
        compiler_params=pltpu.CompilerParams(
            collective_id=0, has_side_effects=True, vmem_limit_bytes=60 * 1024 * 1024
        ),
    )(data, turned, jnp.asarray(forward), jnp.asarray(backward), jnp.asarray(maps))
    return pl.pallas_call(
        finish_kernel,
        out_shape=(jax.ShapeDtypeStruct((vectors, points, steps), f32), jax.ShapeDtypeStruct((vectors,), f32)),
        in_specs=[vmem, vmem],
        out_specs=(vmem, vmem),
    )(pltpu.with_memory_space_constraint(fields, pltpu.VMEM), pltpu.with_memory_space_constraint(scale, pltpu.VMEM))


def solution(mesh):
    in_specs = (P(None, ("sensor", "param"), None), P(None, "sensor", "param", None))
    out_specs = (P(None, "param", None), P())
    n = mesh.shape["param"]
    pair = mesh.shape["sensor"] == 2 and n == 16

    def body(data, spectra):
        vectors, local, _ = data.shape
        sensors, points = spectra.shape[1:3]
        fits = local * n == sensors and local % 8 == 0 and sensors == 2 * LANES and vectors == 2 * CHUNKS
        fits = fits and points * 2 * vectors == LANES and folded_layout_fits(data.shape[2])
        return (paired_body if pair and fits else general_body)(data, spectra)

    return jax.shard_map(body, mesh=mesh, in_specs=in_specs, out_specs=out_specs, check_vma=False)
```

```python
import functools
import math

import jax
import jax.numpy as jnp
import numpy as np
from jax import lax
from jax.experimental import pallas as pl
from jax.experimental.pallas import tpu as pltpu
from jax.sharding import PartitionSpec as P

MESH = pl.DeviceIdType.MESH
LANES = 128
GROUP = 8
CHUNKS = 8
PIECE = 3
BATCHES = 3
PAD_ROWS = 4
NARROW = 2


def spectral_tables(steps):
    length = 2 * steps
    freqs = steps + 1
    times = lax.broadcasted_iota(jnp.int32, (steps, freqs), 0)
    bins = lax.broadcasted_iota(jnp.int32, (steps, freqs), 1)
    phase = 2.0 * math.pi / length * (times * bins % length).astype(jnp.float32)
    forward = jnp.concatenate([jnp.cos(phase), -jnp.sin(phase)], axis=1)
    weight = jnp.where((bins == 0) | (bins == steps), 1.0, 2.0) / length
    backward = jnp.concatenate([(weight * jnp.cos(phase)).T, (-weight * jnp.sin(phase)).T], axis=0)
    return (forward, backward)


def to_spectrum(series, forward):
    vectors, sensors, steps = series.shape
    flat = jnp.dot(
        series.reshape(vectors * sensors, steps),
        forward,
        precision=lax.Precision.HIGHEST,
        preferred_element_type=jnp.float32,
    )
    return flat.reshape(vectors, sensors, forward.shape[1])


def contract(kernel, spectrum):
    return jnp.einsum(
        "spf,rsf->rpf",
        kernel,
        spectrum,
        precision=lax.Precision.HIGHEST,
        preferred_element_type=jnp.float32,
    )


def general_body(data, spectra):
    steps = data.shape[2]
    freqs = steps + 1
    forward, backward = spectral_tables(steps)
    whole = to_spectrum(lax.all_gather(data, "param", axis=1, tiled=True), forward)
    real_part = whole[..., :freqs]
    imag_part = whole[..., freqs:]
    kernel_re = spectra[0]
    kernel_im = spectra[1]
    out_re = contract(kernel_re, real_part) + contract(kernel_im, imag_part)
    out_im = contract(kernel_re, imag_part) - contract(kernel_im, real_part)
    vectors, points = (out_re.shape[0], out_re.shape[1])
    stacked = jnp.concatenate([out_re, out_im], axis=2).reshape(vectors * points, 2 * freqs)
    partial_field = jnp.dot(
        stacked, backward, precision=lax.Precision.HIGHEST, preferred_element_type=jnp.float32
    ).reshape(vectors, points, steps)
    count = points * lax.axis_size("param") * steps
    share = lax.psum_scatter(partial_field, "sensor", scatter_dimension=0, tiled=True)
    squares = lax.psum(jnp.sum(share * share, axis=(1, 2)), "param")
    scale = jnp.sqrt(squares / count + 1e-06)
    normalized = share / scale[:, None, None]
    gradient, rms_all = (
        lax.all_gather(normalized, "sensor", axis=0, tiled=True),
        lax.all_gather(scale, "sensor", axis=0, tiled=True),
    )
    return (gradient, rms_all)


def split(value):
    high = value.astype(jnp.bfloat16)
    return high, (value - high.astype(jnp.float32)).astype(jnp.bfloat16)


NT_DIMS = (((1,), (1,)), ((), ()))


def product(left, right, dims):
    dot = functools.partial(lax.dot_general, dimension_numbers=dims, preferred_element_type=jnp.float32)
    size = left[0].shape[0]
    both = dot(jnp.concatenate(left, axis=0), right[0])
    return both[:size] + (both[size:] + dot(left[0], right[1]))


def split_product(table, rows, right):
    dot = functools.partial(lax.dot_general, dimension_numbers=NT_DIMS, preferred_element_type=jnp.float32)
    half = table.shape[0] // 2
    both = dot(table, right[0])
    return both[:rows] + (both[half : half + rows] + dot(table[:half], right[1])[:rows])


def folded_layout_fits(steps):
    half = steps // 2
    rest = half + 1 - LANES
    groups = -(-(steps + 1) // (2 * GROUP))
    fits = rest - 1 <= 2 * (LANES - (rest - 1)) and steps % 2 == 0 and 0 < rest < LANES and half - LANES - (LANES - rest) <= LANES - rest
    fits = fits and groups % (PIECE * BATCHES) == 0
    return fits and BATCHES * batch_shares(groups // BATCHES * GROUP)[0][1] <= LANES


def frequency_order(freqs, groups):
    bins = np.arange(groups * 2 * GROUP).reshape(groups, 2, GROUP)
    return [bins[:, core].reshape(-1) for core in range(2)]


def lane_times(steps):
    half = steps // 2
    rest = half + 1 - LANES
    room = LANES - rest
    lane = np.arange(LANES)
    first = np.where(lane < rest, LANES + lane, -1)
    first_odd = np.where(lane < rest - 1, LANES + lane, -1)
    second = np.where(lane >= room, LANES + lane - room, -1)
    tail_a = np.where(lane >= rest, LANES + lane - rest, -1)
    tail_b = np.where(lane < rest - 1 - room, LANES + room + lane, -1)
    return lane, first, first_odd, second, tail_a, tail_b


def fold_maps(steps):
    lane, first, first_odd, second, tail_a, tail_b = lane_times(steps)
    shared = np.where(second >= 0, second, tail_b)
    even = np.concatenate([lane, lane, first, first_odd])
    odd = np.concatenate([lane, lane, tail_a, shared])
    ones = np.ones(LANES, np.int64)
    even_sign = np.concatenate([ones, -ones, ones, -ones])
    odd_sign = np.concatenate([ones, -ones, -ones, np.where(second >= 0, 1, -1)])
    maps = np.full((8, 4 * LANES), -1, np.int32)
    for index, (time, sign) in enumerate(((even, even_sign), (odd, odd_sign))):
        mirror = np.where((time > 0) & (2 * time != steps), steps - time, -1)
        maps[3 * index] = time
        maps[3 * index + 1] = np.where(time < 0, -1, mirror)
        maps[3 * index + 2] = sign
    return maps


def halves(values):
    high = values.astype(jnp.bfloat16)
    return high, (values - high.astype(np.float32)).astype(jnp.bfloat16)


def batch_shares(batch):
    first = -(-batch // (2 * GROUP)) * GROUP
    return ((0, first), (first, batch - first))


def paired_tables(steps, freqs, groups, rows_pad, wide):
    half = steps // 2
    lane, first, first_odd, second, tail_a, tail_b = lane_times(steps)
    tail = np.where(tail_a >= 0, tail_a, tail_b)
    forward, backward = [], []
    for bins in frequency_order(freqs, groups):
        count = bins.shape[0]
        known = (bins < freqs)[:, None]
        even = (bins % 2 == 0)[:, None]
        angle = bins[:, None] * np.arange(steps)[None, :] % (2 * steps)
        phase = np.pi / steps * angle
        sine = np.where(angle % steps == 0, 0.0, np.sin(phase))
        cosine = np.cos(phase)
        symmetric = np.where(known, np.where(even, cosine, -sine), 0.0)
        other = np.where(known, np.where(even, -sine, cosine), 0.0)
        blocks = []
        for table, times in (
            (symmetric, lane), (other, lane), (symmetric, first), (other, first_odd), (symmetric, second), (other, tail),
        ):
            limit = half if table is symmetric else half - 1
            inside = (times >= 0) & (times <= limit)
            value = np.where(inside[None, :], table[:, np.clip(times, 0, limit)], 0.0).astype(np.float32)
            block = np.zeros((2, rows_pad, LANES), jnp.bfloat16)
            block[0, :count], block[1, :count] = halves(value)
            blocks.append(block.reshape(2 * rows_pad, LANES))
        forward.append(np.stack(blocks))
        weight = np.where((bins == 0) | (bins == steps), 0.5, 1.0)[:, None] / steps
        inverse = np.zeros((2, 2, 2, LANES, wide), jnp.bfloat16)
        batch = groups // BATCHES * GROUP
        for position, table in enumerate((symmetric, other)):
            value = (table * weight).astype(np.float32)
            for turn in range(BATCHES):
                for share, (begin, size) in enumerate(batch_shares(batch)):
                    target = slice(turn * batch_shares(batch)[0][1], turn * batch_shares(batch)[0][1] + size)
                    source = slice(turn * batch + begin, turn * batch + begin + size)
                    parts = halves(value[source])
                    for index in range(2):
                        inverse[index, position, share, target, :steps] = parts[index]
        backward.append(inverse)
    return np.stack(forward), np.stack(backward)


def kernel(
    n, lines, vectors, local, steps, points, freqs, groups, wide,
    data_ref, spectra_ref, forward_ref, backward_ref, maps_ref,
    out_ref, rms_ref,
    series, fold, raw, packed, kbuf, gathered, table, inverse, spectrum, product_s, own_val, send_val, recv_val,
    partial, pair, square, squares,
    load_sem, raw_sem, k_send, k_recv, z_send, z_recv, y_send, y_recv, c_send, c_recv, w_send, w_recv,
    v_send, v_recv, f_send, f_recv, r_send, r_recv,
):
    me = lax.axis_index("param")
    core = lax.axis_index("sensor")
    x = lax.rem(me, 2)
    y = lax.rem(me // 2, 2)
    z = me // 4
    plane = 4
    other_chip = me + 1 - 2 * x
    y_chip = me + 2 - 4 * y
    other_core = 1 - core
    z_mate = z + 1 - 2 * lax.rem(z, 2)
    half = steps // 2
    rest = half + 1 - LANES
    rows = points * GROUP
    count = groups * GROUP
    pieces = groups // PIECE
    span = PIECE * 2 * GROUP
    pitch = 2 * vectors + PAD_ROWS
    batch = groups // BATCHES

    barrier = pltpu.get_barrier_semaphore()

    for neighbour in ((other_chip, core), (other_chip, other_core), (y_chip, core), (me, other_core)):
        pl.semaphore_signal(barrier, inc=1, device_id=neighbour, device_id_type=MESH)

    @pl.when(z > 0)
    def _():
        pl.semaphore_signal(barrier, inc=1, device_id=(me - plane, core), device_id_type=MESH)

    @pl.when(z + 1 < lines)
    def _():
        pl.semaphore_signal(barrier, inc=1, device_id=(me + plane, core), device_id_type=MESH)

    def filled(piece, target):
        known = -(-(freqs - target * GROUP) // (2 * GROUP))
        return min(PIECE, known - piece * PIECE)

    def raw_copy(piece):
        begin = piece * span
        size = min(span, freqs - begin)
        return pltpu.make_async_copy(
            spectra_ref.at[:, pl.ds(begin, size)], raw.at[:, pl.ds(begin, size)], raw_sem.at[piece]
        )

    data_copy = pltpu.make_async_copy(data_ref, series, load_sem.at[0])
    forward_copy = pltpu.make_async_copy(forward_ref.at[core], table, load_sem.at[1])
    backward_copies = [
        pltpu.make_async_copy(backward_ref.at[source], inverse.at[index], load_sem.at[2 + index])
        for index, source in enumerate((core, other_core))
    ]
    data_copy.start()
    raw_copy(0).start()
    for piece in range(1, pieces):
        raw_copy(piece).start()
    forward_copy.start()
    for backward_copy in backward_copies:
        backward_copy.start()

    strip = 64

    @pl.loop(0, fold.shape[1] // strip)
    def _(part):
        begin = pl.multiple_of(part * strip, strip)
        time = lax.broadcasted_iota(jnp.int32, (strip, 4 * LANES), 0) + begin
        for side in range(2):
            direct = jnp.where(time == maps_ref[3 * side : 3 * side + 1, :], 1.0, 0.0)
            sign = maps_ref[3 * side + 2 : 3 * side + 3, :].astype(jnp.float32)
            mirror = jnp.where(time == maps_ref[3 * side + 1 : 3 * side + 2, :], sign, 0.0)
            fold[side, pl.ds(begin, strip), :] = (direct + mirror).astype(jnp.bfloat16)

    upper = lax.broadcasted_iota(jnp.int32, (8, LANES), 0) < points
    stripe = lax.broadcasted_iota(jnp.int32, (8, LANES), 1) // local % 2 == 0

    def sort_piece(piece):
        @pl.loop(0, 2)
        def _(part):
            @pl.loop(piece * PIECE, (piece + 1) * PIECE)
            def _(group):
                for side in range(2):
                    for duo in range(GROUP // 2):
                        begin = group * 2 * GROUP + side * GROUP + 2 * duo
                        first = raw[part, begin]
                        second = raw[part, begin + 1]
                        low = jnp.where(upper, first, pltpu.roll(second, points, 0))
                        high = jnp.where(upper, pltpu.roll(first, points, 0), second)
                        packed[0, part, group, side, duo] = jnp.where(stripe, low, pltpu.roll(high, local, 1))
                        packed[1, part, group, side, duo] = jnp.where(stripe, pltpu.roll(high, LANES - local, 1), low)

    def k_copy(piece, target):
        begin = piece * PIECE
        size = filled(piece, target)
        rel = core if target == 0 else other_core
        return pltpu.make_async_remote_copy(
            src_ref=packed.at[1 - x, :, pl.ds(begin, size), target],
            dst_ref=kbuf.at[1 + rel, :, pl.ds(begin, size)],
            send_sem=k_send.at[target], recv_sem=k_recv.at[piece // (pieces // BATCHES)],
            device_id=(other_chip, target), device_id_type=MESH,
        )

    def k_keep(piece):
        begin = piece * PIECE
        return pltpu.make_async_remote_copy(
            src_ref=packed.at[x, :, pl.ds(begin, PIECE), other_core],
            dst_ref=kbuf.at[0, :, pl.ds(begin, PIECE)],
            send_sem=k_send.at[2], recv_sem=k_recv.at[piece // (pieces // BATCHES)],
            device_id=(me, other_core), device_id_type=MESH,
        )

    def all_of(ref, send_sem, recv_sem):
        return pltpu.make_async_remote_copy(
            src_ref=ref, dst_ref=ref, send_sem=send_sem, recv_sem=recv_sem,
            device_id=(me, other_core), device_id_type=MESH,
        )

    def wait_batch(turn):
        begin = turn * batch
        full = all_of(kbuf.at[:, :, pl.ds(begin, batch)], k_send.at[2], k_recv.at[turn])
        missing = 0 if turn + 1 < BATCHES else 2 * (PIECE - filled(pieces - 1, 1))
        if missing:
            short = all_of(packed.at[0, 0, pl.ds(0, 3 * batch - missing)], k_send.at[2], k_recv.at[turn])
            pl.when(core == 0)(full.wait_recv)
            pl.when(core == 1)(short.wait_recv)
        else:
            full.wait_recv()

    def send_piece(piece):
        for target in range(2):
            k_copy(piece, target).start()
        k_keep(piece).start()

    def slot(line, row, column):
        return line * plane + row * 2 + column

    def place(line, row):
        upper_line = line // 2
        return lax.rem(line, 2) * plane + row * 2 + upper_line + x - 2 * upper_line * x

    def block(chunk, line, row, rel=0):
        position = rel * (n // 2) + place(line, row)
        row_range = pl.ds(pl.multiple_of(position * local, local), local)
        return gathered.at[chunk, row_range, pl.ds(0, wide_now[0] * LANES)]

    data_copy.wait()
    plain = (((1,), (0,)), ((), ()))
    folded = []
    for side in range(2):
        values = jnp.concatenate([series[side * CHUNKS + chunk] for chunk in range(CHUNKS)], axis=0)
        high = values.astype(jnp.bfloat16)
        left = values - high.astype(jnp.float32)
        middle = left.astype(jnp.bfloat16)
        low = (left - middle.astype(jnp.float32)).astype(jnp.bfloat16)
        result = lax.dot_general(
            jnp.concatenate([high, middle, low], axis=0), fold[side, :steps, :], plain,
            preferred_element_type=jnp.float32,
        )
        size = CHUNKS * local
        folded.append(result[:size] + (result[size : 2 * size] + result[2 * size :]))
    own_row = pl.ds(pl.multiple_of(place(z, y) * local, local), local)
    lane_index = lax.broadcasted_iota(jnp.int32, (gathered.shape[1], LANES), 1)
    lane_small = lax.broadcasted_iota(jnp.int32, (local, LANES), 1)
    spare = LANES - (rest - 1)

    def folded_block(side, chunk, index):
        return folded[side][chunk * local : (chunk + 1) * local, index * LANES : (index + 1) * LANES]

    for chunk in range(CHUNKS):
        for index in range(2):
            gathered[chunk, own_row, index * LANES : (index + 1) * LANES] = folded_block(0, chunk, index)
            gathered[chunk, own_row, (2 + index) * LANES : (3 + index) * LANES] = folded_block(1, chunk, index)
        gathered[chunk, own_row, 4 * LANES : 5 * LANES] = folded_block(0, chunk, 2) + folded_block(1, chunk, 2)
        gathered[chunk, own_row, 5 * LANES : 6 * LANES] = folded_block(1, chunk, 3)
        if chunk < CHUNKS - NARROW:
            last = folded_block(0, chunk, 3)
            if chunk < 2 * NARROW:
                guest = folded_block(0, CHUNKS - NARROW + chunk // 2, 3)
                shift = rest - 1 - chunk % 2 * spare
                last = jnp.where(lane_small >= rest - 1, pltpu.roll(guest, shift, 1), last)
            gathered[chunk, own_row, 6 * LANES :] = last

    def unpack(chunk):
        source = 2 * (chunk - (CHUNKS - NARROW))
        begin = 6 * LANES
        near = pltpu.roll(gathered[source, :, begin:], spare, 1)
        far = pltpu.roll(gathered[source + 1, :, begin:], LANES - (rest - 1 - spare), 1)
        gathered[chunk, :, begin:] = jnp.where(lane_index < spare, near, far)

    wide_now = [7]

    def send(source, target, send_sem, recv_sem):
        return pltpu.make_async_remote_copy(
            src_ref=source, dst_ref=source, send_sem=send_sem, recv_sem=recv_sem,
            device_id=target, device_id_type=MESH,
        )

    def some(blocks, send_sem, recv_sem):
        return all_of(gathered.at[0, pl.ds(0, blocks * local), pl.ds(0, wide_now[0] * LANES)], send_sem, recv_sem)

    def tiles(number, send_sem, recv_sem):
        if number <= raw.shape[1]:
            return all_of(raw.at[0, pl.ds(0, number)], send_sem, recv_sem)
        assert number % 2 == 0
        return all_of(raw.at[:, pl.ds(0, number // 2)], send_sem, recv_sem)

    def line_index(source, target):
        return jnp.where(source < target, source, source - 1)

    def line_copy(chunk, step, way):
        source = jnp.clip(z - way * step, 0, lines - 1)
        target = jnp.clip(z + way, 0, lines - 1)
        return send(
            block(chunk, source, y), (slot(target, y, x), core),
            z_send.at[0], z_recv.at[chunk, jnp.clip(line_index(source, target), 0, lines - 2)],
        )

    def line_arrival(chunk, step, way):
        source = jnp.clip(z - way * (step + 1), 0, lines - 1)
        target = jnp.clip(z + way, 0, lines - 1)
        return source, send(
            block(chunk, source, y), (slot(target, y, x), core),
            z_send.at[0], z_recv.at[chunk, jnp.clip(line_index(source, z), 0, lines - 2)],
        )

    def sends(step, way):
        inside = z + 1 < lines if way > 0 else z > 0
        begun = z >= step if way > 0 else z + step < lines
        return jnp.logical_and(inside, begun)

    def receives(step, way):
        return z >= step + 1 if way > 0 else z + step + 1 < lines

    def y_copy(chunk, line):
        index = jnp.where(line == z, 0, 1)
        return send(block(chunk, line, y), (y_chip, core), y_send.at[0], y_recv.at[chunk, index])

    def turn_copy(chunk):
        return send(block(chunk, z, 1 - y), (slot(z_mate, y, x), core), w_send.at[0], w_recv.at[chunk])

    def turn_arrival(chunk):
        return send(block(chunk, z_mate, 1 - y), (slot(z_mate, y, x), core), w_send.at[0], w_recv.at[chunk])

    def turns(chunk):
        return chunk >= CHUNKS // 2

    def by_row(chunk, line):
        return jnp.logical_not(jnp.logical_and(turns(chunk), line == z_mate))

    def core_copy(chunk, row, line):
        return pltpu.make_async_remote_copy(
            src_ref=block(chunk, line, row), dst_ref=block(chunk, line, row, 1),
            send_sem=c_send.at[0], recv_sem=c_recv.at[chunk],
            device_id=(me, other_core), device_id_type=MESH,
        )

    def start_lines(chunk):
        for way in (1, -1):

            @pl.when(sends(0, way))
            def _():
                line_copy(chunk, 0, way).start()

        y_copy(chunk, z).start()
        core_copy(chunk, y, z).start()

    def from_lines(chunk, step):
        for way in (1, -1):

            @pl.when(receives(step, way))
            def _():
                source, arrival = line_arrival(chunk, step, way)
                arrival.wait_recv()
                if step + 1 < lines - 1:

                    @pl.when(sends(step + 1, way))
                    def _():
                        line_copy(chunk, step + 1, way).start()

                @pl.when(by_row(chunk, source))
                def _():
                    y_copy(chunk, source).start()

                core_copy(chunk, y, source).start()

    def from_mate(chunk):
        some(1, y_send.at[0], y_recv.at[chunk, 0]).wait_recv()
        core_copy(chunk, 1 - y, z).start()

    def to_mate(chunk):
        @pl.when(turns(chunk))
        def _():
            turn_copy(chunk).start()

    def from_row(chunk):
        @pl.when(turns(chunk))
        def _():
            some(lines - 2, y_send.at[0], y_recv.at[chunk, 1]).wait_recv()
            turn_arrival(chunk).wait_recv()

        @pl.when(jnp.logical_not(turns(chunk)))
        def _():
            some(lines - 1, y_send.at[0], y_recv.at[chunk, 1]).wait_recv()

        for step in range(1, lines):
            core_copy(chunk, 1 - y, lax.rem(z + step, lines)).start()

    def from_core(chunk):
        some(n // 2, c_send.at[0], c_recv.at[chunk]).wait_recv()


    def transform(chunk):
        def lanes(index):
            return gathered[chunk, :, index * LANES : (index + 1) * LANES]

        for which in range(4):
            odd = which // 2
            position = which % 2
            if which < 2:
                tail = lanes(4 + 2 * which)
            elif which == 2:
                tail = lanes(5)
            else:
                tail = jnp.where(lane_index >= rest, lanes(4), lanes(5))
            right = split(jnp.concatenate([lanes(which), tail], axis=1))
            left = jnp.concatenate([table[position], table[2 + which]], axis=1)
            result = split_product(left, count, right)
            for lane in range(2):
                spectrum[lane, pl.ds(odd * vectors + position * CHUNKS + chunk, count, stride=pitch), :] = result[
                    :, lane * LANES : (lane + 1) * LANES
                ]

    pl.semaphore_wait(barrier, 4 + jnp.minimum(z, 1) + jnp.minimum(lines - 1 - z, 1))
    def at_width(blocks, action):
        def run(chunk):
            wide_now[0] = blocks
            action(chunk)

        return run

    pl.loop(0, CHUNKS - NARROW)(at_width(7, start_lines))
    pl.loop(CHUNKS - NARROW, CHUNKS)(at_width(6, start_lines))

    raw[:, freqs:] = jnp.zeros((2, raw.shape[1] - freqs) + tuple(raw.shape[2:]), jnp.float32)
    short = filled(pieces - 1, 1)
    if short < PIECE:

        @pl.when(core == 1)
        def _():
            begin = (pieces - 1) * PIECE + short
            for owner in range(1, 3):
                kbuf[owner, :, begin:] = jnp.zeros((2, PIECE - short) + tuple(kbuf.shape[3:]), jnp.float32)


    for piece in range(pieces):
        raw_copy(piece).wait()
        sort_piece(piece)
        send_piece(piece)

    forward_copy.wait()
    for backward_copy in backward_copies:
        backward_copy.wait()

    def finish(chunk):
        @pl.when(chunk >= CHUNKS - NARROW)
        def _():
            unpack(chunk)

        transform(chunk)

    stages = [
        (functools.partial(from_lines, step=0), 0), (from_mate, 2),
        (functools.partial(from_lines, step=1), 2), (functools.partial(from_lines, step=2), 3), (to_mate, 4),
        (from_row, 6), (from_core, 7),
    ]
    last_age = stages[-1][1]

    @pl.loop(0, CHUNKS + last_age)
    def _(turn):
        for stage, age in stages:
            chunk = turn - age
            for blocks, begin, end in ((7, 0, CHUNKS - NARROW), (6, CHUNKS - NARROW, CHUNKS)):

                @pl.when(jnp.logical_and(chunk >= begin, chunk < end))
                def _():
                    at_width(blocks, stage)(chunk)

        pl.when(turn >= last_age)(lambda: finish(turn - last_age))

    columns = GROUP * 2 * vectors
    row_freq = lax.broadcasted_iota(jnp.int32, (4 * rows, columns), 0) // points % GROUP
    col_freq = lax.broadcasted_iota(jnp.int32, (4 * rows, columns), 1) // (2 * vectors)
    own = row_freq == col_freq
    lane = lax.broadcasted_iota(jnp.int32, (2 * rows, LANES), 1)
    row = lax.broadcasted_iota(jnp.int32, (2 * rows, LANES), 0) // points % 2
    first_half = lane % vectors < vectors // 2
    sign = jnp.where(first_half == (row == 0), 1.0, -1.0)
    shares = batch_shares(batch * GROUP)
    step_rows = shares[0][1]
    lane_group = lax.broadcasted_iota(jnp.int32, (step_rows, LANES), 1) // vectors
    known_rows = lax.broadcasted_iota(jnp.int32, (step_rows, LANES), 0) < shares[1][1]

    def value_rows(turn):
        return pl.ds(pl.multiple_of(turn * step_rows, GROUP), step_rows)

    def value_copy(turn, target):
        place_rows = value_rows(turn)
        return pltpu.make_async_remote_copy(
            src_ref=send_val.at[target, place_rows],
            dst_ref=recv_val.at[jnp.where(core == target, 0, 2), place_rows],
            send_sem=v_send.at[0], recv_sem=v_recv.at[0],
            device_id=(other_chip, target), device_id_type=MESH,
        )

    def value_keep(turn):
        place_rows = value_rows(turn)
        return pltpu.make_async_remote_copy(
            src_ref=send_val.at[2, place_rows], dst_ref=recv_val.at[1, place_rows],
            send_sem=v_send.at[0], recv_sem=v_recv.at[0],
            device_id=(me, other_core), device_id_type=MESH,
        )

    @pl.loop(0, BATCHES)
    def _(turn):
        for which in range(BATCHES):

            @pl.when(turn == which)
            def _():
                wait_batch(which)

        for step in range(batch):
            group = turn * batch + step
            begin = pl.multiple_of(group * GROUP * pitch, GROUP)
            sides = []
            for side in range(2):
                pieces_of = [spectrum[side, pl.ds(begin + step_f * pitch, 2 * vectors), :] for step_f in range(GROUP)]
                sides.append(jnp.concatenate(pieces_of, axis=0))
            right = split(jnp.concatenate(sides, axis=1))
            parts = []
            for part in range(2):
                for near, far in (
                    (packed[x, part, group, core], kbuf[0, part, group]), (kbuf[1, part, group], kbuf[2, part, group]),
                ):
                    parts.append(jnp.concatenate([near.reshape(rows, LANES), far.reshape(rows, LANES)], axis=1))
            left = jnp.concatenate(parts, axis=0)
            found = jnp.where(own, product(split(left), right, NT_DIMS), 0.0)
            width = columns
            while width > LANES:
                width //= 2
                found = found[:, :width] + found[:, width:]
            hop = LANES // 2
            while hop >= 2 * vectors:
                found = found + pltpu.roll(found, hop, 1)
                hop //= 2
            turned = found[2 * rows :]
            turned = jnp.where(
                first_half, pltpu.roll(turned, LANES - vectors // 2, 1), pltpu.roll(turned, vectors // 2, 1)
            )
            value = found[: 2 * rows] + sign * turned
            for owner in range(2):
                product_s[owner, pl.ds(pl.multiple_of(group * rows, rows), rows), :] = value[
                    owner * rows : (owner + 1) * rows
                ]
        for owner in (1, 0):
            merged = [jnp.zeros((step_rows, LANES), jnp.float32)] * 2
            for share in range(2):
                for point in range(points):
                    begin = (turn * batch * GROUP + shares[share][0]) * points + point
                    value = product_s[owner, pl.ds(begin, step_rows, stride=points), :]
                    if share == 1:
                        value = jnp.where(known_rows, value, 0.0)
                    shifted = pltpu.roll(value, vectors, 1)
                    index = share * points + point
                    for target in range(2):
                        chosen = value if index % 2 == target else shifted
                        merged[target] = jnp.where(lane_group == index, chosen, merged[target])
            if owner == 1:
                for target in range(2):
                    send_val[target, value_rows(turn), :] = merged[target]
                for target in range(2):
                    value_copy(turn, target).start()
            else:
                send_val[2, value_rows(turn), :] = jnp.where(core == 0, merged[1], merged[0])
                own_val[value_rows(turn), :] = jnp.where(core == 0, merged[0], merged[1])
                value_keep(turn).start()

    sent = BATCHES * step_rows
    all_of(recv_val.at[:, pl.ds(0, sent)], v_send.at[0], v_recv.at[0]).wait_recv()

    own_half = vectors // 2
    blocks = []
    for near in (own_val[:sent, :] + recv_val[0, :sent, :], recv_val[1, :sent, :] + recv_val[2, :sent, :]):
        turned = jnp.concatenate([near, jnp.zeros((LANES - sent, LANES), jnp.float32)], axis=0).T
        for position in range(2):
            for share in range(2):
                begins = [
                    ((share * points + point) * 2 + position) * own_half for point in range(points)
                ]
                blocks.append(jnp.concatenate([turned[begin : begin + own_half] for begin in begins], axis=0))
    left = split(jnp.concatenate(blocks, axis=1))
    right = []
    for index in range(2):
        right.append(jnp.concatenate([inverse[near, index].reshape(4 * LANES, wide) for near in range(2)], axis=0))
    total = product(left, right, plain)
    partial[...] = total

    field_copy = pltpu.make_async_remote_copy(
        src_ref=partial, dst_ref=pair, send_sem=f_send.at[0], recv_sem=f_recv.at[0],
        device_id=(me, other_core), device_id_type=MESH,
    )

    energy = total * total
    summed = energy[:own_half]
    for point in range(1, points):
        summed = summed + energy[point * own_half : (point + 1) * own_half]
    column = jnp.sum(summed, axis=1, keepdims=True)
    lane8 = lax.broadcasted_iota(jnp.int32, (own_half, LANES), 1)
    row8 = lax.broadcasted_iota(jnp.int32, (own_half, LANES), 0)
    flat = jnp.sum(jnp.where(lane8 == row8 + core * own_half, column, 0.0), axis=0, keepdims=True)
    square[...] = flat
    mine = core * n + me
    squares[mine] = flat

    def square_copy(target, target_core):
        return pltpu.make_async_remote_copy(
            src_ref=square, dst_ref=squares.at[mine], send_sem=r_send.at[0], recv_sem=r_recv.at[0],
            device_id=(target, target_core), device_id_type=MESH,
        )

    @pl.loop(1, n)
    def _(step):
        away = jnp.where(z < lines // 2, n - step, step)
        square_copy(lax.rem(me + away, n), core).start()
        square_copy(lax.rem(me + away, n), other_core).start()

    square_copy(me, other_core).start()
    field_copy.start()

    block_tiles = local // 8
    every = sum(7 if chunk < CHUNKS - NARROW else 6 for chunk in range(CHUNKS)) * block_tiles
    late = sum(7 if chunk < CHUNKS - NARROW else 6 for chunk in range(CHUNKS // 2, CHUNKS)) * block_tiles
    for line in range(lines):
        ahead = line + 1 if line + 1 < lines else 0
        back = lines - line if line > 0 else 0

        @pl.when(z == line)
        def _():
            tiles((ahead + back) * every, z_send.at[0], z_recv.at[0, 0]).wait_send()

    tiles(lines * every - late, y_send.at[0], y_recv.at[0, 0]).wait_send()
    tiles(late, w_send.at[0], w_recv.at[0]).wait_send()
    tiles(n // 2 * every, c_send.at[0], c_recv.at[0]).wait_send()
    for target in range(2):
        all_of(packed.at[0, :, pl.ds(0, groups - PIECE + filled(pieces - 1, target)), target],
               k_send.at[target], k_recv.at[0]).wait_send()
    all_of(packed.at[0, :, :, 0], k_send.at[2], k_recv.at[0]).wait_send()
    all_of(send_val.at[:, pl.ds(0, sent)], v_send.at[0], v_recv.at[0]).wait_send()
    field_copy.wait_send()

    field_copy.wait_recv()
    tall = points * own_half
    out_ref[pl.ds(pl.multiple_of(core * tall, tall), tall), :] = total
    out_ref[pl.ds(pl.multiple_of(other_core * tall, tall), tall), :] = pair[...]
    all_of(squares.at[pl.ds(0, 2 * n - 1)], r_send.at[0], r_recv.at[0]).wait()

    energy_all = squares[0]
    for device in range(1, 2 * n):
        energy_all = energy_all + squares[device]
    scale = jnp.sqrt(energy_all / (points * n * steps) + 1e-06)
    rms_ref[...] = jnp.broadcast_to(scale, rms_ref.shape)


def finish_kernel(field_ref, scale_ref, out_ref, rms_ref):
    vectors, points, steps = out_ref.shape
    scale = scale_ref[:1]
    rms_ref[...] = scale[0, :vectors]
    diagonal = lax.broadcasted_iota(jnp.int32, (vectors, LANES), 0) == lax.broadcasted_iota(
        jnp.int32, (vectors, LANES), 1
    )
    spread = jnp.broadcast_to(scale, (vectors, LANES))
    divisor = jnp.sum(jnp.where(diagonal, spread, 0.0), axis=1, keepdims=True)
    half = vectors // 2
    for point in range(points):
        near = field_ref[point * half : (point + 1) * half, :steps]
        far = field_ref[(points + point) * half : (points + point + 1) * half, :steps]
        out_ref[:, point, :] = jnp.concatenate([near, far], axis=0) / divisor


def paired_body(data, spectra):
    n = lax.axis_size("param")
    vectors, local, steps = data.shape
    sensors, points, freqs = spectra.shape[1:]
    wide = -(-steps // LANES) * LANES
    groups = -(-freqs // (2 * GROUP))
    count = groups * GROUP
    rows_pad = -(-count // 16) * 16
    pieces = groups // PIECE
    lines = n // 4
    forward, backward = paired_tables(steps, freqs, groups, rows_pad, wide)
    maps = fold_maps(steps)

    turned = jnp.transpose(spectra, (0, 3, 2, 1)).reshape(2, freqs, points, 2, LANES)
    turned = jnp.transpose(turned, (0, 1, 3, 2, 4)).reshape(2, freqs, 2 * points, LANES)

    hbm = pl.BlockSpec(memory_space=pl.ANY)
    vmem = pl.BlockSpec(memory_space=pltpu.VMEM)
    dma = pltpu.SemaphoreType.DMA
    f32, bf16 = jnp.float32, jnp.bfloat16
    fields, scale = pl.pallas_call(
        functools.partial(kernel, n, lines, vectors, local, steps, points, freqs, groups, wide),
        out_shape=(
            pltpu.VMEM((points * vectors, wide), f32),
            pltpu.VMEM((8, LANES), f32),
        ),
        in_specs=[hbm, hbm, hbm, hbm, vmem],
        out_specs=(vmem, vmem),
        scratch_shapes=[
            pltpu.VMEM((vectors, local, steps), f32),
            pltpu.VMEM((2, wide, 4 * LANES), bf16),
            pltpu.VMEM((2, 2 * count, 2 * points, LANES), f32),
            pltpu.VMEM((2, 2, groups, 2, GROUP // 2, 2 * points, LANES), f32),
            pltpu.VMEM((3, 2, groups, GROUP // 2, 2 * points, LANES), f32),
            pltpu.VMEM((CHUNKS, sensors, 7 * LANES), f32),
            pltpu.VMEM((6, 2 * rows_pad, LANES), bf16),
            pltpu.VMEM((2, 2, 2, 2, LANES, wide), bf16),
            pltpu.VMEM((2, count * (2 * vectors + PAD_ROWS), LANES), f32),
            pltpu.VMEM((2, (count + GROUP) * points, LANES), f32),
            pltpu.VMEM((LANES, LANES), f32),
            pltpu.VMEM((3, LANES, LANES), f32),
            pltpu.VMEM((3, LANES, LANES), f32),
            pltpu.VMEM((points * vectors // 2, wide), f32),
            pltpu.VMEM((points * vectors // 2, wide), f32),
            pltpu.VMEM((1, LANES), f32),
            pltpu.VMEM((2 * n, 1, LANES), f32),
            dma((4,)),
            dma((pieces,)),
            dma((3,)), dma((BATCHES,)),
            dma((1,)), dma((CHUNKS, lines - 1)),
            dma((1,)), dma((CHUNKS, 2)),
            dma((1,)), dma((CHUNKS,)),
            dma((1,)), dma((CHUNKS,)),
            dma((1,)), dma((1,)),
            dma((1,)), dma((1,)),
            dma((1,)), dma((1,)),
        ],
        compiler_params=pltpu.CompilerParams(
            collective_id=0, has_side_effects=True, vmem_limit_bytes=60 * 1024 * 1024
        ),
    )(data, turned, jnp.asarray(forward), jnp.asarray(backward), jnp.asarray(maps))
    return pl.pallas_call(
        finish_kernel,
        out_shape=(jax.ShapeDtypeStruct((vectors, points, steps), f32), jax.ShapeDtypeStruct((vectors,), f32)),
        in_specs=[vmem, vmem],
        out_specs=(vmem, vmem),
    )(pltpu.with_memory_space_constraint(fields, pltpu.VMEM), pltpu.with_memory_space_constraint(scale, pltpu.VMEM))


def solution(mesh):
    in_specs = (P(None, ("sensor", "param"), None), P(None, "sensor", "param", None))
    out_specs = (P(None, "param", None), P())
    n = mesh.shape["param"]
    pair = mesh.shape["sensor"] == 2 and n == 16

    def body(data, spectra):
        vectors, local, _ = data.shape
        sensors, points = spectra.shape[1:3]
        fits = local * n == sensors and local % 8 == 0 and sensors == 2 * LANES and vectors == 2 * CHUNKS
        fits = fits and points * 2 * vectors == LANES and folded_layout_fits(data.shape[2])
        return (paired_body if pair and fits else general_body)(data, spectra)

    return jax.shard_map(body, mesh=mesh, in_specs=in_specs, out_specs=out_specs, check_vma=False)
```
